32 devices in a mesh: group: 2 (over y), win: 16 (over z, x, core).
Axes of the slice: x: 2, y: 2, z: 4, core: 2. Of those that a mesh axis runs over, the one named last changes fastest.
Arguments:
- img_qkv: bfloat16 [64, 256, 4608], P(('group', 'win')), parts along dimension 0, may hold values from -100 to 100
- txt_kv: bfloat16 [64, 128, 3072], P(('group', 'win')), parts along dimension 0, may hold values from -6 to 6
- hidden: bfloat16 [64, 256, 3072], P(('group', 'win')), parts along dimension 0, may hold values from -6 to 6
- w_proj: bfloat16 [1536, 3072], P('win'), may hold values from -0.15625 to 0.15625
- w_out: bfloat16 [3072, 64], replicated, may hold values from -0.109375 to 0.109375
- modulation: float32 [6, 3072], P('group'), parts along dimension 0, may hold values from -3 to 3
- anchors: int32 [64, 2], P(('group', 'win')), parts along dimension 0, may hold values from 0 to 255, as said below
- blend_weight: int32 [64, 32, 32], P(('group', 'win')), parts along dimension 0, may hold values from 0 to 8
Outputs:
- velocity: float32 [16, 512, 64], P(None, ('group', 'win')), parts along dimension 1
The draws below stay inside these ranges and needn't reach their ends.
There are 2 independent parts, one for each index of `group`. The reference program is written for one: setup_inputs(seed, part) draws one part's arguments, and reference() takes and returns one part's arrays. A program takes and returns all parts, laid end to end along the dimension named above; an argument that names none is the same for every part. Nothing has to cross between parts.
Inputs may be any that keep to these rules, and one draw needn't show every extreme that they name: `anchors`: window w's anchor row lies in [16 * (w // 2), 16 * (w // 2) + 16); its columns wrap around the panorama; the 2 windows w with the same w // 2 have anchor columns (s + 32 * (w % 2)) mod 64 for one s of that band, so that they cover all 64 columns.
All inputs are finite; a program needn't handle non-finite values.
Results may differ from the reference program's by a relative error of at most 0.0029.
Values may be sent and summed in bfloat16 or wider, within the bound.
A program may use at most 128 MiB of HBM per device.

```python
import math
import jax
import jax.numpy as jnp
from jax import lax

D = 3072
HD = 128
C = 16
HEADS = 12
PATCH = 2
WIN = 32
TXT = 128
WIN_DEV = 2
LW = 64
BAND = 16
GRID = 16
P_SIZE = 256
HW = 1536
WINDOWS = 32
LH = 256


def draw_img_qkv(key, part):
    key_main = jax.random.fold_in(key, 11)
    values_all = jax.random.normal(key_main, (WINDOWS, P_SIZE, 3 * HW), jnp.float32)
    values_all = jnp.clip(values_all, -4.5, 4.5)
    return values_all.astype(jnp.bfloat16)


def draw_anchors(key, part):
    key_rows = jax.random.fold_in(key, 21)
    key_cols = jax.random.fold_in(key, 22)
    slot_index = jnp.arange(WINDOWS, dtype=jnp.int32)
    band_index = slot_index // WIN_DEV
    within = slot_index % WIN_DEV
    row_anchor = band_index * BAND + jax.random.randint(key_rows, (WINDOWS,), 0, BAND, jnp.int32)
    shift_all = jax.random.randint(key_cols, (WINDOWS,), 0, LW, jnp.int32)
    band_shift = shift_all[band_index * WIN_DEV]
    col_anchor = (band_shift + WIN * within) % LW
    return jnp.stack([row_anchor, col_anchor], axis=1).astype(jnp.int32)


def place_ends(values, rng, least, high):
    longest = values.shape.index(max(values.shape))
    spots = []
    for shift in (0, 1):
        where = [jax.random.randint(jax.random.fold_in(rng, axis), (), 0, length) for axis, length in enumerate(values.shape)]
        where[longest] = (where[longest] + shift) % values.shape[longest]
        spots.append(tuple(where))
    return values.at[spots[0]].set(least).at[spots[1]].set(high)


def block_levels(key, extent, shards, smallest, high):
    factor_of, own = 1.0, jax.random.fold_in(key, 6)
    for dim, parts in shards:
        heights = jnp.exp(jax.random.uniform(jax.random.fold_in(own, dim), (parts,), jnp.float32, smallest / len(shards), high / len(shards)))
        factor_of = factor_of * jnp.repeat(heights, extent[dim] // parts).reshape([-1 if axis == dim else 1 for axis in range(len(extent))])
    return factor_of


def scatter_about(stream_key, shape, scale, reach, shards=(), held_as=jnp.bfloat16):
    loudness = block_levels(stream_key, shape, shards, -0.22, 0.18) if shards else 1.0
    values = jax.random.normal(stream_key, shape, jnp.float32) * scale * loudness
    return jnp.minimum(jnp.maximum(values, -reach), reach).astype(held_as)


def setup_inputs(seed: int = 0, part: int = 0) -> dict:
    streams_of = jax.random.split(jax.random.key(seed), 9)
    own_keys = jax.random.split(jax.random.fold_in(streams_of[8], part), 9)
    return {
        "img_qkv": draw_img_qkv(jax.random.fold_in(jax.random.fold_in(streams_of[8], part), 71), part),
        "txt_kv": scatter_about(own_keys[1], (WINDOWS, TXT, 2 * HW), 1.0, 6.0, ((0, 16),)),
        "hidden": scatter_about(own_keys[2], (WINDOWS, P_SIZE, D), 1.0, 6.0, ((0, 16),)),
        "w_proj": scatter_about(streams_of[3], (HW, D), HW ** -0.5, 0.15625, ((0, 16),)),
        "w_out": scatter_about(streams_of[4], (D, C * PATCH * PATCH), D ** -0.5, 0.109375),
        "modulation": scatter_about(own_keys[5], (3, D), 0.5, 3.0, (), jnp.float32),
        "anchors": draw_anchors(jax.random.fold_in(jax.random.fold_in(streams_of[8], part), 71), part),
        "blend_weight": place_ends(jax.random.randint(own_keys[7], (WINDOWS, WIN, WIN), 0, 9), jax.random.fold_in(own_keys[7], 1), 0, 8).astype(jnp.int32),
    }


def window_velocity(one_qkv, one_txt, one_hidden, w_proj, w_out, modulation):
    features = HEADS * HD
    queries = one_qkv[:, :features].reshape(P_SIZE, HEADS, HD).astype(jnp.float32)
    all_keys = jnp.concatenate([one_txt[:, :features], one_qkv[:, features:2 * features]], axis=0)
    all_keys = all_keys.reshape(TXT + P_SIZE, HEADS, HD).astype(jnp.float32)
    all_values = jnp.concatenate([one_txt[:, features:], one_qkv[:, 2 * features:]], axis=0)
    all_values = all_values.reshape(TXT + P_SIZE, HEADS, HD).astype(jnp.float32)
    scores = jnp.einsum('qhd,khd->hqk', queries, all_keys) / math.sqrt(HD)
    scores = scores - lax.optimization_barrier(jnp.max(scores, axis=-1, keepdims=True))
    exp_scores = jnp.exp(scores)
    soft_weights = (exp_scores / lax.optimization_barrier(jnp.sum(exp_scores, axis=-1, keepdims=True))).astype(jnp.bfloat16)
    attended = jnp.einsum('hqk,khd->qhd', soft_weights.astype(jnp.float32), all_values)
    attended = attended.reshape(P_SIZE, features).astype(jnp.bfloat16)
    projected = jnp.dot(attended, w_proj, preferred_element_type=jnp.float32)
    residual = one_hidden.astype(jnp.float32) + modulation[0] * projected
    row_mean = lax.optimization_barrier(jnp.mean(residual, axis=-1, keepdims=True))
    centred = residual - row_mean
    row_var = lax.optimization_barrier(jnp.mean(centred * centred, axis=-1, keepdims=True))
    normed = centred * lax.rsqrt(row_var + 1e-06)
    modulated = (normed * (1.0 + modulation[1]) + modulation[2]).astype(jnp.bfloat16)
    return jnp.dot(modulated, w_out, preferred_element_type=jnp.float32)

def unpatch(patch_vel):
    window_count = patch_vel.shape[0]
    patch_grid = patch_vel.reshape(window_count, GRID, GRID, C, PATCH, PATCH)
    return patch_grid.transpose(0, 3, 1, 4, 2, 5).reshape(window_count, C, WIN, WIN)

def place_window(canvas, totals, contrib, weights, row_at, col_at):
    zero_index = jnp.zeros((), jnp.int32)
    region = lax.dynamic_slice(canvas, (zero_index, row_at, col_at), (C, WIN, WIN))
    canvas = lax.dynamic_update_slice(canvas, region + contrib, (zero_index, row_at, col_at))
    weight_region = lax.dynamic_slice(totals, (row_at, col_at), (WIN, WIN))
    totals = lax.dynamic_update_slice(totals, weight_region + weights, (row_at, col_at))
    return (canvas, totals)

def fold_columns(field):
    span_cols = field.shape[-1] - WIN
    leading = field[..., :span_cols]
    wrapped = field[..., span_cols:]
    padding = [(0, 0)] * (field.ndim - 1) + [(0, span_cols - WIN)]
    return leading + jnp.pad(wrapped, padding)

def reference(img_qkv, txt_kv, hidden, w_proj, w_out, modulation, anchors, blend_weight):

    def per_window(window_items):
        return window_velocity(window_items[0], window_items[1], window_items[2], w_proj, w_out, modulation)
    patch_vel = lax.map(per_window, (img_qkv, txt_kv, hidden))
    window_vel = unpatch(patch_vel)
    weights = blend_weight.astype(jnp.float32)
    contrib = window_vel * weights[:, None]
    canvas = jnp.zeros((C, LH + WIN, LW + WIN), jnp.float32)
    totals = jnp.zeros((LH + WIN, LW + WIN), jnp.float32)

    def add_one(window, running):
        row_at = anchors[window, 0].astype(jnp.int32)
        col_at = anchors[window, 1].astype(jnp.int32)
        return place_window(running[0], running[1], contrib[window], weights[window], row_at, col_at)
    canvas, totals = lax.fori_loop(0, WINDOWS, add_one, (canvas, totals))
    canvas = fold_columns(canvas)[:, :LH]
    totals = fold_columns(totals)[:LH]
    return canvas / jnp.maximum(totals, 1.0)[None]
```

```python
import functools
import math

import jax
import jax.numpy as jnp
from jax import lax
from jax.experimental import pallas as pl
from jax.experimental.pallas import tpu as pltpu
from jax.sharding import PartitionSpec as P

HD = 128
C = 16
HEADS = 12
PATCH = 2
WIN = 32
LW = 64
BAND = 16
GRID = 16


def shifted(block, axis, distance):
    devices = range(lax.axis_size(axis))
    route = [(i - distance, i) for i in devices if i - distance in devices]
    return lax.ppermute(block, axis, route)


def place_window(canvas, totals, contrib, weights, row_at, col_at):
    zero_index = jnp.zeros((), jnp.int32)
    region = lax.dynamic_slice(canvas, (zero_index, row_at, col_at), (C, WIN, WIN))
    canvas = lax.dynamic_update_slice(canvas, region + contrib, (zero_index, row_at, col_at))
    weight_region = lax.dynamic_slice(totals, (row_at, col_at), (WIN, WIN))
    totals = lax.dynamic_update_slice(totals, weight_region + weights, (row_at, col_at))
    return (canvas, totals)


def fold_columns(field):
    span_cols = field.shape[-1] - WIN
    leading = field[..., :span_cols]
    wrapped = field[..., span_cols:]
    padding = [(0, 0)] * (field.ndim - 1) + [(0, span_cols - WIN)]
    return leading + jnp.pad(wrapped, padding)


def plain_shards(img_qkv, txt_kv, hidden, w_proj, w_out, modulation, anchors, blend_weight):
    window_count, tokens, _ = img_qkv.shape
    features = HEADS * HD
    queries = img_qkv[:, :, :features].reshape(window_count, tokens, HEADS, HD)
    all_keys = jnp.concatenate(
        [txt_kv[:, :, :features], img_qkv[:, :, features : 2 * features]], axis=1
    )
    all_keys = all_keys.reshape(window_count, -1, HEADS, HD)
    all_values = jnp.concatenate([txt_kv[:, :, features:], img_qkv[:, :, 2 * features :]], axis=1)
    all_values = all_values.reshape(window_count, -1, HEADS, HD)
    scores = jnp.einsum(
        "wqhd,wkhd->whqk", queries, all_keys, preferred_element_type=jnp.float32
    ) / math.sqrt(HD)
    scores = scores - jnp.max(scores, axis=-1, keepdims=True)
    exp_scores = jnp.exp(scores)
    soft_weights = (exp_scores / jnp.sum(exp_scores, axis=-1, keepdims=True)).astype(jnp.bfloat16)
    attended = jnp.einsum(
        "whqk,wkhd->wqhd", soft_weights, all_values, preferred_element_type=jnp.float32
    )
    attended = attended.reshape(window_count * tokens, features).astype(jnp.bfloat16)
    whole_proj = lax.all_gather(w_proj, "win", axis=0, tiled=True)
    projected = jnp.dot(attended, whole_proj, preferred_element_type=jnp.float32)
    residual = (
        hidden.reshape(window_count * tokens, -1).astype(jnp.float32) + modulation[0] * projected
    )
    row_mean = jnp.mean(residual, axis=-1, keepdims=True)
    centred = residual - row_mean
    row_var = jnp.mean(centred * centred, axis=-1, keepdims=True)
    normed = centred * lax.rsqrt(row_var + 1e-06)
    modulated = (normed * (1.0 + modulation[1]) + modulation[2]).astype(jnp.bfloat16)
    patch_vel = jnp.dot(modulated, w_out, preferred_element_type=jnp.float32)
    patch_grid = patch_vel.reshape(window_count, GRID, GRID, C, PATCH, PATCH)
    window_vel = patch_grid.transpose(0, 3, 1, 4, 2, 5).reshape(window_count, C, WIN, WIN)
    weights = blend_weight.astype(jnp.float32)
    contrib = window_vel * weights[:, None]
    band_start = lax.axis_index("win") * BAND
    canvas = jnp.zeros((C, BAND + WIN, LW + WIN), jnp.float32)
    totals = jnp.zeros((BAND + WIN, LW + WIN), jnp.float32)

    def add_one(window, running):
        row_at = anchors[window, 0] - band_start
        col_at = anchors[window, 1]
        return place_window(
            running[0], running[1], contrib[window], weights[window], row_at, col_at
        )

    canvas, totals = lax.fori_loop(0, window_count, add_one, (canvas, totals))
    canvas = fold_columns(canvas)
    totals = fold_columns(totals)
    own_canvas = canvas[:, :BAND]
    own_totals = totals[:BAND]
    near_canvas = canvas[:, BAND : 2 * BAND]
    near_totals = totals[BAND : 2 * BAND]
    far_canvas = canvas[:, 2 * BAND :]
    far_totals = totals[2 * BAND :]
    prev_canvas, prev_totals = shifted((near_canvas, near_totals), "win", 1)
    second_canvas, second_totals = shifted((far_canvas, far_totals), "win", 2)
    sum_canvas = own_canvas + prev_canvas + second_canvas
    sum_totals = own_totals + prev_totals + second_totals
    return sum_canvas / jnp.maximum(sum_totals, 1.0)[None]


LOG2E = 1.4426950408889634
MESH_ID = pl.DeviceIdType.MESH


def block_kernel(
    n,
    qkv_hbm,
    txt_hbm,
    hid_hbm,
    wp_hbm,
    wout_hbm,
    mod_hbm,
    anchors_hbm,
    blend_hbm,
    out_ref,
    qkv,
    txt,
    hid,
    weights,
    att,
    left_first,
    left_mid,
    left_last,
    acc,
    wout,
    wperm,
    mod,
    anchors,
    blend,
    cells,
    hot,
    totals,
    total_near,
    total_far,
    sum_one,
    sum_two,
    centre,
    vel,
    feature,
    near_out,
    far_out,
    near_in,
    far_in,
    load_sems,
    cw_send,
    cw_recv,
    ccw_send,
    ccw_recv,
    y_send,
    y_recv,
    part_send,
    part_recv,
    halo_send,
    halo_recv,
):
    windows, tokens, _ = qkv.shape
    rows = wp_hbm.shape[0]
    width = weights.shape[1]
    features = HEADS * HD
    deep = 2 * rows
    unit = width // 6
    half = unit // 2
    chips = n // 2
    reach = chips // 2
    group = lax.axis_index("group")
    me = lax.axis_index("win")
    core = me % 2
    chip = me // 2
    depth, side = chip // 2, chip % 2
    place = depth + side * (chips - 1 - 2 * depth)

    def chip_at(position):
        spot = (position + chips) % chips
        turn = spot // reach
        return 2 * (spot + turn * (chips - 1 - 2 * spot)) + turn

    onward = (group, chip_at(place + 1) * 2 + core)
    backward = (group, chip_at(place - 1) * 2 + core)
    across = (1 - group, me)
    partner = (group, me + 1 - 2 * core)

    def source(way, d):
        return chip_at(place + d) if way else chip_at(place - d)

    def column(way, which, u):
        flip = which * (5 - 2 * u) * unit
        return (5 - u) * unit - flip if way else u * unit + flip

    def region(which_chip, which_core, col, cols):
        row = pl.multiple_of((which_chip * 2 + which_core) * rows, 16)
        return weights.at[pl.ds(row, rows), pl.ds(pl.multiple_of(col, 128), cols)]

    def remote(src, dst, send, recv, device):
        return pltpu.make_async_remote_copy(
            src_ref=src, dst_ref=dst, send_sem=send, recv_sem=recv,
            device_id=device, device_id_type=MESH_ID,
        )

    def ring(way, d, piece, hop):
        if d == reach and piece >= 2:
            col, cols = column(way, group, 2) + (piece - 2) * half, half
        else:
            col, cols = column(way, group, piece), unit
        ref = region(source(way, d - 1 + hop), core, col, cols)
        send, recv = (ccw_send, ccw_recv) if way else (cw_send, cw_recv)
        return remote(
            ref, ref, send.at[d - 1, piece], recv.at[d - 1, piece], backward if way else onward
        )

    def yy(d, u, way, which):
        ref = region(source(way, d), core, column(way, which, u), unit)
        j = ((d - 1) * 2 + u) * 2 + way
        return remote(ref, ref, y_send.at[j], y_recv.at[j], across)

    names = [("own",)]
    for d in range(1, reach):
        for way in range(2):
            names += [("ring", d, way, 0), ("ring", d, way, 1)]
            names += [("far", d, way, 0), ("far", d, way, 1)] if d == reach - 1 else [("both", d, way)]
    for way in range(2):
        names += [("last", way, piece) for piece in range(4)]
    spot_of = {name: i for i, name in enumerate(names)}

    def part(name, which_core):
        kind = name[0]
        if kind == "own":
            ref = region(chip, which_core, 0, width)
        elif kind == "ring":
            _, d, way, upper = name
            low = jnp.minimum(column(way, group, 0), column(way, group, 1))
            col = 2 * unit if upper else low
            ref = region(source(way, d), which_core, col, 2 * unit)
        elif kind == "both":
            _, d, way = name
            low = jnp.minimum(column(way, 1 - group, 0), column(way, 1 - group, 1))
            ref = region(source(way, d), which_core, low, 2 * unit)
        elif kind == "far":
            _, d, way, u = name
            ref = region(source(way, d), which_core, column(way, 1 - group, u), unit)
        else:
            _, way, piece = name
            if piece >= 2:
                ref = region(
                    source(way, reach), which_core, column(way, group, 2) + (piece - 2) * half, half
                )
            else:
                ref = region(source(way, reach), which_core, column(way, group, piece), unit)
        i = spot_of[name]
        return remote(ref, ref, part_send.at[i], part_recv.at[i], partner)

    landed = set()

    def need(*wanted):
        for name in wanted:
            if name not in landed:
                landed.add(name)
                part(name, 1 - core).wait_recv()

    own_load = pltpu.make_async_copy(wp_hbm, region(chip, core, 0, width), load_sems.at[0])
    own_load.start()
    loads = []
    for w in range(windows):
        loads.append(
            (
                pltpu.make_async_copy(qkv_hbm.at[w], qkv.at[w], load_sems.at[1 + 2 * w]),
                pltpu.make_async_copy(txt_hbm.at[w], txt.at[w], load_sems.at[2 + 2 * w]),
            )
        )
    base = 1 + 2 * windows
    side_loads = [
        pltpu.make_async_copy(wout_hbm, wout, load_sems.at[base]),
        pltpu.make_async_copy(mod_hbm, mod, load_sems.at[base + 1]),
        pltpu.make_async_copy(anchors_hbm, anchors, load_sems.at[base + 2]),
        pltpu.make_async_copy(blend_hbm, blend, load_sems.at[base + 3]),
    ]
    hid_load = pltpu.make_async_copy(hid_hbm, hid, load_sems.at[base + 4])

    barrier = pltpu.get_barrier_semaphore()
    after = [(group, (me + 1) % n), (group, (me + 2) % n)]
    before = [(group, (me + n - 1) % n), (group, (me + n - 2) % n)]
    greeted = [onward, backward, across, partner] + after + before
    for device in greeted:
        pl.semaphore_signal(barrier, inc=1, device_id=device, device_id_type=MESH_ID)
    for copy in loads[0]:
        copy.start()
    pl.semaphore_wait(barrier, len(greeted))

    own_load.wait()
    for piece in range(4):
        ring(0, 1, piece, 0).start()
        ring(1, 1, piece, 0).start()
    part(("own",), core).start()
    for pair in loads[1:]:
        for copy in pair:
            copy.start()
    for copy in side_loads:
        copy.start()
    hid_load.start()

    scale = LOG2E / math.sqrt(HD)

    def attend(w, h):
        col = pl.multiple_of(h * HD, HD)
        cols = pl.ds(col, HD)
        kcols = pl.ds(pl.multiple_of(col + features, HD), HD)
        vcols = pl.ds(pl.multiple_of(col + 2 * features, HD), HD)
        q = qkv[w, :, cols]
        dims = (((1,), (1,)), ((), ()))
        st = lax.dot_general(txt[w, :, cols], q, dims, preferred_element_type=jnp.float32)
        si = lax.dot_general(qkv[w, :, kcols], q, dims, preferred_element_type=jnp.float32)
        top = jnp.maximum(jnp.max(st, axis=0, keepdims=True), jnp.max(si, axis=0, keepdims=True))
        pt = jnp.exp2((st - top) * scale)
        pi = jnp.exp2((si - top) * scale)
        total = jnp.sum(pt, axis=0, keepdims=True) + jnp.sum(pi, axis=0, keepdims=True)
        back = (((0,), (0,)), ((), ()))
        out = lax.dot_general(
            txt[w, :, kcols], pt.astype(jnp.bfloat16), back, preferred_element_type=jnp.float32
        ) + lax.dot_general(
            qkv[w, :, vcols], pi.astype(jnp.bfloat16), back, preferred_element_type=jnp.float32
        )
        att[pl.ds(col, HD), pl.ds(pl.multiple_of(w * tokens, 128), tokens)] = (
            out * (1.0 / total)
        ).astype(jnp.bfloat16)

    def spot(which_chip):
        return pl.ds(pl.multiple_of(which_chip * deep, 16), deep)

    def turn_left():
        def turned(chips_held):
            return jnp.concatenate([att[spot(c), :] for c in chips_held], axis=0).T

        left_first[...] = turned([chip, source(0, 1), source(1, 1)])
        for d in range(2, reach):
            left_mid[d - 2] = turned([source(0, d), source(1, d)])
        left_last[...] = turned([source(0, reach)])

    def right(chips_held, at):
        return jnp.concatenate([weights[spot(c), at] for c in chips_held], axis=0)

    def project_first(t):
        at = pl.ds(t * unit, unit)
        held = [chip, source(0, 1), source(1, 1)]
        acc[:, at] = jnp.dot(left_first[...], right(held, at), preferred_element_type=jnp.float32)

    def project_mid(d, t):
        at = pl.ds(t * unit, unit)
        held = [source(0, d), source(1, d)]
        acc[:, at] += jnp.dot(
            left_mid[d - 2], right(held, at), preferred_element_type=jnp.float32
        )

    def finalize(t, piece, first=False):
        at = pl.ds(t * unit + piece * half, half)
        term = acc[:, at] + jnp.dot(
            left_last[...], right([source(0, reach)], at), preferred_element_type=jnp.float32
        )
        residual = hid[:, at].astype(jnp.float32) + mod[0:1, at] * term
        if first:
            mean = jnp.sum(residual, axis=-1, keepdims=True) * (1.0 / half)
            centre[...] = jnp.broadcast_to(mean, centre.shape)
        lanes = centre.shape[1]
        pieces = [residual[:, i : i + lanes] - centre[...] for i in range(0, half, lanes)]
        one = functools.reduce(lambda a, b: a + b, pieces)
        two = functools.reduce(lambda a, b: a + b, [x * x for x in pieces])
        sum_one[...] = one if first else sum_one[...] + one
        sum_two[...] = two if first else sum_two[...] + two
        scaled = (jnp.concatenate(pieces, axis=1) * (1.0 + mod[1:2, at])).astype(jnp.bfloat16)
        term = lax.dot_general(
            wperm[:, at], scaled, (((1,), (1,)), ((), ())), preferred_element_type=jnp.float32
        )
        vel[...] = term if first else vel[...] + term

    grid_log = GRID.bit_length() - 1
    spread = hot.shape[2]
    band = spread // 3
    outs = wout.shape[0]

    def parity(w):
        row_at = anchors[w : w + 1, 0:1] - me * BAND
        return row_at & 1, row_at >> 1, anchors[w : w + 1, 1:2]

    def prepare_weights():
        for copy in side_loads:
            copy.wait()
        order = lax.broadcasted_iota(jnp.int32, (outs, outs), 0)
        taken = lax.broadcasted_iota(jnp.int32, (outs, outs), 1)
        wanted = (order % C) * (PATCH * PATCH) + order // C
        permute = (taken == wanted).astype(jnp.bfloat16)
        wperm[...] = jnp.dot(permute, wout[...], preferred_element_type=jnp.float32).astype(
            jnp.bfloat16
        )
        plain = wperm[...].astype(jnp.float32)
        gain = jnp.sum(plain * (1.0 + mod[1:2, :]), axis=-1, keepdims=True)
        shift = jnp.sum(plain * mod[2:3, :], axis=-1, keepdims=True)
        feature[0] = jnp.broadcast_to(gain, feature.shape[1:])
        feature[1] = jnp.broadcast_to(shift, feature.shape[1:])
        token = lax.broadcasted_iota(jnp.int32, (WIN, tokens), 1)
        line = lax.broadcasted_iota(jnp.int32, (WIN, tokens), 0)
        for w in range(windows):
            held = blend[w].astype(jnp.float32).astype(jnp.bfloat16)
            for b in range(PATCH):
                pick = (line == PATCH * (token & (GRID - 1)) + b).astype(jnp.bfloat16)
                wide = jnp.dot(held, pick, preferred_element_type=jnp.float32)
                for a in range(PATCH):
                    mine = jnp.where(line == PATCH * (token >> grid_log) + a, wide, 0.0)
                    row = jnp.sum(mine, axis=0, keepdims=True)
                    cells[a * PATCH + b, :, w * tokens : (w + 1) * tokens] = jnp.broadcast_to(
                        row, (8, tokens)
                    )

    def prepare_hot(alpha):
        token = lax.broadcasted_iota(jnp.int32, (tokens, 128), 0)
        lane = lax.broadcasted_iota(jnp.int32, (tokens, 128), 1)
        for w in range(windows):
            odd, row_at, col_at = parity(w)
            tall = (token >> grid_log) + row_at + odd * (1 - alpha)
            for b in range(PATCH):
                wide = (PATCH * (token & (GRID - 1)) + b + col_at) & (LW - 1)
                target = tall * LW + wide - lane
                for j in range(spread // 128):
                    hot[alpha * PATCH + b, w * tokens : (w + 1) * tokens, j * 128 : (j + 1) * 128] = (
                        jnp.where(target == j * 128, 1.0, 0.0).astype(jnp.bfloat16)
                    )

    def by_parity(w, straight, swapped):
        odd = parity(w)[0]
        return jnp.where(jnp.broadcast_to(odd, straight.shape) == 0, straight, swapped)

    def prepare_totals():
        found = []
        for alpha in range(PATCH):
            total = jnp.zeros((8, spread), jnp.float32)
            for b in range(PATCH):
                held = []
                for w in range(windows):
                    at = slice(w * tokens, (w + 1) * tokens)
                    straight = cells[alpha * PATCH + b, :, at]
                    swapped = cells[(1 - alpha) * PATCH + b, :, at]
                    held.append(by_parity(w, straight, swapped))
                left = jnp.concatenate(held, axis=1).astype(jnp.bfloat16)
                total += jnp.dot(
                    left, hot[alpha * PATCH + b], preferred_element_type=jnp.float32
                )
            found.append(total)
        upper = lax.broadcasted_iota(jnp.int32, (8, spread), 0) < 4
        total = jnp.where(upper, found[0], found[1])
        for i in range(3):
            totals[i] = total[:, i * band : (i + 1) * band]

    halos = (
        (1, remote(totals.at[1], total_near, halo_send.at[0], halo_recv.at[0], after[0])),
        (2, remote(totals.at[2], total_far, halo_send.at[1], halo_recv.at[1], after[1])),
        (1, remote(near_out, near_in, halo_send.at[2], halo_recv.at[2], after[0])),
        (2, remote(far_out, far_in, halo_send.at[3], halo_recv.at[3], after[1])),
    )

    def send_halo(i):
        ahead, copy = halos[i]

        @pl.when(me + ahead < n)
        def _():
            copy.start()

    def take_halo(i):
        ahead, copy = halos[i]

        @pl.when(me >= ahead)
        def _():
            copy.wait_recv()

    def close_halo(i):
        ahead, copy = halos[i]

        @pl.when(me + ahead < n)
        def _():
            copy.wait_send()

    def clear_halos():
        @pl.when(me < 1)
        def _():
            total_near[...] = jnp.zeros_like(total_near)
            near_in[...] = jnp.zeros_like(near_in)

        @pl.when(me < 2)
        def _():
            total_far[...] = jnp.zeros_like(total_far)
            far_in[...] = jnp.zeros_like(far_in)

    def send_totals():
        send_halo(0)
        send_halo(1)

    def close_totals():
        take_halo(0)
        take_halo(1)
        summed = totals[0] + total_near[...] + total_far[...]
        totals[0] = 1.0 / jnp.maximum(summed, 1.0)

    slots = [(d, u) for d in range(1, reach) for u in range(4)]
    slots += [(reach, piece) for piece in range(4)]
    across_order = [(d, u, way) for d in range(1, reach) for u in range(2) for way in range(2)]

    def serve(d, piece):
        for way in range(2):
            ring(way, d, piece, 1).wait_recv()
            if d + 1 < reach or (d + 1 == reach and piece < 2):
                ring(way, d + 1, piece, 0).start()
            elif d + 1 == reach and piece == 2:
                ring(way, reach, 2, 0).start()
                ring(way, reach, 3, 0).start()
            if d < reach and piece < 2:
                yy(d, piece, way, group).start()
        for way in range(2):
            if d < reach and piece % 2 == 1:
                part(("ring", d, way, piece // 2), core).start()
            elif d == reach:
                part(("last", way, piece), core).start()

    def serve_across(j):
        d, u, way = across_order[j]
        yy(d, u, way, 1 - group).wait_recv()
        if d == reach - 1:
            part(("far", d, way, u), core).start()
        elif u == 1:
            part(("both", d, way), core).start()

    units = [(w, h) for w in range(windows) for h in range(HEADS)]
    ready = set()

    def attend_some(count):
        for _ in range(min(count, len(units))):
            w, h = units.pop(0)
            if w not in ready:
                for copy in loads[w]:
                    copy.wait()
                ready.add(w)
            attend(w, h)

    def first_ones(which):
        need(("own",))
        for way in range(2):
            need(("ring", 1, way, 0), ("ring", 1, way, 1), ("both", 1, way))
        for t in which:
            project_first(t)

    def mid_ones(d, which):
        for way in range(2):
            need(("ring", d, way, 0), ("ring", d, way, 1))
            if d < reach - 1:
                need(("both", d, way))
        for t in which:
            project_mid(d, t)

    last = reach - 1
    total_slots = len(slots)
    work = {i: [] for i in range(total_slots + 1)}
    per = -(-len(units) // 5)
    for i in range(5):
        work[i].append(functools.partial(attend_some, per))
    work[5] += [functools.partial(attend_some, len(units)), turn_left, prepare_weights, clear_halos]
    work[6] += [functools.partial(prepare_hot, 0), functools.partial(prepare_hot, 1)]
    work[7] += [prepare_totals, send_totals, hid_load.wait]
    work[8] += [functools.partial(first_ones, range(3))]
    work[9] += [functools.partial(first_ones, range(3, 6))]
    work[10] += [close_totals]
    for d in range(2, last):
        at = 4 * d + 4
        work[at] += [functools.partial(mid_ones, d, range(6))]

    def third_middle():
        mid_ones(last, (2, 3))

    def end_outer():
        for way in range(2):
            need(("far", last, way, 0), ("last", way, 0))
        for i, t in enumerate((0, 5)):
            project_mid(last, t)
            for piece in range(2):
                finalize(t, piece, first=i == 0 and piece == 0)

    def end_inner(t):
        for way in range(2):
            need(("far", last, way, 1), ("last", way, 1))
        project_mid(last, t)
        for piece in range(2):
            finalize(t, piece)

    def end_middle(piece):
        for way in range(2):
            need(("last", way, 2 + piece))
        for t in (2, 3):
            finalize(t, piece)

    across_done = 0
    for i, (d, piece) in enumerate(slots):
        for step in work[i]:
            step()
        if i == total_slots - 3:
            third_middle()
            end_outer()
        if i == total_slots - 1:
            end_inner(1)
        serve(d, piece)
        until = max(0, i - 2) if i < total_slots - 3 else len(across_order)
        if i == total_slots - 4:
            until = i - 2 + 1
        until = min(until, len(across_order))
        while across_done < until:
            serve_across(across_done)
            across_done += 1
    end_inner(4)
    end_middle(0)
    end_middle(1)

    flat_one = jnp.sum(sum_one[...].T, axis=0, keepdims=True) * (1.0 / width)
    flat_two = jnp.sum(sum_two[...].T, axis=0, keepdims=True) * (1.0 / width)
    rate = lax.rsqrt(flat_two - flat_one * flat_one + 1e-06)
    gain = jnp.concatenate([feature[0]] * (windows * tokens // 128), axis=1)
    shift = jnp.concatenate([feature[1]] * (windows * tokens // 128), axis=1)
    value = rate * (vel[...] - flat_one * gain) + shift
    weighted = []
    for q in range(PATCH * PATCH):
        cell = jnp.concatenate([cells[q]] * (C // 8), axis=0)
        weighted.append(value[q * C : (q + 1) * C] * cell)
    chosen = []
    for alpha in range(PATCH):
        for b in range(PATCH):
            held = []
            for w in range(windows):
                at = slice(w * tokens, (w + 1) * tokens)
                straight = weighted[alpha * PATCH + b][:, at]
                swapped = weighted[(1 - alpha) * PATCH + b][:, at]
                held.append(by_parity(w, straight, swapped))
            both = jnp.concatenate(held, axis=1)
            high = both.astype(jnp.bfloat16)
            low = (both - high.astype(jnp.float32)).astype(jnp.bfloat16)
            chosen.append(jnp.concatenate([high, low], axis=0))

    def placed(alpha, which):
        total = jnp.zeros((2 * C, band), jnp.float32)
        for b in range(PATCH):
            total += jnp.dot(
                chosen[alpha * PATCH + b],
                hot[alpha * PATCH + b, :, which * band : (which + 1) * band],
                preferred_element_type=jnp.float32,
            )
        return total[:C] + total[C:]

    for which, ref, halo in ((2, far_out, 3), (1, near_out, 2)):
        for alpha in range(PATCH):
            ref[alpha * C : (alpha + 1) * C, :] = placed(alpha, which)
        send_halo(halo)
    own = [placed(alpha, 0) for alpha in range(PATCH)]
    inverse = totals[0]
    take_halo(2)
    take_halo(3)
    for alpha in range(PATCH):
        at = slice(alpha * C, (alpha + 1) * C)
        summed = (own[alpha] + near_in[at, :] + far_in[at, :]) * inverse[4 * alpha : 4 * alpha + 1, :]
        for i in range(band // LW):
            out_ref[pl.ds(PATCH * i + alpha, C, stride=BAND), :] = summed[:, i * LW : (i + 1) * LW]

    for d, piece in slots:
        for way in range(2):
            ring(way, d, piece, 0).wait_send()
    for d, u, way in across_order:
        yy(d, u, way, group).wait_send()
    for name in names:
        part(name, core).wait_send()
    for i in range(len(halos)):
        close_halo(i)


def shards(n, img_qkv, txt_kv, hidden, w_proj, w_out, modulation, anchors, blend_weight):
    windows, tokens, qkv_width = img_qkv.shape
    rows, width = w_proj.shape
    total = windows * tokens
    reach = n // 4
    deep = 2 * rows
    outs = w_out.shape[1]
    spread = (BAND + WIN) // PATCH * LW
    band = spread // 3
    any_space = pl.BlockSpec(memory_space=pl.ANY)
    vmem = pl.BlockSpec(memory_space=pltpu.VMEM)
    dma = pltpu.SemaphoreType.DMA
    f32, bf16 = jnp.float32, jnp.bfloat16
    parts = 1 + 6 * (reach - 2) + 8 + 8
    velocity = pl.pallas_call(
        functools.partial(block_kernel, n),
        out_shape=jax.ShapeDtypeStruct((C * BAND, LW), f32),
        in_specs=[any_space] * 8,
        out_specs=vmem,
        scratch_shapes=[
            pltpu.VMEM(img_qkv.shape, bf16),
            pltpu.VMEM(txt_kv.shape, bf16),
            pltpu.VMEM((total, width), bf16),
            pltpu.VMEM((n * rows, width), bf16),
            pltpu.VMEM((n * rows, total), bf16),
            pltpu.VMEM((total, 3 * deep), bf16),
            pltpu.VMEM((reach - 2, total, 2 * deep), bf16),
            pltpu.VMEM((total, deep), bf16),
            pltpu.VMEM((total, width), f32),
            pltpu.VMEM((outs, width), bf16),
            pltpu.VMEM((outs, width), bf16),
            pltpu.VMEM(modulation.shape, f32),
            pltpu.VMEM(anchors.shape, jnp.int32),
            pltpu.VMEM(blend_weight.shape, jnp.int32),
            pltpu.VMEM((PATCH * PATCH, 8, total), f32),
            pltpu.VMEM((PATCH * PATCH, total, spread), bf16),
            pltpu.VMEM((3, 8, band), f32),
            pltpu.VMEM((8, band), f32),
            pltpu.VMEM((8, band), f32),
            pltpu.VMEM((total, 128), f32),
            pltpu.VMEM((total, 128), f32),
            pltpu.VMEM((total, 128), f32),
            pltpu.VMEM((outs, total), f32),
            pltpu.VMEM((2, outs, 128), f32),
            pltpu.VMEM((PATCH * C, band), f32),
            pltpu.VMEM((PATCH * C, band), f32),
            pltpu.VMEM((PATCH * C, band), f32),
            pltpu.VMEM((PATCH * C, band), f32),
            dma((6 + 2 * windows,)),
            dma((reach, 4)),
            dma((reach, 4)),
            dma((reach, 4)),
            dma((reach, 4)),
            dma((4 * (reach - 1),)),
            dma((4 * (reach - 1),)),
            dma((parts,)),
            dma((parts,)),
            dma((4,)),
            dma((4,)),
        ],
        compiler_params=pltpu.CompilerParams(
            collective_id=0, has_side_effects=True, vmem_limit_bytes=60 * 1024 * 1024
        ),
    )(
        img_qkv,
        txt_kv,
        hidden.reshape(total, width),
        w_proj,
        w_out.T,
        modulation,
        anchors,
        blend_weight,
    )
    return velocity.reshape(C, BAND, LW)


def solution(mesh):
    in_specs = (
        P(("group", "win"), None, None),
        P(("group", "win"), None, None),
        P(("group", "win"), None, None),
        P("win", None),
        P(),
        P("group", None),
        P(("group", "win"), None),
        P(("group", "win"), None, None),
    )
    out_specs = P(None, ("group", "win"), None)
    n = mesh.shape["win"]

    def body(*args):
        rows, width = args[3].shape
        ringed = (
            mesh.shape["group"] == 2
            and n % 4 == 0
            and n >= 16
            and rows % 16 == 0
            and width % 1536 == 0
        )
        if ringed:
            return shards(n, *args)
        return plain_shards(*args)

    return jax.shard_map(body, mesh=mesh, in_specs=in_specs, out_specs=out_specs, check_vma=False)
```

```python
import functools
import math

import jax
import jax.numpy as jnp
from jax import lax
from jax.experimental import pallas as pl
from jax.experimental.pallas import tpu as pltpu
from jax.sharding import PartitionSpec as P

HD = 128
C = 16
HEADS = 12
PATCH = 2
WIN = 32
LW = 64
BAND = 16
GRID = 16


def shifted(block, axis, distance):
    devices = range(lax.axis_size(axis))
    route = [(i - distance, i) for i in devices if i - distance in devices]
    return lax.ppermute(block, axis, route)


def place_window(canvas, totals, contrib, weights, row_at, col_at):
    zero_index = jnp.zeros((), jnp.int32)
    region = lax.dynamic_slice(canvas, (zero_index, row_at, col_at), (C, WIN, WIN))
    canvas = lax.dynamic_update_slice(canvas, region + contrib, (zero_index, row_at, col_at))
    weight_region = lax.dynamic_slice(totals, (row_at, col_at), (WIN, WIN))
    totals = lax.dynamic_update_slice(totals, weight_region + weights, (row_at, col_at))
    return (canvas, totals)


def fold_columns(field):
    span_cols = field.shape[-1] - WIN
    leading = field[..., :span_cols]
    wrapped = field[..., span_cols:]
    padding = [(0, 0)] * (field.ndim - 1) + [(0, span_cols - WIN)]
    return leading + jnp.pad(wrapped, padding)


def plain_shards(img_qkv, txt_kv, hidden, w_proj, w_out, modulation, anchors, blend_weight):
    window_count, tokens, _ = img_qkv.shape
    features = HEADS * HD
    queries = img_qkv[:, :, :features].reshape(window_count, tokens, HEADS, HD)
    all_keys = jnp.concatenate(
        [txt_kv[:, :, :features], img_qkv[:, :, features : 2 * features]], axis=1
    )
    all_keys = all_keys.reshape(window_count, -1, HEADS, HD)
    all_values = jnp.concatenate([txt_kv[:, :, features:], img_qkv[:, :, 2 * features :]], axis=1)
    all_values = all_values.reshape(window_count, -1, HEADS, HD)
    scores = jnp.einsum(
        "wqhd,wkhd->whqk", queries, all_keys, preferred_element_type=jnp.float32
    ) / math.sqrt(HD)
    scores = scores - jnp.max(scores, axis=-1, keepdims=True)
    exp_scores = jnp.exp(scores)
    soft_weights = (exp_scores / jnp.sum(exp_scores, axis=-1, keepdims=True)).astype(jnp.bfloat16)
    attended = jnp.einsum(
        "whqk,wkhd->wqhd", soft_weights, all_values, preferred_element_type=jnp.float32
    )
    attended = attended.reshape(window_count * tokens, features).astype(jnp.bfloat16)
    whole_proj = lax.all_gather(w_proj, "win", axis=0, tiled=True)
    projected = jnp.dot(attended, whole_proj, preferred_element_type=jnp.float32)
    residual = (
        hidden.reshape(window_count * tokens, -1).astype(jnp.float32) + modulation[0] * projected
    )
    row_mean = jnp.mean(residual, axis=-1, keepdims=True)
    centred = residual - row_mean
    row_var = jnp.mean(centred * centred, axis=-1, keepdims=True)
    normed = centred * lax.rsqrt(row_var + 1e-06)
    modulated = (normed * (1.0 + modulation[1]) + modulation[2]).astype(jnp.bfloat16)
    patch_vel = jnp.dot(modulated, w_out, preferred_element_type=jnp.float32)
    patch_grid = patch_vel.reshape(window_count, GRID, GRID, C, PATCH, PATCH)
    window_vel = patch_grid.transpose(0, 3, 1, 4, 2, 5).reshape(window_count, C, WIN, WIN)
    weights = blend_weight.astype(jnp.float32)
    contrib = window_vel * weights[:, None]
    band_start = lax.axis_index("win") * BAND
    canvas = jnp.zeros((C, BAND + WIN, LW + WIN), jnp.float32)
    totals = jnp.zeros((BAND + WIN, LW + WIN), jnp.float32)

    def add_one(window, running):
        row_at = anchors[window, 0] - band_start
        col_at = anchors[window, 1]
        return place_window(
            running[0], running[1], contrib[window], weights[window], row_at, col_at
        )

    canvas, totals = lax.fori_loop(0, window_count, add_one, (canvas, totals))
    canvas = fold_columns(canvas)
    totals = fold_columns(totals)
    own_canvas = canvas[:, :BAND]
    own_totals = totals[:BAND]
    near_canvas = canvas[:, BAND : 2 * BAND]
    near_totals = totals[BAND : 2 * BAND]
    far_canvas = canvas[:, 2 * BAND :]
    far_totals = totals[2 * BAND :]
    prev_canvas, prev_totals = shifted((near_canvas, near_totals), "win", 1)
    second_canvas, second_totals = shifted((far_canvas, far_totals), "win", 2)
    sum_canvas = own_canvas + prev_canvas + second_canvas
    sum_totals = own_totals + prev_totals + second_totals
    return sum_canvas / jnp.maximum(sum_totals, 1.0)[None]


LOG2E = 1.4426950408889634
MESH_ID = pl.DeviceIdType.MESH


def block_kernel(
    n,
    qkv_hbm,
    txt_hbm,
    hid_hbm,
    wp_hbm,
    wout_hbm,
    mod_hbm,
    anchors_hbm,
    blend_hbm,
    out_ref,
    qkv,
    txt,
    hid,
    weights,
    att,
    left_first,
    left_mid,
    left_last,
    acc,
    wout,
    wperm,
    mod,
    anchors,
    blend,
    cells,
    hot,
    totals,
    total_near,
    total_far,
    sum_two,
    centre,
    vel,
    feature,
    near_out,
    far_out,
    near_in,
    far_in,
    load_sems,
    cw_send,
    cw_recv,
    ccw_send,
    ccw_recv,
    y_send,
    y_recv,
    part_send,
    part_recv,
    halo_send,
    halo_recv,
):
    windows, tokens, _ = qkv.shape
    rows = wp_hbm.shape[0]
    width = weights.shape[1]
    features = HEADS * HD
    deep = 2 * rows
    unit = width // 6
    half = unit // 2
    outs = wout.shape[0]
    chips = n // 2
    reach = chips // 2
    group = lax.axis_index("group")
    me = lax.axis_index("win")
    core = me % 2
    chip = me // 2
    depth, side = chip // 2, chip % 2
    place = depth + side * (chips - 1 - 2 * depth)

    def chip_at(position):
        spot = (position + chips) % chips
        turn = spot // reach
        return 2 * (spot + turn * (chips - 1 - 2 * spot)) + turn

    onward = (group, chip_at(place + 1) * 2 + core)
    backward = (group, chip_at(place - 1) * 2 + core)
    across = (1 - group, me)
    partner = (group, me + 1 - 2 * core)

    def source(way, d):
        return chip_at(place + d) if way else chip_at(place - d)

    def column(way, which, u):
        flip = which * (5 - 2 * u) * unit
        return (5 - u) * unit - flip if way else u * unit + flip

    def region(which_chip, which_core, col, cols):
        row = pl.multiple_of((which_chip * 2 + which_core) * rows, 16)
        return weights.at[pl.ds(row, rows), pl.ds(pl.multiple_of(col, 128), cols)]

    def remote(src, dst, send, recv, device):
        return pltpu.make_async_remote_copy(
            src_ref=src, dst_ref=dst, send_sem=send, recv_sem=recv,
            device_id=device, device_id_type=MESH_ID,
        )

    def cut(way, which, piece):
        u, side_of = piece
        col = column(way, which, u)
        return (col, unit) if side_of is None else (col + side_of * half, half)

    def mark(piece):
        return 4 if piece[1] == 1 else piece[0]

    def ring(way, d, piece, hop):
        ref = region(source(way, d - 1 + hop), core, *cut(way, group, piece))
        send, recv = (ccw_send, ccw_recv) if way else (cw_send, cw_recv)
        i = mark(piece)
        return remote(ref, ref, send.at[d - 1, i], recv.at[d - 1, i], backward if way else onward)

    def yy(d, piece, way, which):
        ref = region(source(way, d), core, *cut(way, which, piece))
        i = mark(piece)
        if i == 4:
            i = 2
        j = ((d - 1) * 3 + i) * 2 + way
        return remote(ref, ref, y_send.at[j], y_recv.at[j], across)

    names = [("own",)]
    for d in range(1, reach):
        for way in range(2):
            names += [("ring", d, way, 0), ("ring", d, way, 1)]
            names += [("far", d, way, 0), ("far", d, way, 1)] if d == reach - 1 else [("both", d, way)]
    for way in range(2):
        names += [("last", way, 0, None), ("last", way, 1, None)]
        names += [("last", way, 2, 0), ("last", way, 2, 1)]
    spot_of = {name: i for i, name in enumerate(names)}

    def part(name, which_core):
        kind = name[0]
        if kind == "own":
            ref = region(chip, which_core, 0, width)
        elif kind == "ring":
            _, d, way, upper = name
            low = jnp.minimum(column(way, group, 0), column(way, group, 1))
            col = 2 * unit if upper else low
            ref = region(source(way, d), which_core, col, 2 * unit)
        elif kind == "both":
            _, d, way = name
            low = jnp.minimum(column(way, 1 - group, 0), column(way, 1 - group, 1))
            ref = region(source(way, d), which_core, low, 2 * unit)
        elif kind == "far":
            _, d, way, u = name
            ref = region(source(way, d), which_core, column(way, 1 - group, u), unit)
        else:
            _, way, u, side_of = name
            ref = region(source(way, reach), which_core, *cut(way, group, (u, side_of)))
        i = spot_of[name]
        return remote(ref, ref, part_send.at[i], part_recv.at[i], partner)

    landed = set()

    def need(*wanted):
        for name in wanted:
            if name not in landed:
                landed.add(name)
                part(name, 1 - core).wait_recv()

    own_load = pltpu.make_async_copy(wp_hbm, region(chip, core, 0, width), load_sems.at[0])
    own_load.start()
    loads = []
    for w in range(windows):
        loads.append(
            (
                pltpu.make_async_copy(qkv_hbm.at[w], qkv.at[w], load_sems.at[1 + 2 * w]),
                pltpu.make_async_copy(txt_hbm.at[w], txt.at[w], load_sems.at[2 + 2 * w]),
            )
        )
    base = 1 + 2 * windows
    side_loads = [
        pltpu.make_async_copy(wout_hbm, wout, load_sems.at[base]),
        pltpu.make_async_copy(mod_hbm, mod, load_sems.at[base + 1]),
        pltpu.make_async_copy(anchors_hbm, anchors, load_sems.at[base + 2]),
        pltpu.make_async_copy(blend_hbm, blend, load_sems.at[base + 3]),
    ]
    hid_load = pltpu.make_async_copy(hid_hbm, hid, load_sems.at[base + 4])

    barrier = pltpu.get_barrier_semaphore()
    after = [(group, (me + 1) % n), (group, (me + 2) % n)]
    expected = 4
    for device in (onward, backward, across, partner):
        pl.semaphore_signal(barrier, inc=1, device_id=device, device_id_type=MESH_ID)
    for ahead in (-2, -1, 1, 2):
        there = (me + ahead >= 0) & (me + ahead < n)

        @pl.when(there)
        def _():
            pl.semaphore_signal(
                barrier, inc=1, device_id=(group, (me + ahead + n) % n), device_id_type=MESH_ID
            )

        expected = expected + there.astype(jnp.int32)
    for copy in loads[0]:
        copy.start()
    pl.semaphore_wait(barrier, expected)

    own_load.wait()
    slots = [(1, (0, 0)), (1, (0, 1)), (1, (1, None)), (1, (2, None)), (1, (3, None))]
    slots += [(d, (u, None)) for d in range(2, reach) for u in range(4)]
    slots += [(reach, (0, None)), (reach, (1, None)), (reach, (2, 0)), (reach, (2, 1))]
    for d, piece in slots[:5]:
        ring(0, d, piece, 0).start()
        ring(1, d, piece, 0).start()
    part(("own",), core).start()
    for pair in loads[1:]:
        for copy in pair:
            copy.start()
    for copy in side_loads:
        copy.start()
    hid_load.start()

    scale = LOG2E / math.sqrt(HD)

    def attend(w, h):
        col = pl.multiple_of(h * HD, HD)
        cols = pl.ds(col, HD)
        kcols = pl.ds(pl.multiple_of(col + features, HD), HD)
        vcols = pl.ds(pl.multiple_of(col + 2 * features, HD), HD)
        q = qkv[w, :, cols]
        dims = (((1,), (1,)), ((), ()))
        st = lax.dot_general(txt[w, :, cols], q, dims, preferred_element_type=jnp.float32)
        si = lax.dot_general(qkv[w, :, kcols], q, dims, preferred_element_type=jnp.float32)
        top = jnp.maximum(jnp.max(st, axis=0, keepdims=True), jnp.max(si, axis=0, keepdims=True))
        pt = jnp.exp2((st - top) * scale)
        pi = jnp.exp2((si - top) * scale)
        total = jnp.sum(pt, axis=0, keepdims=True) + jnp.sum(pi, axis=0, keepdims=True)
        back = (((0,), (0,)), ((), ()))
        out = lax.dot_general(
            txt[w, :, kcols], pt.astype(jnp.bfloat16), back, preferred_element_type=jnp.float32
        ) + lax.dot_general(
            qkv[w, :, vcols], pi.astype(jnp.bfloat16), back, preferred_element_type=jnp.float32
        )
        att[pl.ds(col, HD), pl.ds(pl.multiple_of(w * tokens, 128), tokens)] = (
            out * (1.0 / total)
        ).astype(jnp.bfloat16)

    def spot(which_chip):
        return pl.ds(pl.multiple_of(which_chip * deep, 16), deep)

    def turn_left():
        def turned(chips_held):
            return jnp.concatenate([att[spot(c), :] for c in chips_held], axis=0).T

        left_first[...] = turned([chip, source(0, 1), source(1, 1)])
        for d in range(2, reach):
            left_mid[d - 2] = turned([source(0, d), source(1, d)])
        left_last[...] = turned([source(0, reach)])

    def right(chips_held, at):
        return jnp.concatenate([weights[spot(c), at] for c in chips_held], axis=0)

    def project_first(t):
        at = pl.ds(t * unit, unit)
        held = [chip, source(0, 1), source(1, 1)]
        acc[:, at] = jnp.dot(left_first[...], right(held, at), preferred_element_type=jnp.float32)

    def project_mid(d, t):
        at = pl.ds(t * unit, unit)
        held = [source(0, d), source(1, d)]
        term = jnp.dot(left_mid[d - 2], right(held, at), preferred_element_type=jnp.float32)
        if d == 2:
            acc[:, at] = hid[:, at].astype(jnp.float32) + mod[0:1, at] * (acc[:, at] + term)
        else:
            acc[:, at] += mod[0:1, at] * term

    def finalize(t, piece, first=False):
        at = pl.ds(t * unit + piece * half, half)
        term = jnp.dot(
            left_last[...], right([source(0, reach)], at), preferred_element_type=jnp.float32
        )
        residual = acc[:, at] + mod[0:1, at] * term
        if first:
            mean = jnp.sum(residual, axis=-1, keepdims=True) * (1.0 / half)
            centre[...] = jnp.broadcast_to(mean, centre.shape)
        lanes = centre.shape[1]
        pieces = [residual[:, i : i + lanes] - centre[...] for i in range(0, half, lanes)]
        two = functools.reduce(lambda a, b: a + b, [x * x for x in pieces])
        sum_two[...] = two if first else sum_two[...] + two
        moved = jnp.concatenate(pieces, axis=1).astype(jnp.bfloat16)
        term = lax.dot_general(
            wperm[:, at], moved, (((1,), (1,)), ((), ())), preferred_element_type=jnp.float32
        )
        term = jnp.concatenate([term[:outs] + term[outs : 2 * outs], term[2 * outs :]], axis=0)
        vel[...] = term if first else vel[...] + term

    grid_log = GRID.bit_length() - 1
    spread = hot.shape[2]
    band = spread // 3

    def parity(w):
        row_at = anchors[w : w + 1, 0:1] - me * BAND
        return row_at & 1, row_at >> 1, anchors[w : w + 1, 1:2]

    def prepare_weights():
        for copy in side_loads:
            copy.wait()
        order = lax.broadcasted_iota(jnp.int32, (outs, outs), 0)
        taken = lax.broadcasted_iota(jnp.int32, (outs, outs), 1)
        wanted = (order % C) * (PATCH * PATCH) + order // C
        permute = (taken == wanted).astype(jnp.bfloat16)
        plain = jnp.dot(permute, wout[...], preferred_element_type=jnp.float32)
        gained = plain * (1.0 + mod[1:2, :])
        high = gained.astype(jnp.bfloat16)
        wperm[:outs, :] = high
        wperm[outs : 2 * outs, :] = (gained - high.astype(jnp.float32)).astype(jnp.bfloat16)
        wperm[2 * outs :, :] = jnp.ones((wperm.shape[0] - 2 * outs, width), jnp.bfloat16)
        gain = jnp.sum(gained, axis=-1, keepdims=True)
        shift = jnp.sum(plain * mod[2:3, :], axis=-1, keepdims=True)
        feature[0] = jnp.broadcast_to(gain, feature.shape[1:])
        feature[1] = jnp.broadcast_to(shift, feature.shape[1:])
        token = lax.broadcasted_iota(jnp.int32, (WIN, tokens), 1)
        line = lax.broadcasted_iota(jnp.int32, (WIN, tokens), 0)
        for w in range(windows):
            held = blend[w].astype(jnp.float32).astype(jnp.bfloat16)
            for b in range(PATCH):
                pick = (line == PATCH * (token & (GRID - 1)) + b).astype(jnp.bfloat16)
                wide = jnp.dot(held, pick, preferred_element_type=jnp.float32)
                for a in range(PATCH):
                    mine = jnp.where(line == PATCH * (token >> grid_log) + a, wide, 0.0)
                    row = jnp.sum(mine, axis=0, keepdims=True)
                    cells[a * PATCH + b, :, w * tokens : (w + 1) * tokens] = jnp.broadcast_to(
                        row, (8, tokens)
                    )

    def prepare_hot(alpha):
        token = lax.broadcasted_iota(jnp.int32, (tokens, 128), 0)
        lane = lax.broadcasted_iota(jnp.int32, (tokens, 128), 1)
        for w in range(windows):
            odd, row_at, col_at = parity(w)
            tall = (token >> grid_log) + row_at + odd * (1 - alpha)
            for b in range(PATCH):
                wide = (PATCH * (token & (GRID - 1)) + b + col_at) & (LW - 1)
                target = tall * LW + wide - lane
                for j in range(spread // 128):
                    hot[alpha * PATCH + b, w * tokens : (w + 1) * tokens, j * 128 : (j + 1) * 128] = (
                        jnp.where(target == j * 128, 1.0, 0.0).astype(jnp.bfloat16)
                    )

    def by_parity(w, straight, swapped):
        odd = parity(w)[0]
        return jnp.where(jnp.broadcast_to(odd, straight.shape) == 0, straight, swapped)

    def prepare_totals():
        found = []
        for alpha in range(PATCH):
            total = jnp.zeros((8, spread), jnp.float32)
            for b in range(PATCH):
                held = []
                for w in range(windows):
                    at = slice(w * tokens, (w + 1) * tokens)
                    straight = cells[alpha * PATCH + b, :, at]
                    swapped = cells[(1 - alpha) * PATCH + b, :, at]
                    held.append(by_parity(w, straight, swapped))
                left = jnp.concatenate(held, axis=1).astype(jnp.bfloat16)
                total += jnp.dot(
                    left, hot[alpha * PATCH + b], preferred_element_type=jnp.float32
                )
            found.append(total)
        upper = lax.broadcasted_iota(jnp.int32, (8, spread), 0) < 4
        total = jnp.where(upper, found[0], found[1])
        for i in range(3):
            totals[i] = total[:, i * band : (i + 1) * band]

    halos = (
        (1, remote(totals.at[1], total_near, halo_send.at[0], halo_recv.at[0], after[0])),
        (2, remote(totals.at[2], total_far, halo_send.at[1], halo_recv.at[1], after[1])),
        (1, remote(near_out, near_in, halo_send.at[2], halo_recv.at[2], after[0])),
        (2, remote(far_out, far_in, halo_send.at[3], halo_recv.at[3], after[1])),
    )

    def send_halo(i):
        ahead, copy = halos[i]

        @pl.when(me + ahead < n)
        def _():
            copy.start()

    def take_halo(i):
        ahead, copy = halos[i]

        @pl.when(me >= ahead)
        def _():
            copy.wait_recv()

    def close_halo(i):
        ahead, copy = halos[i]

        @pl.when(me + ahead < n)
        def _():
            copy.wait_send()

    def clear_halos():
        @pl.when(me < 1)
        def _():
            total_near[...] = jnp.zeros_like(total_near)
            near_in[...] = jnp.zeros_like(near_in)

        @pl.when(me < 2)
        def _():
            total_far[...] = jnp.zeros_like(total_far)
            far_in[...] = jnp.zeros_like(far_in)

    def send_totals():
        send_halo(0)
        send_halo(1)

    def close_totals():
        take_halo(0)
        take_halo(1)
        summed = totals[0] + total_near[...] + total_far[...]
        totals[0] = 1.0 / jnp.maximum(summed, 1.0)

    across_order = [(1, (0, 0), 0), (1, (0, 0), 1), (1, (0, 1), 0), (1, (0, 1), 1)]
    across_order += [
        (d, (u, None), way)
        for d in range(1, reach)
        for u in range(2)
        for way in range(2)
        if (d, u) != (1, 0)
    ]

    def serve(d, piece):
        u, side_of = piece
        for way in range(2):
            ring(way, d, piece, 1).wait_recv()
            if d == 1 and u == 0:
                if side_of == 1:
                    ring(way, 2, (0, None), 0).start()
            elif d + 1 < reach or (d + 1 == reach and u < 2):
                ring(way, d + 1, piece, 0).start()
            elif d + 1 == reach and u == 2:
                ring(way, reach, (2, 0), 0).start()
                ring(way, reach, (2, 1), 0).start()
            if d < reach and u < 2:
                yy(d, piece, way, group).start()
        for way in range(2):
            if d < reach and u % 2 == 1:
                part(("ring", d, way, u // 2), core).start()
            elif d == reach:
                part(("last", way, u, side_of), core).start()

    def serve_across(j):
        d, (u, side_of), way = across_order[j]
        yy(d, (u, side_of), way, 1 - group).wait_recv()
        if d == reach - 1:
            part(("far", d, way, u), core).start()
        elif u == 1:
            part(("both", d, way), core).start()

    units = [(w, h) for w in range(windows) for h in range(HEADS)]
    ready = set()

    def attend_some(count):
        for _ in range(min(count, len(units))):
            w, h = units.pop(0)
            if w not in ready:
                for copy in loads[w]:
                    copy.wait()
                ready.add(w)
            attend(w, h)

    def first_ones(which):
        need(("own",))
        for way in range(2):
            need(("ring", 1, way, 0), ("ring", 1, way, 1), ("both", 1, way))
        for t in which:
            project_first(t)

    def mid_ones(d, which):
        for way in range(2):
            need(("ring", d, way, 0), ("ring", d, way, 1))
            if d < reach - 1:
                need(("both", d, way))
        for t in which:
            project_mid(d, t)

    last = reach - 1

    def third(which, *kinds):
        for way in range(2):
            need(*[(kind[0], last, way) + kind[1:] for kind in kinds])
        for t in which:
            project_mid(last, t)

    def end(which, pieces, u, side_of, first=False):
        for way in range(2):
            need(("last", way, u, side_of))
        for t in which:
            for piece in pieces:
                finalize(t, piece, first and t == which[0] and piece == pieces[0])

    across_done = [0]

    def take_across(count):
        for _ in range(count):
            serve_across(across_done[0])
            across_done[0] += 1

    def some(fn, *args, **kwargs):
        return functools.partial(fn, *args, **kwargs)

    def begun():
        hid_load.wait()
        close_totals()

    count = len(units)
    plan = {
        0: [some(attend_some, count // 3)],
        1: [some(attend_some, count // 12)],
        2: [some(attend_some, count // 5 + 1)],
        3: [some(attend_some, count // 5 + 1)],
        4: [some(attend_some, count)],
        5: [turn_left, prepare_weights, clear_halos],
        6: [some(prepare_hot, 0), some(prepare_hot, 1)],
        7: [prepare_totals, send_totals],
        8: [some(first_ones, range(3))],
        9: [some(first_ones, range(3, 6))],
        10: [begun],
    }
    across_after = {4: 4}
    for d in range(2, reach):
        for u in range(4):
            across_after[4 * d + u - 3] = 1
    tail = len(slots) - 4
    for d in range(2, last):
        at = 4 * d + 3
        plan.setdefault(at, []).append(some(mid_ones, d, range(3)))
        plan.setdefault(at + 1, []).append(some(mid_ones, d, range(3, 6)))
    for i, (d, piece) in enumerate(slots[:tail]):
        for step in plan.get(i, []):
            step()
        serve(d, piece)
        take_across(across_after.get(i, 0))
    third((2, 3), ("ring", 1))
    serve(*slots[tail])
    take_across(1)
    third((0, 5), ("ring", 0), ("far", 0))
    end((0,), range(2), 0, None, first=True)
    take_across(1)
    end((5,), range(2), 0, None)
    serve(*slots[tail + 1])
    serve(*slots[tail + 2])
    third((1, 4), ("far", 1))
    end((1,), range(2), 1, None)
    serve(*slots[tail + 3])
    end((4,), range(2), 1, None)
    end((2, 3), (0,), 2, 0)
    end((2, 3), (1,), 2, 1)

    flat_one = vel[outs : outs + 1, :] * (1.0 / width)
    flat_two = jnp.sum(sum_two[...].T, axis=0, keepdims=True) * (1.0 / width)
    rate = lax.rsqrt(flat_two - flat_one * flat_one + 1e-06)
    gain = jnp.concatenate([feature[0]] * (windows * tokens // 128), axis=1)
    shift = jnp.concatenate([feature[1]] * (windows * tokens // 128), axis=1)
    value = rate * (vel[:outs, :] - flat_one * gain) + shift
    weighted = []
    for q in range(PATCH * PATCH):
        cell = jnp.concatenate([cells[q]] * (C // 8), axis=0)
        weighted.append(value[q * C : (q + 1) * C] * cell)
    chosen = []
    for alpha in range(PATCH):
        for b in range(PATCH):
            held = []
            for w in range(windows):
                at = slice(w * tokens, (w + 1) * tokens)
                straight = weighted[alpha * PATCH + b][:, at]
                swapped = weighted[(1 - alpha) * PATCH + b][:, at]
                held.append(by_parity(w, straight, swapped))
            both = jnp.concatenate(held, axis=1)
            high = both.astype(jnp.bfloat16)
            low = (both - high.astype(jnp.float32)).astype(jnp.bfloat16)
            chosen.append(jnp.concatenate([high, low], axis=0))

    def placed(alpha, which):
        total = jnp.zeros((2 * C, band), jnp.float32)
        for b in range(PATCH):
            total += jnp.dot(
                chosen[alpha * PATCH + b],
                hot[alpha * PATCH + b, :, which * band : (which + 1) * band],
                preferred_element_type=jnp.float32,
            )
        return total[:C] + total[C:]

    for which, ref, halo in ((2, far_out, 3), (1, near_out, 2)):
        for alpha in range(PATCH):
            ref[alpha * C : (alpha + 1) * C, :] = placed(alpha, which)
        send_halo(halo)
    own = [placed(alpha, 0) for alpha in range(PATCH)]
    inverse = totals[0]
    for d, piece in slots:
        for way in range(2):
            ring(way, d, piece, 0).wait_send()
    for d, piece, way in across_order:
        yy(d, piece, way, group).wait_send()
    for name in names:
        part(name, core).wait_send()
    take_halo(2)
    take_halo(3)
    for alpha in range(PATCH):
        at = slice(alpha * C, (alpha + 1) * C)
        summed = (own[alpha] + near_in[at, :] + far_in[at, :]) * inverse[4 * alpha : 4 * alpha + 1, :]
        for i in range(band // LW):
            out_ref[pl.ds(PATCH * i + alpha, C, stride=BAND), :] = summed[:, i * LW : (i + 1) * LW]

    for i in range(len(halos)):
        close_halo(i)


def shards(n, img_qkv, txt_kv, hidden, w_proj, w_out, modulation, anchors, blend_weight):
    windows, tokens, qkv_width = img_qkv.shape
    rows, width = w_proj.shape
    total = windows * tokens
    reach = n // 4
    deep = 2 * rows
    outs = w_out.shape[1]
    spread = (BAND + WIN) // PATCH * LW
    band = spread // 3
    any_space = pl.BlockSpec(memory_space=pl.ANY)
    vmem = pl.BlockSpec(memory_space=pltpu.VMEM)
    dma = pltpu.SemaphoreType.DMA
    f32, bf16 = jnp.float32, jnp.bfloat16
    parts = 1 + 6 * (reach - 2) + 8 + 8
    velocity = pl.pallas_call(
        functools.partial(block_kernel, n),
        out_shape=jax.ShapeDtypeStruct((C * BAND, LW), f32),
        in_specs=[any_space] * 8,
        out_specs=vmem,
        scratch_shapes=[
            pltpu.VMEM(img_qkv.shape, bf16),
            pltpu.VMEM(txt_kv.shape, bf16),
            pltpu.VMEM((total, width), bf16),
            pltpu.VMEM((n * rows, width), bf16),
            pltpu.VMEM((n * rows, total), bf16),
            pltpu.VMEM((total, 3 * deep), bf16),
            pltpu.VMEM((reach - 2, total, 2 * deep), bf16),
            pltpu.VMEM((total, deep), bf16),
            pltpu.VMEM((total, width), f32),
            pltpu.VMEM((outs, width), bf16),
            pltpu.VMEM((2 * outs + 16, width), bf16),
            pltpu.VMEM(modulation.shape, f32),
            pltpu.VMEM(anchors.shape, jnp.int32),
            pltpu.VMEM(blend_weight.shape, jnp.int32),
            pltpu.VMEM((PATCH * PATCH, 8, total), f32),
            pltpu.VMEM((PATCH * PATCH, total, spread), bf16),
            pltpu.VMEM((3, 8, band), f32),
            pltpu.VMEM((8, band), f32),
            pltpu.VMEM((8, band), f32),
            pltpu.VMEM((total, 128), f32),
            pltpu.VMEM((total, 128), f32),
            pltpu.VMEM((outs + 16, total), f32),
            pltpu.VMEM((2, outs, 128), f32),
            pltpu.VMEM((PATCH * C, band), f32),
            pltpu.VMEM((PATCH * C, band), f32),
            pltpu.VMEM((PATCH * C, band), f32),
            pltpu.VMEM((PATCH * C, band), f32),
            dma((6 + 2 * windows,)),
            dma((reach, 5)),
            dma((reach, 5)),
            dma((reach, 5)),
            dma((reach, 5)),
            dma((6 * (reach - 1),)),
            dma((6 * (reach - 1),)),
            dma((parts,)),
            dma((parts,)),
            dma((4,)),
            dma((4,)),
        ],
        compiler_params=pltpu.CompilerParams(
            collective_id=0, has_side_effects=True, vmem_limit_bytes=60 * 1024 * 1024
        ),
    )(
        img_qkv,
        txt_kv,
        hidden.reshape(total, width),
        w_proj,
        w_out.T,
        modulation,
        anchors,
        blend_weight,
    )
    return velocity.reshape(C, BAND, LW)


def solution(mesh):
    in_specs = (
        P(("group", "win"), None, None),
        P(("group", "win"), None, None),
        P(("group", "win"), None, None),
        P("win", None),
        P(),
        P("group", None),
        P(("group", "win"), None),
        P(("group", "win"), None, None),
    )
    out_specs = P(None, ("group", "win"), None)
    n = mesh.shape["win"]

    def body(*args):
        rows, width = args[3].shape
        ringed = (
            mesh.shape["group"] == 2
            and n % 4 == 0
            and n >= 16
            and rows % 16 == 0
            and width % 1536 == 0
        )
        if ringed:
            return shards(n, *args)
        return plain_shards(*args)

    return jax.shard_map(body, mesh=mesh, in_specs=in_specs, out_specs=out_specs, check_vma=False)
```

```python
import functools
import math

import jax
import jax.numpy as jnp
from jax import lax
from jax.experimental import pallas as pl
from jax.experimental.pallas import tpu as pltpu
from jax.sharding import PartitionSpec as P

HD = 128
C = 16
HEADS = 12
PATCH = 2
WIN = 32
LW = 64
BAND = 16
GRID = 16


def shifted(block, axis, distance):
    devices = range(lax.axis_size(axis))
    route = [(i - distance, i) for i in devices if i - distance in devices]
    return lax.ppermute(block, axis, route)


def place_window(canvas, totals, contrib, weights, row_at, col_at):
    zero_index = jnp.zeros((), jnp.int32)
    region = lax.dynamic_slice(canvas, (zero_index, row_at, col_at), (C, WIN, WIN))
    canvas = lax.dynamic_update_slice(canvas, region + contrib, (zero_index, row_at, col_at))
    weight_region = lax.dynamic_slice(totals, (row_at, col_at), (WIN, WIN))
    totals = lax.dynamic_update_slice(totals, weight_region + weights, (row_at, col_at))
    return (canvas, totals)


def fold_columns(field):
    span_cols = field.shape[-1] - WIN
    leading = field[..., :span_cols]
    wrapped = field[..., span_cols:]
    padding = [(0, 0)] * (field.ndim - 1) + [(0, span_cols - WIN)]
    return leading + jnp.pad(wrapped, padding)


def plain_shards(img_qkv, txt_kv, hidden, w_proj, w_out, modulation, anchors, blend_weight):
    window_count, tokens, _ = img_qkv.shape
    features = HEADS * HD
    queries = img_qkv[:, :, :features].reshape(window_count, tokens, HEADS, HD)
    all_keys = jnp.concatenate(
        [txt_kv[:, :, :features], img_qkv[:, :, features : 2 * features]], axis=1
    )
    all_keys = all_keys.reshape(window_count, -1, HEADS, HD)
    all_values = jnp.concatenate([txt_kv[:, :, features:], img_qkv[:, :, 2 * features :]], axis=1)
    all_values = all_values.reshape(window_count, -1, HEADS, HD)
    scores = jnp.einsum(
        "wqhd,wkhd->whqk", queries, all_keys, preferred_element_type=jnp.float32
    ) / math.sqrt(HD)
    scores = scores - jnp.max(scores, axis=-1, keepdims=True)
    exp_scores = jnp.exp(scores)
    soft_weights = (exp_scores / jnp.sum(exp_scores, axis=-1, keepdims=True)).astype(jnp.bfloat16)
    attended = jnp.einsum(
        "whqk,wkhd->wqhd", soft_weights, all_values, preferred_element_type=jnp.float32
    )
    attended = attended.reshape(window_count * tokens, features).astype(jnp.bfloat16)
    whole_proj = lax.all_gather(w_proj, "win", axis=0, tiled=True)
    projected = jnp.dot(attended, whole_proj, preferred_element_type=jnp.float32)
    residual = (
        hidden.reshape(window_count * tokens, -1).astype(jnp.float32) + modulation[0] * projected
    )
    row_mean = jnp.mean(residual, axis=-1, keepdims=True)
    centred = residual - row_mean
    row_var = jnp.mean(centred * centred, axis=-1, keepdims=True)
    normed = centred * lax.rsqrt(row_var + 1e-06)
    modulated = (normed * (1.0 + modulation[1]) + modulation[2]).astype(jnp.bfloat16)
    patch_vel = jnp.dot(modulated, w_out, preferred_element_type=jnp.float32)
    patch_grid = patch_vel.reshape(window_count, GRID, GRID, C, PATCH, PATCH)
    window_vel = patch_grid.transpose(0, 3, 1, 4, 2, 5).reshape(window_count, C, WIN, WIN)
    weights = blend_weight.astype(jnp.float32)
    contrib = window_vel * weights[:, None]
    band_start = lax.axis_index("win") * BAND
    canvas = jnp.zeros((C, BAND + WIN, LW + WIN), jnp.float32)
    totals = jnp.zeros((BAND + WIN, LW + WIN), jnp.float32)

    def add_one(window, running):
        row_at = anchors[window, 0] - band_start
        col_at = anchors[window, 1]
        return place_window(
            running[0], running[1], contrib[window], weights[window], row_at, col_at
        )

    canvas, totals = lax.fori_loop(0, window_count, add_one, (canvas, totals))
    canvas = fold_columns(canvas)
    totals = fold_columns(totals)
    own_canvas = canvas[:, :BAND]
    own_totals = totals[:BAND]
    near_canvas = canvas[:, BAND : 2 * BAND]
    near_totals = totals[BAND : 2 * BAND]
    far_canvas = canvas[:, 2 * BAND :]
    far_totals = totals[2 * BAND :]
    prev_canvas, prev_totals = shifted((near_canvas, near_totals), "win", 1)
    second_canvas, second_totals = shifted((far_canvas, far_totals), "win", 2)
    sum_canvas = own_canvas + prev_canvas + second_canvas
    sum_totals = own_totals + prev_totals + second_totals
    return sum_canvas / jnp.maximum(sum_totals, 1.0)[None]


LOG2E = 1.4426950408889634
MESH_ID = pl.DeviceIdType.MESH


def block_kernel(
    n,
    qkv_hbm,
    txt_hbm,
    hid_hbm,
    wp_hbm,
    wout_hbm,
    mod_hbm,
    anchors_hbm,
    blend_hbm,
    out_ref,
    qkv,
    txt,
    hid,
    weights,
    att,
    left_first,
    left_mid,
    left_last,
    acc,
    wout,
    wperm,
    mod,
    anchors,
    blend,
    cells,
    hot,
    totals,
    total_near,
    total_far,
    sum_two,
    centre,
    vel,
    feature,
    near_out,
    far_out,
    near_in,
    far_in,
    load_sems,
    sent,
    ring_recv,
    y_recv,
    part_recv,
    halo_send,
    halo_recv,
):
    windows, tokens, _ = qkv.shape
    rows = wp_hbm.shape[0]
    width = weights.shape[1]
    features = HEADS * HD
    deep = 2 * rows
    unit = width // 6
    half = unit // 2
    outs = wout.shape[0]
    chips = n // 2
    reach = chips // 2
    group = lax.axis_index("group")
    me = lax.axis_index("win")
    core = me % 2
    chip = me // 2
    depth, side = chip // 2, chip % 2
    place = depth + side * (chips - 1 - 2 * depth)

    def chip_at(position):
        spot = (position + chips) % chips
        turn = spot // reach
        return 2 * (spot + turn * (chips - 1 - 2 * spot)) + turn

    onward = (group, chip_at(place + 1) * 2 + core)
    backward = (group, chip_at(place - 1) * 2 + core)
    across = (1 - group, me)
    partner = (group, me + 1 - 2 * core)

    def source(way, d):
        return chip_at(place + d) if way else chip_at(place - d)

    def column(way, which, u):
        flip = which * (5 - 2 * u) * unit
        return (5 - u) * unit - flip if way else u * unit + flip

    def region(which_chip, which_core, col, cols):
        row = pl.multiple_of((which_chip * 2 + which_core) * rows, 16)
        return weights.at[pl.ds(row, rows), pl.ds(pl.multiple_of(col, 128), cols)]

    def remote(src, dst, send, recv, device):
        return pltpu.make_async_remote_copy(
            src_ref=src, dst_ref=dst, send_sem=send, recv_sem=recv,
            device_id=device, device_id_type=MESH_ID,
        )

    def cut(way, which, piece):
        u, side_of = piece
        col = column(way, which, u)
        if side_of is None:
            return col, unit
        return col + (way if side_of == 2 else side_of) * half, half

    pair = (2, 2)

    whole = [(u, None) for u in range(4)]
    closing = [pair, (0, None), (1, 0), (1, 1)]
    slots = [(1, (0, 0)), (1, (0, 1)), (1, (1, None)), (1, (2, None)), (1, (3, None))]
    slots += [(d, piece) for d in range(2, reach) for piece in whole]
    slots += [(reach, piece) for piece in closing]
    last = reach - 1
    across_groups = [[(1, (0, side_of), way) for side_of in range(2) for way in range(2)]]
    across_groups += [
        [(d, piece, way) for way in range(2)]
        for d in range(1, last)
        for piece in whole[:2]
        if (d, piece[0]) != (1, 0)
    ]
    across_groups += [[(last, piece, way)] for piece in whole[:2] for way in range(2)]
    across_groups += [[(reach, pair, way)] for way in range(2)]
    across_of = {copy: i for i, group_of in enumerate(across_groups) for copy in group_of}

    def block_of(d, pieces, crossed, ways=(0, 1)):
        found = [("ring", d, way, piece) for way in ways for piece in pieces]
        return found + [("far", d, way, piece) for way in ways for piece in crossed]

    part_groups = {"own": [("own",)], "first": block_of(1, whole, whole[:2])}
    for d in range(2, last):
        for u in range(2):
            part_groups["mid", d, u] = block_of(d, whole[u : u + 1], whole[u : u + 1])
        part_groups["mid", d, 2] = block_of(d, whole[2:], [])
    part_groups["inner"] = block_of(last, whole[2:], [])
    for u in range(2):
        for way in range(2):
            part_groups["outer", u, way] = [
                ("ring", last, 1 - way, whole[u]),
                ("far", last, way, whole[u]),
            ]
    part_groups["pair"] = block_of(reach, [pair], [])
    part_groups["end"] = block_of(reach, [(0, None)], [])
    for side_of in range(2):
        part_groups["close", side_of] = block_of(reach, [(1, side_of)], []) + [
            ("far", reach, side_of, pair)
        ]
    part_of = {name: i for i, held in enumerate(part_groups.values()) for name in held}

    def ring(way, d, piece, hop):
        ref = region(source(way, d - 1 + hop), core, *cut(way, group, piece))
        arrived = ring_recv.at[slots.index((d, piece))]
        return remote(ref, ref, sent.at[0], arrived, backward if way else onward)

    def yy(d, piece, way, which):
        ref = region(source(way, d), core, *cut(way, which, piece))
        return remote(ref, ref, sent.at[0], y_recv.at[across_of[d, piece, way]], across)

    def part(name):
        if name[0] == "own":
            ref = region(chip, core, 0, width)
        else:
            kind, d, way, piece = name
            which = group if kind == "ring" else 1 - group
            ref = region(source(way, d), core, *cut(way, which, piece))
        return remote(ref, ref, sent.at[0], part_recv.at[part_of[name]], partner)

    def arrived(sem, halves):
        if halves % 2:
            ref = weights.at[pl.ds(0, halves * rows), pl.ds(0, half)]
        else:
            ref = weights.at[pl.ds(0, halves // 2 * rows), pl.ds(0, unit)]
        pltpu.make_async_copy(ref, ref, sem).wait()

    def size_of(piece):
        return 2 if piece[1] is None else 1

    landed = set()

    def need(name):
        if name not in landed:
            landed.add(name)
            held = part_groups[name]
            sizes = [12 if one[0] == "own" else size_of(one[3]) for one in held]
            arrived(part_recv.at[part_of[held[0]]], sum(sizes))

    own_load = pltpu.make_async_copy(wp_hbm, region(chip, core, 0, width), load_sems.at[0])
    own_load.start()
    loads = []
    for w in range(windows):
        loads.append(
            (
                pltpu.make_async_copy(qkv_hbm.at[w], qkv.at[w], load_sems.at[1 + 2 * w]),
                pltpu.make_async_copy(txt_hbm.at[w], txt.at[w], load_sems.at[2 + 2 * w]),
            )
        )
    base = 1 + 2 * windows
    side_loads = [
        pltpu.make_async_copy(wout_hbm, wout, load_sems.at[base]),
        pltpu.make_async_copy(mod_hbm, mod, load_sems.at[base + 1]),
        pltpu.make_async_copy(anchors_hbm, anchors, load_sems.at[base + 2]),
        pltpu.make_async_copy(blend_hbm, blend, load_sems.at[base + 3]),
    ]
    hid_load = pltpu.make_async_copy(hid_hbm, hid, load_sems.at[base + 4])

    barrier = pltpu.get_barrier_semaphore()
    after = [(group, (me + 1) % n), (group, (me + 2) % n)]
    expected = 4
    for device in (onward, backward, across, partner):
        pl.semaphore_signal(barrier, inc=1, device_id=device, device_id_type=MESH_ID)
    for ahead in (-2, -1, 1, 2):
        there = (me + ahead >= 0) & (me + ahead < n)

        @pl.when(there)
        def _():
            pl.semaphore_signal(
                barrier, inc=1, device_id=(group, (me + ahead + n) % n), device_id_type=MESH_ID
            )

        expected = expected + there.astype(jnp.int32)
    for copy in loads[0]:
        copy.start()
    pl.semaphore_wait(barrier, expected)

    own_load.wait()
    for d, piece in slots[:5]:
        ring(0, d, piece, 0).start()
        ring(1, d, piece, 0).start()
    part(("own",)).start()
    for both in loads[1:]:
        for copy in both:
            copy.start()
    for copy in side_loads:
        copy.start()
    hid_load.start()

    scale = LOG2E / math.sqrt(HD)

    def attend(w, h):
        col = pl.multiple_of(h * HD, HD)
        cols = pl.ds(col, HD)
        kcols = pl.ds(pl.multiple_of(col + features, HD), HD)
        vcols = pl.ds(pl.multiple_of(col + 2 * features, HD), HD)
        q = qkv[w, :, cols]
        dims = (((1,), (1,)), ((), ()))
        st = lax.dot_general(txt[w, :, cols], q, dims, preferred_element_type=jnp.float32)
        si = lax.dot_general(qkv[w, :, kcols], q, dims, preferred_element_type=jnp.float32)
        top = jnp.maximum(jnp.max(st, axis=0, keepdims=True), jnp.max(si, axis=0, keepdims=True))
        pt = jnp.exp2((st - top) * scale)
        pi = jnp.exp2((si - top) * scale)
        total = jnp.sum(pt, axis=0, keepdims=True) + jnp.sum(pi, axis=0, keepdims=True)
        back = (((0,), (0,)), ((), ()))
        out = lax.dot_general(
            txt[w, :, kcols], pt.astype(jnp.bfloat16), back, preferred_element_type=jnp.float32
        ) + lax.dot_general(
            qkv[w, :, vcols], pi.astype(jnp.bfloat16), back, preferred_element_type=jnp.float32
        )
        att[pl.ds(col, HD), pl.ds(pl.multiple_of(w * tokens, 128), tokens)] = (
            out * (1.0 / total)
        ).astype(jnp.bfloat16)

    def spot(which_chip):
        return pl.ds(pl.multiple_of(which_chip * deep, 16), deep)

    def turn_left():
        def turned(chips_held):
            return jnp.concatenate([att[spot(c), :] for c in chips_held], axis=0).T

        left_first[...] = turned([chip, source(0, 1), source(1, 1)])
        for d in range(2, reach):
            left_mid[d - 2] = turned([source(0, d), source(1, d)])
        left_last[...] = turned([source(0, reach)])

    def right(chips_held, at):
        return jnp.concatenate([weights[spot(c), at] for c in chips_held], axis=0)

    def project_first(t):
        at = pl.ds(t * unit, unit)
        held = [chip, source(0, 1), source(1, 1)]
        acc[:, at] = jnp.dot(left_first[...], right(held, at), preferred_element_type=jnp.float32)

    def project_mid(d, col):
        at = pl.ds(pl.multiple_of(col, 128), unit)
        held = [source(0, d), source(1, d)]
        term = jnp.dot(left_mid[d - 2], right(held, at), preferred_element_type=jnp.float32)
        if d == 2:
            acc[:, at] = hid[:, at].astype(jnp.float32) + mod[0:1, at] * (acc[:, at] + term)
        else:
            acc[:, at] += mod[0:1, at] * term

    def finalize(col, first=False):
        at = pl.ds(pl.multiple_of(col, 128), half)
        term = jnp.dot(
            left_last[...], right([source(0, reach)], at), preferred_element_type=jnp.float32
        )
        residual = acc[:, at] + mod[0:1, at] * term
        if first:
            mean = jnp.sum(residual, axis=-1, keepdims=True) * (1.0 / half)
            centre[...] = jnp.broadcast_to(mean, centre.shape)
        lanes = centre.shape[1]
        pieces = [residual[:, i : i + lanes] - centre[...] for i in range(0, half, lanes)]
        two = functools.reduce(lambda a, b: a + b, [x * x for x in pieces])
        sum_two[...] = two if first else sum_two[...] + two
        moved = jnp.concatenate(pieces, axis=1).astype(jnp.bfloat16)
        term = lax.dot_general(
            wperm[:, at], moved, (((1,), (1,)), ((), ())), preferred_element_type=jnp.float32
        )
        term = jnp.concatenate([term[:outs] + term[outs : 2 * outs], term[2 * outs :]], axis=0)
        vel[...] = term if first else vel[...] + term

    grid_log = GRID.bit_length() - 1
    spread = hot.shape[2]
    band = spread // 3
    quarters = band // 128

    def parity(w):
        row_at = anchors[w : w + 1, 0:1] - me * BAND
        return row_at & 1, row_at >> 1, anchors[w : w + 1, 1:2]

    def prepare_weights():
        for copy in side_loads:
            copy.wait()
        order = lax.broadcasted_iota(jnp.int32, (outs, outs), 0)
        taken = lax.broadcasted_iota(jnp.int32, (outs, outs), 1)
        wanted = (order % C) * (PATCH * PATCH) + order // C
        permute = (taken == wanted).astype(jnp.bfloat16)
        plain = jnp.dot(permute, wout[...], preferred_element_type=jnp.float32)
        gained = plain * (1.0 + mod[1:2, :])
        high = gained.astype(jnp.bfloat16)
        wperm[:outs, :] = high
        wperm[outs : 2 * outs, :] = (gained - high.astype(jnp.float32)).astype(jnp.bfloat16)
        wperm[2 * outs :, :] = jnp.ones((wperm.shape[0] - 2 * outs, width), jnp.bfloat16)
        gain = jnp.sum(gained, axis=-1, keepdims=True)
        shift = jnp.sum(plain * mod[2:3, :], axis=-1, keepdims=True)
        feature[0] = jnp.broadcast_to(gain, feature.shape[1:])
        feature[1] = jnp.broadcast_to(shift, feature.shape[1:])
        token = lax.broadcasted_iota(jnp.int32, (WIN, tokens), 1)
        line = lax.broadcasted_iota(jnp.int32, (WIN, tokens), 0)
        for w in range(windows):
            held = blend[w].astype(jnp.float32).astype(jnp.bfloat16)
            for b in range(PATCH):
                pick = (line == PATCH * (token & (GRID - 1)) + b).astype(jnp.bfloat16)
                wide = jnp.dot(held, pick, preferred_element_type=jnp.float32)
                for a in range(PATCH):
                    mine = jnp.where(line == PATCH * (token >> grid_log) + a, wide, 0.0)
                    row = jnp.sum(mine, axis=0, keepdims=True)
                    cells[a * PATCH + b, :, w * tokens : (w + 1) * tokens] = jnp.broadcast_to(
                        row, (8, tokens)
                    )

    def prepare_hot(alpha):
        token = lax.broadcasted_iota(jnp.int32, (tokens, 128), 0)
        lane = lax.broadcasted_iota(jnp.int32, (tokens, 128), 1)
        for w in range(windows):
            odd, row_at, col_at = parity(w)
            tall = (token >> grid_log) + row_at + odd * (1 - alpha)
            for b in range(PATCH):
                wide = (PATCH * (token & (GRID - 1)) + b + col_at) & (LW - 1)
                target = tall * LW + wide - lane
                for j in range(spread // 128):
                    hot[alpha * PATCH + b, w * tokens : (w + 1) * tokens, j * 128 : (j + 1) * 128] = (
                        jnp.where(target == j * 128, 1.0, 0.0).astype(jnp.bfloat16)
                    )

    def by_parity(w, straight, swapped):
        odd = parity(w)[0]
        return jnp.where(jnp.broadcast_to(odd, straight.shape) == 0, straight, swapped)

    def prepare_totals():
        found = []
        for alpha in range(PATCH):
            total = jnp.zeros((8, spread), jnp.float32)
            for b in range(PATCH):
                held = []
                for w in range(windows):
                    at = slice(w * tokens, (w + 1) * tokens)
                    straight = cells[alpha * PATCH + b, :, at]
                    swapped = cells[(1 - alpha) * PATCH + b, :, at]
                    held.append(by_parity(w, straight, swapped))
                left = jnp.concatenate(held, axis=1).astype(jnp.bfloat16)
                total += jnp.dot(
                    left, hot[alpha * PATCH + b], preferred_element_type=jnp.float32
                )
            found.append(total)
        line = lax.broadcasted_iota(jnp.int32, (8, 128), 0)
        for i in range(3):
            total = jnp.zeros((8, 128), jnp.float32)
            for alpha in range(PATCH):
                for q in range(quarters):
                    at = i * band + q * 128
                    mine = found[alpha][:, at : at + 128]
                    total = jnp.where(line == alpha * quarters + q, mine, total)
            totals[i] = total

    halos = (
        (1, remote(totals.at[1], total_near, halo_send.at[0], halo_recv.at[0], after[0])),
        (2, remote(totals.at[2], total_far, halo_send.at[1], halo_recv.at[1], after[1])),
        (1, remote(near_out, near_in, halo_send.at[2], halo_recv.at[2], after[0])),
        (2, remote(far_out, far_in, halo_send.at[3], halo_recv.at[3], after[1])),
    )

    def send_halo(i):
        ahead, copy = halos[i]

        @pl.when(me + ahead < n)
        def _():
            copy.start()

    def take_halo(i):
        ahead, copy = halos[i]

        @pl.when(me >= ahead)
        def _():
            copy.wait_recv()

    def close_halo(i):
        ahead, copy = halos[i]

        @pl.when(me + ahead < n)
        def _():
            copy.wait_send()

    def clear_halos():
        @pl.when(me < 1)
        def _():
            total_near[...] = jnp.zeros_like(total_near)
            near_in[...] = jnp.zeros_like(near_in)

        @pl.when(me < 2)
        def _():
            total_far[...] = jnp.zeros_like(total_far)
            far_in[...] = jnp.zeros_like(far_in)

    def send_totals():
        send_halo(0)
        send_halo(1)

    def close_totals():
        take_halo(0)
        take_halo(1)
        summed = totals[0] + total_near[...] + total_far[...]
        totals[0] = 1.0 / jnp.maximum(summed, 1.0)

    def hand(kind, d, way, piece):
        if (d, piece[0]) == (1, 0):
            if piece[1] == 0:
                return
            piece = (0, None)
        part((kind, d, way, piece)).start()

    def serve(d, piece):
        u, side_of = piece
        arrived(ring_recv.at[slots.index((d, piece))], 2 * size_of(piece))
        for way in range(2):
            if d + 1 < reach:
                if side_of is None:
                    ring(way, d + 1, piece, 0).start()
                elif side_of == 1:
                    ring(way, d + 1, (0, None), 0).start()
            elif d + 1 == reach and u == 2:
                for later in closing:
                    ring(way, reach, later, 0).start()
            if (d < reach and u < 2) or piece == pair:
                yy(d, piece, way, group).start()
        for way in range(2):
            hand("ring", d, way, piece)

    def serve_across(j):
        held = across_groups[j]
        arrived(y_recv.at[j], sum(size_of(piece) for _, piece, _ in held))
        for d, piece, way in held:
            hand("far", d, way, piece)

    units = [(w, h) for w in range(windows) for h in range(HEADS)]
    ready = set()

    def attend_some(count):
        for _ in range(min(count, len(units))):
            w, h = units.pop(0)
            if w not in ready:
                for copy in loads[w]:
                    copy.wait()
                ready.add(w)
            attend(w, h)

    def first_ones(which):
        need("own")
        need("first")
        for t in which:
            project_first(t)

    def mid_ones(d, u):
        need(("mid", d, u))
        for t in (u, 5 - u):
            project_mid(d, t * unit)

    def third_inner():
        need("inner")
        for t in (2, 3):
            project_mid(last, t * unit)

    def third_outer(u, way):
        need(("outer", u, way))
        project_mid(last, column(way, 1 - group, u))

    def end_pair():
        need("pair")
        for way in range(2):
            finalize(cut(way, group, pair)[0], first=way == 0)

    def end(cols):
        need("end")
        for col in cols:
            finalize(col)

    def close(side_of):
        need(("close", side_of))
        for col in (unit, 4 * unit):
            finalize(col + side_of * half)
        finalize(cut(side_of, 1 - group, pair)[0])

    across_done = [0]

    def take_across(count):
        for _ in range(count):
            serve_across(across_done[0])
            across_done[0] += 1

    def some(fn, *args, **kwargs):
        return functools.partial(fn, *args, **kwargs)

    count = len(units)
    plan = {
        0: [some(attend_some, count // 3 - 1)],
        1: [some(attend_some, count // 12)],
        2: [some(attend_some, count // 5 + 1)],
        3: [some(attend_some, count // 5 + 1)],
        4: [some(attend_some, count // 5 + 1)],
        5: [some(attend_some, count), turn_left, prepare_weights, clear_halos],
        6: [some(prepare_hot, 0), some(prepare_hot, 1)],
        7: [prepare_totals, send_totals],
        8: [some(first_ones, range(3))],
        9: [some(first_ones, range(3, 6))],
        10: [hid_load.wait],
    }
    across_after = {4: 1, 6: 1}
    for d in range(2, last):
        plan.setdefault(4 * d + 2, []).extend([some(mid_ones, d, 2), some(mid_ones, d, 0)])
        plan.setdefault(4 * d + 3, []).append(some(mid_ones, d, 1))
        across_after[4 * d] = 1
        across_after[4 * d + 2] = 1
    tail = len(slots) - 4
    across_after[tail - 2] = 1
    across_after[tail - 1] = 1
    across_after[tail] = 1
    plan.setdefault(tail - 1, []).append(some(third_outer, 0, 0))
    for i, (d, piece) in enumerate(slots[: tail + 1]):
        for step in plan.get(i, []):
            step()
        serve(d, piece)
        take_across(across_after.get(i, 0))
    third_inner()
    third_outer(0, 1)
    end_pair()
    serve(*slots[tail + 1])
    take_across(1)
    third_outer(1, 0)
    close_totals()
    serve(*slots[tail + 2])
    take_across(1)
    third_outer(1, 1)
    end([0])
    serve(*slots[tail + 3])
    take_across(1)
    end([half, 5 * unit, 5 * unit + half])
    close(0)
    close(1)

    flat_one = vel[outs : outs + 1, :] * (1.0 / width)
    flat_two = jnp.sum(sum_two[...].T, axis=0, keepdims=True) * (1.0 / width)
    rate = lax.rsqrt(flat_two - flat_one * flat_one + 1e-06)
    gain = jnp.concatenate([feature[0]] * (windows * tokens // 128), axis=1)
    shift = jnp.concatenate([feature[1]] * (windows * tokens // 128), axis=1)
    value = rate * (vel[:outs, :] - flat_one * gain) + shift
    weighted = []
    for q in range(PATCH * PATCH):
        cell = jnp.concatenate([cells[q]] * (C // 8), axis=0)
        weighted.append(value[q * C : (q + 1) * C] * cell)
    chosen = []
    for alpha in range(PATCH):
        for b in range(PATCH):
            held = []
            for w in range(windows):
                at = slice(w * tokens, (w + 1) * tokens)
                straight = weighted[alpha * PATCH + b][:, at]
                swapped = weighted[(1 - alpha) * PATCH + b][:, at]
                held.append(by_parity(w, straight, swapped))
            both = jnp.concatenate(held, axis=1)
            high = both.astype(jnp.bfloat16)
            low = (both - high.astype(jnp.float32)).astype(jnp.bfloat16)
            chosen.append(jnp.concatenate([high, low], axis=0))

    def placed(alpha, which):
        total = jnp.zeros((2 * C, band), jnp.float32)
        for b in range(PATCH):
            total += jnp.dot(
                chosen[alpha * PATCH + b],
                hot[alpha * PATCH + b, :, which * band : (which + 1) * band],
                preferred_element_type=jnp.float32,
            )
        return total[:C] + total[C:]

    for which, ref, halo in ((2, far_out, 3), (1, near_out, 2)):
        for alpha in range(PATCH):
            ref[alpha * C : (alpha + 1) * C, :] = placed(alpha, which).astype(jnp.bfloat16)
        send_halo(halo)
    own = [placed(alpha, 0) for alpha in range(PATCH)]
    inverse = totals[0]
    everything = weights.at[pl.ds(0, (n - 1) * rows), :]
    pltpu.make_async_copy(everything, everything, sent.at[0]).wait()
    take_halo(2)
    take_halo(3)
    for alpha in range(PATCH):
        at = slice(alpha * C, (alpha + 1) * C)
        lines = range(alpha * quarters, (alpha + 1) * quarters)
        factor = jnp.concatenate([inverse[q : q + 1, :] for q in lines], axis=1)
        near = near_in[at, :].astype(jnp.float32)
        summed = (own[alpha] + near + far_in[at, :].astype(jnp.float32)) * factor
        for i in range(band // LW):
            out_ref[pl.ds(PATCH * i + alpha, C, stride=BAND), :] = summed[:, i * LW : (i + 1) * LW]

    for i in range(len(halos)):
        close_halo(i)


def shards(n, img_qkv, txt_kv, hidden, w_proj, w_out, modulation, anchors, blend_weight):
    windows, tokens, qkv_width = img_qkv.shape
    rows, width = w_proj.shape
    total = windows * tokens
    reach = n // 4
    deep = 2 * rows
    outs = w_out.shape[1]
    spread = (BAND + WIN) // PATCH * LW
    band = spread // 3
    any_space = pl.BlockSpec(memory_space=pl.ANY)
    vmem = pl.BlockSpec(memory_space=pltpu.VMEM)
    dma = pltpu.SemaphoreType.DMA
    f32, bf16 = jnp.float32, jnp.bfloat16
    velocity = pl.pallas_call(
        functools.partial(block_kernel, n),
        out_shape=pltpu.VMEM((C * BAND, LW), f32),
        in_specs=[any_space] * 8,
        out_specs=vmem,
        scratch_shapes=[
            pltpu.VMEM(img_qkv.shape, bf16),
            pltpu.VMEM(txt_kv.shape, bf16),
            pltpu.VMEM((total, width), bf16),
            pltpu.VMEM((n * rows, width), bf16),
            pltpu.VMEM((n * rows, total), bf16),
            pltpu.VMEM((total, 3 * deep), bf16),
            pltpu.VMEM((reach - 2, total, 2 * deep), bf16),
            pltpu.VMEM((total, deep), bf16),
            pltpu.VMEM((total, width), f32),
            pltpu.VMEM((outs, width), bf16),
            pltpu.VMEM((2 * outs + 16, width), bf16),
            pltpu.VMEM(modulation.shape, f32),
            pltpu.VMEM(anchors.shape, jnp.int32),
            pltpu.VMEM(blend_weight.shape, jnp.int32),
            pltpu.VMEM((PATCH * PATCH, 8, total), f32),
            pltpu.VMEM((PATCH * PATCH, total, spread), bf16),
            pltpu.VMEM((3, 8, 128), f32),
            pltpu.VMEM((8, 128), f32),
            pltpu.VMEM((8, 128), f32),
            pltpu.VMEM((total, 128), f32),
            pltpu.VMEM((total, 128), f32),
            pltpu.VMEM((outs + 16, total), f32),
            pltpu.VMEM((2, outs, 128), f32),
            pltpu.VMEM((PATCH * C, band), bf16),
            pltpu.VMEM((PATCH * C, band), bf16),
            pltpu.VMEM((PATCH * C, band), bf16),
            pltpu.VMEM((PATCH * C, band), bf16),
            dma((6 + 2 * windows,)),
            dma((1,)),
            dma((4 * reach + 1,)),
            dma((2 * (reach - 2) + 6,)),
            dma((3 * (reach - 3) + 11,)),
            dma((4,)),
            dma((4,)),
        ],
        compiler_params=pltpu.CompilerParams(
            collective_id=0, has_side_effects=True, vmem_limit_bytes=60 * 1024 * 1024
        ),
    )(
        img_qkv,
        txt_kv,
        hidden.reshape(total, width),
        w_proj,
        w_out.T,
        modulation,
        anchors,
        blend_weight,
    )
    return velocity.reshape(C, BAND, LW)


def solution(mesh):
    in_specs = (
        P(("group", "win"), None, None),
        P(("group", "win"), None, None),
        P(("group", "win"), None, None),
        P("win", None),
        P(),
        P("group", None),
        P(("group", "win"), None),
        P(("group", "win"), None, None),
    )
    out_specs = P(None, ("group", "win"), None)
    n = mesh.shape["win"]

    def body(*args):
        rows, width = args[3].shape
        ringed = (
            mesh.shape["group"] == 2
            and n % 4 == 0
            and n >= 16
            and rows % 16 == 0
            and width % 1536 == 0
        )
        if ringed:
            return shards(n, *args)
        return plain_shards(*args)

    return jax.shard_map(body, mesh=mesh, in_specs=in_specs, out_specs=out_specs, check_vma=False)
```

```python
import functools
import math

import jax
import jax.numpy as jnp
from jax import lax
from jax.experimental import pallas as pl
from jax.experimental.pallas import tpu as pltpu
from jax.sharding import PartitionSpec as P

HD = 128
C = 16
HEADS = 12
PATCH = 2
WIN = 32
LW = 64
BAND = 16
GRID = 16


def shifted(block, axis, distance):
    devices = range(lax.axis_size(axis))
    route = [(i - distance, i) for i in devices if i - distance in devices]
    return lax.ppermute(block, axis, route)


def place_window(canvas, totals, contrib, weights, row_at, col_at):
    zero_index = jnp.zeros((), jnp.int32)
    region = lax.dynamic_slice(canvas, (zero_index, row_at, col_at), (C, WIN, WIN))
    canvas = lax.dynamic_update_slice(canvas, region + contrib, (zero_index, row_at, col_at))
    weight_region = lax.dynamic_slice(totals, (row_at, col_at), (WIN, WIN))
    totals = lax.dynamic_update_slice(totals, weight_region + weights, (row_at, col_at))
    return (canvas, totals)


def fold_columns(field):
    span_cols = field.shape[-1] - WIN
    leading = field[..., :span_cols]
    wrapped = field[..., span_cols:]
    padding = [(0, 0)] * (field.ndim - 1) + [(0, span_cols - WIN)]
    return leading + jnp.pad(wrapped, padding)


def plain_shards(img_qkv, txt_kv, hidden, w_proj, w_out, modulation, anchors, blend_weight):
    window_count, tokens, _ = img_qkv.shape
    features = HEADS * HD
    queries = img_qkv[:, :, :features].reshape(window_count, tokens, HEADS, HD)
    all_keys = jnp.concatenate(
        [txt_kv[:, :, :features], img_qkv[:, :, features : 2 * features]], axis=1
    )
    all_keys = all_keys.reshape(window_count, -1, HEADS, HD)
    all_values = jnp.concatenate([txt_kv[:, :, features:], img_qkv[:, :, 2 * features :]], axis=1)
    all_values = all_values.reshape(window_count, -1, HEADS, HD)
    scores = jnp.einsum(
        "wqhd,wkhd->whqk", queries, all_keys, preferred_element_type=jnp.float32
    ) / math.sqrt(HD)
    scores = scores - jnp.max(scores, axis=-1, keepdims=True)
    exp_scores = jnp.exp(scores)
    soft_weights = (exp_scores / jnp.sum(exp_scores, axis=-1, keepdims=True)).astype(jnp.bfloat16)
    attended = jnp.einsum(
        "whqk,wkhd->wqhd", soft_weights, all_values, preferred_element_type=jnp.float32
    )
    attended = attended.reshape(window_count * tokens, features).astype(jnp.bfloat16)
    whole_proj = lax.all_gather(w_proj, "win", axis=0, tiled=True)
    projected = jnp.dot(attended, whole_proj, preferred_element_type=jnp.float32)
    residual = (
        hidden.reshape(window_count * tokens, -1).astype(jnp.float32) + modulation[0] * projected
    )
    row_mean = jnp.mean(residual, axis=-1, keepdims=True)
    centred = residual - row_mean
    row_var = jnp.mean(centred * centred, axis=-1, keepdims=True)
    normed = centred * lax.rsqrt(row_var + 1e-06)
    modulated = (normed * (1.0 + modulation[1]) + modulation[2]).astype(jnp.bfloat16)
    patch_vel = jnp.dot(modulated, w_out, preferred_element_type=jnp.float32)
    patch_grid = patch_vel.reshape(window_count, GRID, GRID, C, PATCH, PATCH)
    window_vel = patch_grid.transpose(0, 3, 1, 4, 2, 5).reshape(window_count, C, WIN, WIN)
    weights = blend_weight.astype(jnp.float32)
    contrib = window_vel * weights[:, None]
    band_start = lax.axis_index("win") * BAND
    canvas = jnp.zeros((C, BAND + WIN, LW + WIN), jnp.float32)
    totals = jnp.zeros((BAND + WIN, LW + WIN), jnp.float32)

    def add_one(window, running):
        row_at = anchors[window, 0] - band_start
        col_at = anchors[window, 1]
        return place_window(
            running[0], running[1], contrib[window], weights[window], row_at, col_at
        )

    canvas, totals = lax.fori_loop(0, window_count, add_one, (canvas, totals))
    canvas = fold_columns(canvas)
    totals = fold_columns(totals)
    own_canvas = canvas[:, :BAND]
    own_totals = totals[:BAND]
    near_canvas = canvas[:, BAND : 2 * BAND]
    near_totals = totals[BAND : 2 * BAND]
    far_canvas = canvas[:, 2 * BAND :]
    far_totals = totals[2 * BAND :]
    prev_canvas, prev_totals = shifted((near_canvas, near_totals), "win", 1)
    second_canvas, second_totals = shifted((far_canvas, far_totals), "win", 2)
    sum_canvas = own_canvas + prev_canvas + second_canvas
    sum_totals = own_totals + prev_totals + second_totals
    return sum_canvas / jnp.maximum(sum_totals, 1.0)[None]


LOG2E = 1.4426950408889634
MESH_ID = pl.DeviceIdType.MESH


def block_kernel(
    n,
    qkv_hbm,
    txt_hbm,
    hid_hbm,
    wp_hbm,
    wout_hbm,
    mod_hbm,
    anchors_hbm,
    blend_hbm,
    out_ref,
    qkv,
    txt,
    hid,
    weights,
    att,
    left_first,
    left_mid,
    left_side,
    left_close,
    left_last,
    acc,
    wout,
    wperm,
    mod,
    anchors,
    blend,
    cells,
    hot,
    totals,
    total_near,
    total_far,
    sum_two,
    centre,
    vel,
    feature,
    near_out,
    far_out,
    near_in,
    far_in,
    load_sems,
    sent,
    ring_recv,
    y_recv,
    part_recv,
    halo_send,
    halo_recv,
):
    windows, tokens, _ = qkv.shape
    rows = wp_hbm.shape[0]
    width = weights.shape[1]
    features = HEADS * HD
    deep = 2 * rows
    unit = width // 6
    half = unit // 2
    outs = wout.shape[0]
    chips = n // 2
    reach = chips // 2
    group = lax.axis_index("group")
    me = lax.axis_index("win")
    core = me % 2
    chip = me // 2
    depth, side = chip // 2, chip % 2
    place = depth + side * (chips - 1 - 2 * depth)

    def chip_at(position):
        spot = (position + chips) % chips
        turn = spot // reach
        return 2 * (spot + turn * (chips - 1 - 2 * spot)) + turn

    onward = (group, chip_at(place + 1) * 2 + core)
    backward = (group, chip_at(place - 1) * 2 + core)
    across = (1 - group, me)
    partner = (group, me + 1 - 2 * core)

    def source(way, d):
        return chip_at(place + d) if way else chip_at(place - d)

    def toward(way, d):
        return chip_at(place + (2 * way - 1) * d)

    def column(way, which, u):
        flip = which * (5 - 2 * u) * unit
        return (5 - u) * unit - flip if way else u * unit + flip

    def region(which_chip, which_core, col, cols):
        row = pl.multiple_of((which_chip * 2 + which_core) * rows, 16)
        return weights.at[pl.ds(row, rows), pl.ds(pl.multiple_of(col, 128), cols)]

    def remote(src, dst, send, recv, device):
        return pltpu.make_async_remote_copy(
            src_ref=src, dst_ref=dst, send_sem=send, recv_sem=recv,
            device_id=device, device_id_type=MESH_ID,
        )

    def cut(way, which, piece):
        u, side_of = piece
        col = column(way, which, u)
        if side_of is None:
            return col, unit
        return col + side_of * half, half

    whole = [(u, None) for u in range(4)]
    opening = [(0, 0), (0, 1)]
    slots = [(d, piece) for d in range(1, reach) for piece in opening + whole[1:]]
    slots += [(reach, piece) for piece in whole[:2]]
    last = reach - 1
    across_groups = []
    for d in range(1, reach):
        across_groups.append([(d, piece, way) for piece in opening for way in range(2)])
        if d < last:
            across_groups.append([(d, whole[1], way) for way in range(2)])
        else:
            across_groups += [[(d, whole[1], way)] for way in range(2)]
    across_of = {copy: i for i, group_of in enumerate(across_groups) for copy in group_of}

    def block_of(d, pieces, crossed, ways=(0, 1)):
        found = [("ring", d, way, piece) for way in ways for piece in pieces]
        return found + [("far", d, way, piece) for way in ways for piece in crossed]

    part_groups = {"own": [("own",)], "first": block_of(1, whole, whole[:2])}
    for d in range(2, last):
        for u in range(2):
            part_groups["mid", d, u] = block_of(d, whole[u : u + 1], whole[u : u + 1])
        part_groups["mid", d, 2] = block_of(d, whole[2:], [])
    for u in range(4):
        part_groups["ring", u] = block_of(last, whole[u : u + 1], [])
    for u in range(2):
        part_groups["far", u] = block_of(last, [], whole[u : u + 1])
    for u in range(2):
        part_groups["end", u] = block_of(reach, whole[u : u + 1], [])
    part_of = {name: i for i, held in enumerate(part_groups.values()) for name in held}

    def ring(way, d, piece, hop):
        ref = region(source(way, d - 1 + hop), core, *cut(way, group, piece))
        there = ring_recv.at[slots.index((d, piece))]
        return remote(ref, ref, sent.at[d // reach], there, backward if way else onward)

    def final_ring(way, side_of, which_core):
        ref = region(source(way, last), which_core, *cut(way, group, (2, side_of)))
        there = ring_recv.at[len(slots) + side_of]
        return remote(ref, ref, sent.at[1], there, backward if way else onward)

    def final_part(way, side_of):
        col, cols = cut(way, group, (2, side_of))
        row = pl.multiple_of(source(way, reach) * deep, 16)
        ref = weights.at[pl.ds(row, deep), pl.ds(pl.multiple_of(col, 128), cols)]
        there = part_recv.at[len(part_groups) + side_of]
        return remote(ref, ref, sent.at[1], there, partner)

    def yy(d, piece, way, which):
        ref = region(source(way, d), core, *cut(way, which, piece))
        return remote(ref, ref, sent.at[0], y_recv.at[across_of[d, piece, way]], across)

    def part(name):
        d = 0
        if name[0] == "own":
            ref = region(chip, core, 0, width)
        else:
            kind, d, way, piece = name
            which = group if kind == "ring" else 1 - group
            ref = region(source(way, d), core, *cut(way, which, piece))
        return remote(ref, ref, sent.at[d // reach], part_recv.at[part_of[name]], partner)

    def arrived(sem, halves):
        if halves % 2:
            ref = weights.at[pl.ds(0, halves * rows), pl.ds(0, half)]
        else:
            ref = weights.at[pl.ds(0, halves // 2 * rows), pl.ds(0, unit)]
        pltpu.make_async_copy(ref, ref, sem).wait()

    def size_of(piece):
        return 2 if piece[1] is None else 1

    landed = set()

    def wait_part(name):
        held = part_groups[name]
        sizes = [12 if one[0] == "own" else size_of(one[3]) for one in held]
        arrived(part_recv.at[part_of[held[0]]], sum(sizes))

    def need(name):
        if name not in landed:
            landed.add(name)
            wait_part(name)

    def only(which_core, *steps):
        @pl.when(core == which_core)
        def _():
            for step in steps:
                step()

    own_load = pltpu.make_async_copy(wp_hbm, region(chip, core, 0, width), load_sems.at[0])
    own_load.start()
    loads = []
    for w in range(windows):
        loads.append(
            (
                pltpu.make_async_copy(qkv_hbm.at[w], qkv.at[w], load_sems.at[1 + 2 * w]),
                pltpu.make_async_copy(txt_hbm.at[w], txt.at[w], load_sems.at[2 + 2 * w]),
            )
        )
    base = 1 + 2 * windows
    side_loads = [
        pltpu.make_async_copy(wout_hbm, wout, load_sems.at[base]),
        pltpu.make_async_copy(mod_hbm, mod, load_sems.at[base + 1]),
        pltpu.make_async_copy(anchors_hbm, anchors, load_sems.at[base + 2]),
        pltpu.make_async_copy(blend_hbm, blend, load_sems.at[base + 3]),
    ]
    hid_load = pltpu.make_async_copy(hid_hbm, hid, load_sems.at[base + 4])

    barrier = pltpu.get_barrier_semaphore()
    after = [(group, (me + 1) % n), (group, (me + 2) % n)]
    expected = 4
    for device in (onward, backward, across, partner):
        pl.semaphore_signal(barrier, inc=1, device_id=device, device_id_type=MESH_ID)
    for ahead in (-2, -1, 1, 2):
        there = (me + ahead >= 0) & (me + ahead < n)

        @pl.when(there)
        def _():
            pl.semaphore_signal(
                barrier, inc=1, device_id=(group, (me + ahead + n) % n), device_id_type=MESH_ID
            )

        expected = expected + there.astype(jnp.int32)
    for copy in loads[0]:
        copy.start()
    pl.semaphore_wait(barrier, expected)

    own_load.wait()
    for d, piece in slots[:5]:
        ring(0, d, piece, 0).start()
        ring(1, d, piece, 0).start()
    part(("own",)).start()
    for both in loads[1:]:
        for copy in both:
            copy.start()
    for copy in side_loads:
        copy.start()
    hid_load.start()

    scale = LOG2E / math.sqrt(HD)

    def attend(w, h):
        col = pl.multiple_of(h * HD, HD)
        cols = pl.ds(col, HD)
        kcols = pl.ds(pl.multiple_of(col + features, HD), HD)
        vcols = pl.ds(pl.multiple_of(col + 2 * features, HD), HD)
        q = qkv[w, :, cols]
        dims = (((1,), (1,)), ((), ()))
        st = lax.dot_general(txt[w, :, cols], q, dims, preferred_element_type=jnp.float32)
        si = lax.dot_general(qkv[w, :, kcols], q, dims, preferred_element_type=jnp.float32)
        top = jnp.maximum(jnp.max(st, axis=0, keepdims=True), jnp.max(si, axis=0, keepdims=True))
        pt = jnp.exp2((st - top) * scale)
        pi = jnp.exp2((si - top) * scale)
        total = jnp.sum(pt, axis=0, keepdims=True) + jnp.sum(pi, axis=0, keepdims=True)
        back = (((0,), (0,)), ((), ()))
        out = lax.dot_general(
            txt[w, :, kcols], pt.astype(jnp.bfloat16), back, preferred_element_type=jnp.float32
        ) + lax.dot_general(
            qkv[w, :, vcols], pi.astype(jnp.bfloat16), back, preferred_element_type=jnp.float32
        )
        att[pl.ds(col, HD), pl.ds(pl.multiple_of(w * tokens, 128), tokens)] = (
            out * (1.0 / total)
        ).astype(jnp.bfloat16)

    def spot(which_chip):
        return pl.ds(pl.multiple_of(which_chip * deep, 16), deep)

    def turn_left():
        def joined(chips_held):
            return jnp.concatenate([att[spot(c), :] for c in chips_held], axis=0).T

        left_first[...] = joined([chip, source(0, 1), source(1, 1)])
        for d in range(2, reach):
            left_mid[d - 2] = joined([source(0, d), source(1, d)])
        for way in range(2):
            left_side[way] = joined([source(way, last)])
            left_close[way] = joined([source(way, last), source(0, reach)])
        left_last[...] = joined([source(0, reach)])

    def right(chips_held, at):
        return jnp.concatenate([weights[spot(c), at] for c in chips_held], axis=0)

    def project_first(t):
        at = pl.ds(t * unit, unit)
        held = [chip, source(0, 1), source(1, 1)]
        acc[:, at] = jnp.dot(left_first[...], right(held, at), preferred_element_type=jnp.float32)

    def project_mid(d, col):
        at = pl.ds(pl.multiple_of(col, 128), unit)
        held = [source(0, d), source(1, d)]
        term = jnp.dot(left_mid[d - 2], right(held, at), preferred_element_type=jnp.float32)
        if d == 2:
            acc[:, at] = hid[:, at].astype(jnp.float32) + mod[0:1, at] * (acc[:, at] + term)
        else:
            acc[:, at] += mod[0:1, at] * term

    def project_side(t, way):
        at = pl.ds(t * unit, unit)
        term = jnp.dot(
            left_side[way], weights[spot(toward(way, last)), at], preferred_element_type=jnp.float32
        )
        acc[:, at] += mod[0:1, at] * term

    def finalize(cols, far=None, first=False):
        spans = [pl.ds(pl.multiple_of(col, 128), half) for col in cols]
        held = [source(0, reach)] if far is None else [toward(far, last), source(0, reach)]
        term = jnp.dot(
            left_last[...] if far is None else left_close[far],
            jnp.concatenate([right(held, at) for at in spans], axis=1),
            preferred_element_type=jnp.float32,
        )
        lanes = centre.shape[1]
        pieces = []
        for i, at in enumerate(spans):
            residual = acc[:, at] + mod[0:1, at] * term[:, i * half : (i + 1) * half]
            if first and i == 0:
                mean = jnp.sum(residual, axis=-1, keepdims=True) * (1.0 / half)
                centre[...] = jnp.broadcast_to(mean, centre.shape)
            pieces += [residual[:, k : k + lanes] - centre[...] for k in range(0, half, lanes)]
        two = functools.reduce(lambda a, b: a + b, [x * x for x in pieces])
        sum_two[...] = two if first else sum_two[...] + two
        moved = jnp.concatenate(pieces, axis=1).astype(jnp.bfloat16)
        term = lax.dot_general(
            jnp.concatenate([wperm[:, at] for at in spans], axis=1),
            moved,
            (((1,), (1,)), ((), ())),
            preferred_element_type=jnp.float32,
        )
        term = jnp.concatenate([term[:outs] + term[outs : 2 * outs], term[2 * outs :]], axis=0)
        vel[...] = term if first else vel[...] + term

    grid_log = GRID.bit_length() - 1
    spread = hot.shape[2]
    band = spread // 3
    quarters = band // 128

    def parity(w):
        row_at = anchors[w : w + 1, 0:1] - me * BAND
        return row_at & 1, row_at >> 1, anchors[w : w + 1, 1:2]

    def prepare_weights():
        for copy in side_loads:
            copy.wait()
        order = lax.broadcasted_iota(jnp.int32, (outs, outs), 0)
        taken = lax.broadcasted_iota(jnp.int32, (outs, outs), 1)
        wanted = (order % C) * (PATCH * PATCH) + order // C
        permute = (taken == wanted).astype(jnp.bfloat16)
        plain = jnp.dot(permute, wout[...], preferred_element_type=jnp.float32)
        gained = plain * (1.0 + mod[1:2, :])
        high = gained.astype(jnp.bfloat16)
        wperm[:outs, :] = high
        wperm[outs : 2 * outs, :] = (gained - high.astype(jnp.float32)).astype(jnp.bfloat16)
        wperm[2 * outs :, :] = jnp.ones((wperm.shape[0] - 2 * outs, width), jnp.bfloat16)
        gain = jnp.sum(gained, axis=-1, keepdims=True)
        shift = jnp.sum(plain * mod[2:3, :], axis=-1, keepdims=True)
        feature[0] = jnp.broadcast_to(gain, feature.shape[1:])
        feature[1] = jnp.broadcast_to(shift, feature.shape[1:])
        token = lax.broadcasted_iota(jnp.int32, (WIN, tokens), 1)
        line = lax.broadcasted_iota(jnp.int32, (WIN, tokens), 0)
        for w in range(windows):
            held = blend[w].astype(jnp.float32).astype(jnp.bfloat16)
            for b in range(PATCH):
                pick = (line == PATCH * (token & (GRID - 1)) + b).astype(jnp.bfloat16)
                wide = jnp.dot(held, pick, preferred_element_type=jnp.float32)
                for a in range(PATCH):
                    mine = jnp.where(line == PATCH * (token >> grid_log) + a, wide, 0.0)
                    row = jnp.sum(mine, axis=0, keepdims=True)
                    cells[a * PATCH + b, :, w * tokens : (w + 1) * tokens] = jnp.broadcast_to(
                        row, (8, tokens)
                    )

    def prepare_hot(alpha):
        token = lax.broadcasted_iota(jnp.int32, (tokens, 128), 0)
        lane = lax.broadcasted_iota(jnp.int32, (tokens, 128), 1)
        for w in range(windows):
            odd, row_at, col_at = parity(w)
            tall = (token >> grid_log) + row_at + odd * (1 - alpha)
            wide = (PATCH * (token & (GRID - 1)) + col_at) & (LW - 1)
            target = tall * LW + wide - lane
            for j in range(spread // 128):
                hot[alpha, w * tokens : (w + 1) * tokens, j * 128 : (j + 1) * 128] = jnp.where(
                    target == j * 128, 1.0, 0.0
                ).astype(jnp.bfloat16)

    def turned(field):
        lane = lax.broadcasted_iota(jnp.int32, (field.shape[0], 128), 1) & (LW - 1)
        moved = []
        for j in range(0, field.shape[1], 128):
            piece = field[:, j : j + 128]
            step, wrap = pltpu.roll(piece, 1, 1), pltpu.roll(piece, 1 + LW, 1)
            moved.append(jnp.where(lane == 0, wrap, step))
        return jnp.concatenate(moved, axis=1)

    def by_parity(w, straight, swapped):
        odd = parity(w)[0]
        return jnp.where(jnp.broadcast_to(odd, straight.shape) == 0, straight, swapped)

    def prepare_totals():
        found = []
        for alpha in range(PATCH):
            sides = []
            for b in range(PATCH):
                held = []
                for w in range(windows):
                    at = slice(w * tokens, (w + 1) * tokens)
                    straight = cells[alpha * PATCH + b, :, at]
                    swapped = cells[(1 - alpha) * PATCH + b, :, at]
                    held.append(by_parity(w, straight, swapped))
                sides.append(jnp.concatenate(held, axis=1))
            left = jnp.concatenate(sides, axis=0).astype(jnp.bfloat16)
            total = jnp.dot(left, hot[alpha], preferred_element_type=jnp.float32)
            found.append(total[:8] + turned(total[8:]))
        line = lax.broadcasted_iota(jnp.int32, (8, 128), 0)
        for i in range(3):
            total = jnp.zeros((8, 128), jnp.float32)
            for alpha in range(PATCH):
                for q in range(quarters):
                    at = i * band + q * 128
                    mine = found[alpha][:, at : at + 128]
                    total = jnp.where(line == alpha * quarters + q, mine, total)
            totals[i] = total

    halos = (
        (1, remote(totals.at[1], total_near, halo_send.at[0], halo_recv.at[0], after[0])),
        (2, remote(totals.at[2], total_far, halo_send.at[1], halo_recv.at[1], after[1])),
        (1, remote(near_out, near_in, halo_send.at[2], halo_recv.at[2], after[0])),
        (2, remote(far_out, far_in, halo_send.at[3], halo_recv.at[3], after[1])),
    )

    def send_halo(i):
        ahead, copy = halos[i]

        @pl.when(me + ahead < n)
        def _():
            copy.start()

    def take_halo(i):
        ahead, copy = halos[i]

        @pl.when(me >= ahead)
        def _():
            copy.wait_recv()

    def close_halo(i):
        ahead, copy = halos[i]

        @pl.when(me + ahead < n)
        def _():
            copy.wait_send()

    def clear_halos():
        @pl.when(me < 1)
        def _():
            total_near[...] = jnp.zeros_like(total_near)
            near_in[...] = jnp.zeros_like(near_in)

        @pl.when(me < 2)
        def _():
            total_far[...] = jnp.zeros_like(total_far)
            far_in[...] = jnp.zeros_like(far_in)

    def send_totals():
        send_halo(0)
        send_halo(1)

    def close_totals():
        take_halo(0)
        take_halo(1)
        summed = totals[0] + total_near[...] + total_far[...]
        totals[0] = 1.0 / jnp.maximum(summed, 1.0)

    def hand(kind, d, way, piece):
        if piece == opening[0]:
            return
        if piece == opening[1]:
            piece = whole[0]
        part((kind, d, way, piece)).start()

    def serve(d, piece):
        u = piece[0]
        arrived(ring_recv.at[slots.index((d, piece))], 2 * size_of(piece))
        for way in range(2):
            if d + 1 < reach:
                ring(way, d + 1, piece, 0).start()
            elif d == last and piece == opening[1]:
                ring(way, reach, whole[0], 0).start()
            elif d == last and u == 1:
                ring(way, reach, whole[1], 0).start()
            if d < reach and u < 2:
                yy(d, piece, way, group).start()
        if d == last and u == 2:

            @pl.when(core == 1)
            def _():
                for way in range(2):
                    final_ring(way, 0, 1).start()

        for way in range(2):
            hand("ring", d, way, piece)

    def send_final():
        need(("ring", 2))

        @pl.when(core == 1)
        def _():
            for side_of, which_core in ((0, 0), (1, 1), (1, 0)):
                for way in range(2):
                    final_ring(way, side_of, which_core).start()

    def serve_final(side_of):
        arrived(ring_recv.at[len(slots) + side_of], 4)
        for way in range(2):
            final_part(way, side_of).start()

    def take_final(side_of):
        arrived(part_recv.at[len(part_groups) + side_of], 4)

    def serve_across(j):
        held = across_groups[j]
        arrived(y_recv.at[j], sum(size_of(piece) for _, piece, _ in held))
        for d, piece, way in held:
            hand("far", d, way, piece)

    units = [(w, h) for w in range(windows) for h in range(HEADS)]
    ready = set()

    def attend_some(count):
        for _ in range(min(count, len(units))):
            w, h = units.pop(0)
            if w not in ready:
                for copy in loads[w]:
                    copy.wait()
                ready.add(w)
            attend(w, h)

    def first_ones(which):
        need("own")
        need("first")
        for t in which:
            project_first(t)

    def mid_ones(d, u):
        need(("mid", d, u))
        for t in (u, 5 - u):
            project_mid(d, t * unit)

    def third_inner():
        wait_part(("ring", 3))
        for t in (2, 3):
            project_mid(last, t * unit)

    def third_side(u):
        need(("ring", u))
        project_side(u, group)
        project_side(5 - u, 1 - group)

    def end(u):
        wait_part(("far", u))
        wait_part(("end", u))
        for t, far in ((u, 1 - group), (5 - u, group)):
            finalize([t * unit, t * unit + half], far, first=t == 0)

    def close(side_of):
        finalize([t * unit + side_of * half for t in (2, 3)])

    across_done = [0]

    def take_across(count):
        for _ in range(count):
            serve_across(across_done[0])
            across_done[0] += 1

    def some(fn, *args, **kwargs):
        return functools.partial(fn, *args, **kwargs)

    count = len(units)
    plan = {
        0: [some(attend_some, count // 3 - 1)],
        1: [some(attend_some, count // 12)],
        2: [some(attend_some, count // 5 + 1)],
        3: [some(attend_some, count // 5 + 1)],
        4: [some(attend_some, count // 5 + 1)],
        5: [some(attend_some, count), turn_left],
        6: [prepare_weights, clear_halos],
        7: [some(prepare_hot, 0), some(prepare_hot, 1)],
        8: [prepare_totals, send_totals],
        9: [some(first_ones, range(3))],
        11: [some(first_ones, range(3, 6)), hid_load.wait],
    }
    across_after = {4: 1, 7: 1}
    for d in range(2, last):
        plan.setdefault(5 * d + 2, []).extend([some(mid_ones, d, 2), some(mid_ones, d, 0)])
        plan.setdefault(5 * d + 4, []).append(some(mid_ones, d, 1))
        across_after[5 * d - 1] = 1
        across_after[5 * d + 2] = 1
    plan.setdefault(5 * last - 2, []).append(some(third_side, 0))
    plan.setdefault(5 * last - 1, []).append(some(third_side, 1))
    tail = len(slots) - 2
    across_after[tail - 1] = 1
    for i, (d, piece) in enumerate(slots[:tail]):
        for step in plan.get(i, []):
            step()
        serve(d, piece)
        take_across(across_after.get(i, 0))
    send_final()
    only(0, third_inner)
    serve(*slots[tail])
    take_across(1)
    only(1, third_inner)
    close_totals()
    only(0, some(end, 0))
    serve(*slots[tail + 1])
    take_across(1)
    only(1, some(end, 0), some(serve_final, 0), some(close, 0), some(serve_final, 1))
    end(1)
    only(0, some(take_final, 0), some(close, 0), some(take_final, 1))
    close(1)

    flat_one = vel[outs : outs + 1, :] * (1.0 / width)
    flat_two = jnp.sum(sum_two[...].T, axis=0, keepdims=True) * (1.0 / width)
    rate = lax.rsqrt(flat_two - flat_one * flat_one + 1e-06)
    gain = jnp.concatenate([feature[0]] * (windows * tokens // 128), axis=1)
    shift = jnp.concatenate([feature[1]] * (windows * tokens // 128), axis=1)
    value = rate * (vel[:outs, :] - flat_one * gain) + shift
    weighted = []
    for q in range(PATCH * PATCH):
        cell = jnp.concatenate([cells[q]] * (C // 8), axis=0)
        weighted.append(value[q * C : (q + 1) * C] * cell)
    chosen = []
    for alpha in range(PATCH):
        rows_of = []
        for b in range(PATCH):
            held = []
            for w in range(windows):
                at = slice(w * tokens, (w + 1) * tokens)
                straight = weighted[alpha * PATCH + b][:, at]
                swapped = weighted[(1 - alpha) * PATCH + b][:, at]
                held.append(by_parity(w, straight, swapped))
            both = jnp.concatenate(held, axis=1)
            high = both.astype(jnp.bfloat16)
            rows_of += [high, (both - high.astype(jnp.float32)).astype(jnp.bfloat16)]
        chosen.append(jnp.concatenate(rows_of, axis=0))

    def placed(alpha, which):
        at = slice(which * band, (which + 1) * band)
        total = jnp.dot(chosen[alpha], hot[alpha, :, at], preferred_element_type=jnp.float32)
        return total[:C] + total[C : 2 * C] + turned(total[2 * C : 3 * C] + total[3 * C :])

    for which, ref, halo in ((2, far_out, 3), (1, near_out, 2)):
        for alpha in range(PATCH):
            ref[alpha * C : (alpha + 1) * C, :] = placed(alpha, which).astype(ref.dtype)
        send_halo(halo)
    own = [placed(alpha, 0) for alpha in range(PATCH)]
    inverse = totals[0]
    everything = weights.at[pl.ds(0, (4 * reach - 3) * rows), :]
    pltpu.make_async_copy(everything, everything, sent.at[0]).wait()
    for side_of in range(2):

        @pl.when(core == side_of)
        def _():
            arrived(sent.at[1], 16 * (1 + side_of))

    take_halo(2)
    take_halo(3)
    for alpha in range(PATCH):
        at = slice(alpha * C, (alpha + 1) * C)
        lines = range(alpha * quarters, (alpha + 1) * quarters)
        factor = jnp.concatenate([inverse[q : q + 1, :] for q in lines], axis=1)
        summed = (own[alpha] + near_in[at, :] + far_in[at, :].astype(jnp.float32)) * factor
        for i in range(band // LW):
            out_ref[pl.ds(PATCH * i + alpha, C, stride=BAND), :] = summed[:, i * LW : (i + 1) * LW]

    for i in range(len(halos)):
        close_halo(i)


def shards(n, img_qkv, txt_kv, hidden, w_proj, w_out, modulation, anchors, blend_weight):
    windows, tokens, qkv_width = img_qkv.shape
    rows, width = w_proj.shape
    total = windows * tokens
    reach = n // 4
    deep = 2 * rows
    outs = w_out.shape[1]
    spread = (BAND + WIN) // PATCH * LW
    band = spread // 3
    any_space = pl.BlockSpec(memory_space=pl.ANY)
    vmem = pl.BlockSpec(memory_space=pltpu.VMEM)
    dma = pltpu.SemaphoreType.DMA
    f32, bf16 = jnp.float32, jnp.bfloat16
    velocity = pl.pallas_call(
        functools.partial(block_kernel, n),
        out_shape=pltpu.VMEM((C * BAND, LW), f32),
        in_specs=[any_space] * 8,
        out_specs=vmem,
        scratch_shapes=[
            pltpu.VMEM(img_qkv.shape, bf16),
            pltpu.VMEM(txt_kv.shape, bf16),
            pltpu.VMEM((total, width), bf16),
            pltpu.VMEM((n * rows, width), bf16),
            pltpu.VMEM((n * rows, total), bf16),
            pltpu.VMEM((total, 3 * deep), bf16),
            pltpu.VMEM((reach - 2, total, 2 * deep), bf16),
            pltpu.VMEM((2, total, deep), bf16),
            pltpu.VMEM((2, total, 2 * deep), bf16),
            pltpu.VMEM((total, deep), bf16),
            pltpu.VMEM((total, width), f32),
            pltpu.VMEM((outs, width), bf16),
            pltpu.VMEM((2 * outs + 16, width), bf16),
            pltpu.VMEM(modulation.shape, f32),
            pltpu.VMEM(anchors.shape, jnp.int32),
            pltpu.VMEM(blend_weight.shape, jnp.int32),
            pltpu.VMEM((PATCH * PATCH, 8, total), f32),
            pltpu.VMEM((PATCH, total, spread), bf16),
            pltpu.VMEM((3, 8, 128), f32),
            pltpu.VMEM((8, 128), f32),
            pltpu.VMEM((8, 128), f32),
            pltpu.VMEM((total, 128), f32),
            pltpu.VMEM((total, 128), f32),
            pltpu.VMEM((outs + 16, total), f32),
            pltpu.VMEM((2, outs, 128), f32),
            pltpu.VMEM((PATCH * C, band), f32),
            pltpu.VMEM((PATCH * C, band), bf16),
            pltpu.VMEM((PATCH * C, band), f32),
            pltpu.VMEM((PATCH * C, band), bf16),
            dma((6 + 2 * windows,)),
            dma((2,)),
            dma((5 * reach - 1,)),
            dma((2 * (reach - 2) + 3,)),
            dma((3 * (reach - 3) + 12,)),
            dma((4,)),
            dma((4,)),
        ],
        compiler_params=pltpu.CompilerParams(
            collective_id=0, has_side_effects=True, vmem_limit_bytes=60 * 1024 * 1024
        ),
    )(
        img_qkv,
        txt_kv,
        hidden.reshape(total, width),
        w_proj,
        w_out.T,
        modulation,
        anchors,
        blend_weight,
    )
    return velocity.reshape(C, BAND, LW)


def solution(mesh):
    in_specs = (
        P(("group", "win"), None, None),
        P(("group", "win"), None, None),
        P(("group", "win"), None, None),
        P("win", None),
        P(),
        P("group", None),
        P(("group", "win"), None),
        P(("group", "win"), None, None),
    )
    out_specs = P(None, ("group", "win"), None)
    n = mesh.shape["win"]

    def body(*args):
        rows, width = args[3].shape
        ringed = (
            mesh.shape["group"] == 2
            and n % 4 == 0
            and n >= 16
            and rows % 16 == 0
            and width % 1536 == 0
        )
        if ringed:
            return shards(n, *args)
        return plain_shards(*args)

    return jax.shard_map(body, mesh=mesh, in_specs=in_specs, out_specs=out_specs, check_vma=False)
```

```python
import functools
import math

import jax
import jax.numpy as jnp
from jax import lax
from jax.experimental import pallas as pl
from jax.experimental.pallas import tpu as pltpu
from jax.sharding import PartitionSpec as P

HD = 128
C = 16
HEADS = 12
PATCH = 2
WIN = 32
LW = 64
BAND = 16
GRID = 16


def shifted(block, axis, distance):
    devices = range(lax.axis_size(axis))
    route = [(i - distance, i) for i in devices if i - distance in devices]
    return lax.ppermute(block, axis, route)


def place_window(canvas, totals, contrib, weights, row_at, col_at):
    zero_index = jnp.zeros((), jnp.int32)
    region = lax.dynamic_slice(canvas, (zero_index, row_at, col_at), (C, WIN, WIN))
    canvas = lax.dynamic_update_slice(canvas, region + contrib, (zero_index, row_at, col_at))
    weight_region = lax.dynamic_slice(totals, (row_at, col_at), (WIN, WIN))
    totals = lax.dynamic_update_slice(totals, weight_region + weights, (row_at, col_at))
    return (canvas, totals)


def fold_columns(field):
    span_cols = field.shape[-1] - WIN
    leading = field[..., :span_cols]
    wrapped = field[..., span_cols:]
    padding = [(0, 0)] * (field.ndim - 1) + [(0, span_cols - WIN)]
    return leading + jnp.pad(wrapped, padding)


def plain_shards(img_qkv, txt_kv, hidden, w_proj, w_out, modulation, anchors, blend_weight):
    window_count, tokens, _ = img_qkv.shape
    features = HEADS * HD
    queries = img_qkv[:, :, :features].reshape(window_count, tokens, HEADS, HD)
    all_keys = jnp.concatenate(
        [txt_kv[:, :, :features], img_qkv[:, :, features : 2 * features]], axis=1
    )
    all_keys = all_keys.reshape(window_count, -1, HEADS, HD)
    all_values = jnp.concatenate([txt_kv[:, :, features:], img_qkv[:, :, 2 * features :]], axis=1)
    all_values = all_values.reshape(window_count, -1, HEADS, HD)
    scores = jnp.einsum(
        "wqhd,wkhd->whqk", queries, all_keys, preferred_element_type=jnp.float32
    ) / math.sqrt(HD)
    scores = scores - jnp.max(scores, axis=-1, keepdims=True)
    exp_scores = jnp.exp(scores)
    soft_weights = (exp_scores / jnp.sum(exp_scores, axis=-1, keepdims=True)).astype(jnp.bfloat16)
    attended = jnp.einsum(
        "whqk,wkhd->wqhd", soft_weights, all_values, preferred_element_type=jnp.float32
    )
    attended = attended.reshape(window_count * tokens, features).astype(jnp.bfloat16)
    whole_proj = lax.all_gather(w_proj, "win", axis=0, tiled=True)
    projected = jnp.dot(attended, whole_proj, preferred_element_type=jnp.float32)
    residual = (
        hidden.reshape(window_count * tokens, -1).astype(jnp.float32) + modulation[0] * projected
    )
    row_mean = jnp.mean(residual, axis=-1, keepdims=True)
    centred = residual - row_mean
    row_var = jnp.mean(centred * centred, axis=-1, keepdims=True)
    normed = centred * lax.rsqrt(row_var + 1e-06)
    modulated = (normed * (1.0 + modulation[1]) + modulation[2]).astype(jnp.bfloat16)
    patch_vel = jnp.dot(modulated, w_out, preferred_element_type=jnp.float32)
    patch_grid = patch_vel.reshape(window_count, GRID, GRID, C, PATCH, PATCH)
    window_vel = patch_grid.transpose(0, 3, 1, 4, 2, 5).reshape(window_count, C, WIN, WIN)
    weights = blend_weight.astype(jnp.float32)
    contrib = window_vel * weights[:, None]
    band_start = lax.axis_index("win") * BAND
    canvas = jnp.zeros((C, BAND + WIN, LW + WIN), jnp.float32)
    totals = jnp.zeros((BAND + WIN, LW + WIN), jnp.float32)

    def add_one(window, running):
        row_at = anchors[window, 0] - band_start
        col_at = anchors[window, 1]
        return place_window(
            running[0], running[1], contrib[window], weights[window], row_at, col_at
        )

    canvas, totals = lax.fori_loop(0, window_count, add_one, (canvas, totals))
    canvas = fold_columns(canvas)
    totals = fold_columns(totals)
    own_canvas = canvas[:, :BAND]
    own_totals = totals[:BAND]
    near_canvas = canvas[:, BAND : 2 * BAND]
    near_totals = totals[BAND : 2 * BAND]
    far_canvas = canvas[:, 2 * BAND :]
    far_totals = totals[2 * BAND :]
    prev_canvas, prev_totals = shifted((near_canvas, near_totals), "win", 1)
    second_canvas, second_totals = shifted((far_canvas, far_totals), "win", 2)
    sum_canvas = own_canvas + prev_canvas + second_canvas
    sum_totals = own_totals + prev_totals + second_totals
    return sum_canvas / jnp.maximum(sum_totals, 1.0)[None]


LOG2E = 1.4426950408889634
MESH_ID = pl.DeviceIdType.MESH


def block_kernel(
    n,
    qkv_hbm,
    txt_hbm,
    hid_hbm,
    wp_hbm,
    wout_hbm,
    mod_hbm,
    anchors_hbm,
    blend_hbm,
    out_ref,
    qkv,
    txt,
    hid,
    weights,
    att,
    left_first,
    left_mid,
    left_side,
    left_close,
    left_last,
    acc,
    wout,
    wperm,
    mod,
    anchors,
    blend,
    cells,
    hot,
    totals,
    total_near,
    total_far,
    sum_two,
    centre,
    vel,
    feature,
    near_out,
    far_out,
    near_in,
    far_in,
    load_sems,
    sent,
    ring_recv,
    y_recv,
    part_recv,
    halo_send,
    halo_recv,
):
    windows, tokens, _ = qkv.shape
    rows = wp_hbm.shape[0]
    width = weights.shape[1]
    features = HEADS * HD
    deep = 2 * rows
    unit = width // 6
    half = unit // 2
    outs = wout.shape[0]
    chips = n // 2
    reach = chips // 2
    group = lax.axis_index("group")
    me = lax.axis_index("win")
    core = me % 2
    chip = me // 2
    depth, side = chip // 2, chip % 2
    place = depth + side * (chips - 1 - 2 * depth)

    def chip_at(position):
        spot = (position + chips) % chips
        turn = spot // reach
        return 2 * (spot + turn * (chips - 1 - 2 * spot)) + turn

    onward = (group, chip_at(place + 1) * 2 + core)
    backward = (group, chip_at(place - 1) * 2 + core)
    across = (1 - group, me)
    partner = (group, me + 1 - 2 * core)

    def source(way, d):
        return chip_at(place + d) if way else chip_at(place - d)

    def toward(way, d):
        return chip_at(place + (2 * way - 1) * d)

    def column(way, which, u):
        flip = which * (5 - 2 * u) * unit
        return (5 - u) * unit - flip if way else u * unit + flip

    def region(which_chip, which_core, col, cols):
        row = pl.multiple_of((which_chip * 2 + which_core) * rows, 16)
        return weights.at[pl.ds(row, rows), pl.ds(pl.multiple_of(col, 128), cols)]

    def remote(src, dst, send, recv, device):
        return pltpu.make_async_remote_copy(
            src_ref=src, dst_ref=dst, send_sem=send, recv_sem=recv,
            device_id=device, device_id_type=MESH_ID,
        )

    def cut(way, which, piece):
        u, side_of = piece
        col = column(way, which, u)
        if side_of is None:
            return col, unit
        return col + side_of * half, half

    whole = [(u, None) for u in range(4)]
    opening = [(0, 0), (0, 1)]
    slots = [(d, piece) for d in range(1, reach) for piece in opening + whole[1:]]
    slots += [(reach, piece) for piece in whole[:2]]
    last = reach - 1
    across_groups = []
    for d in range(1, reach):
        across_groups.append([(d, piece, way) for piece in opening for way in range(2)])
        if d < last:
            across_groups.append([(d, whole[1], way) for way in range(2)])
        else:
            across_groups += [[(d, whole[1], way)] for way in range(2)]
    across_of = {copy: i for i, group_of in enumerate(across_groups) for copy in group_of}

    def block_of(d, pieces, crossed, ways=(0, 1)):
        found = [("ring", d, way, piece) for way in ways for piece in pieces]
        return found + [("far", d, way, piece) for way in ways for piece in crossed]

    part_groups = {"own": [("own",)], "first": block_of(1, whole, whole[:2])}
    for d in range(2, last):
        for u in range(2):
            part_groups["mid", d, u] = block_of(d, whole[u : u + 1], whole[u : u + 1])
        part_groups["mid", d, 2] = block_of(d, whole[2:], [])
    for u in range(4):
        part_groups["ring", u] = block_of(last, whole[u : u + 1], [])
    for u in range(2):
        part_groups["far", u] = block_of(last, [], whole[u : u + 1])
    for u in range(2):
        part_groups["end", u] = block_of(reach, whole[u : u + 1], [])
    part_of = {name: i for i, held in enumerate(part_groups.values()) for name in held}

    def ring(way, d, piece, hop):
        ref = region(source(way, d - 1 + hop), core, *cut(way, group, piece))
        there = ring_recv.at[slots.index((d, piece))]
        return remote(ref, ref, sent.at[d // reach], there, backward if way else onward)

    def final_cut(way, side_of):
        col = column(way, group, 2)
        return col + side_of * half, half

    def final_ring(way, side_of, which_core):
        ref = region(source(way, last), which_core, *final_cut(way, side_of))
        there = ring_recv.at[len(slots) + side_of]
        return remote(ref, ref, sent.at[1], there, backward if way else onward)

    def final_part(way, side_of):
        col, cols = final_cut(way, side_of)
        row = pl.multiple_of(source(way, reach) * deep, 16)
        ref = weights.at[pl.ds(row, deep), pl.ds(pl.multiple_of(col, 128), cols)]
        there = part_recv.at[len(part_groups) + side_of]
        return remote(ref, ref, sent.at[1], there, partner)

    def yy(d, piece, way, which):
        ref = region(source(way, d), core, *cut(way, which, piece))
        return remote(ref, ref, sent.at[0], y_recv.at[across_of[d, piece, way]], across)

    def part(name):
        d = 0
        if name[0] == "own":
            ref = region(chip, core, 0, width)
        else:
            kind, d, way, piece = name
            which = group if kind == "ring" else 1 - group
            ref = region(source(way, d), core, *cut(way, which, piece))
        return remote(ref, ref, sent.at[d // reach], part_recv.at[part_of[name]], partner)

    def arrived(sem, halves):
        if halves % 2:
            ref = weights.at[pl.ds(0, halves * rows), pl.ds(0, half)]
        else:
            ref = weights.at[pl.ds(0, halves // 2 * rows), pl.ds(0, unit)]
        pltpu.make_async_copy(ref, ref, sem).wait()

    def size_of(piece):
        return 2 if piece[1] is None else 1

    landed = set()

    def wait_part(name):
        held = part_groups[name]
        sizes = [12 if one[0] == "own" else size_of(one[3]) for one in held]
        arrived(part_recv.at[part_of[held[0]]], sum(sizes))

    def need(name):
        if name not in landed:
            landed.add(name)
            wait_part(name)

    def only(which_core, *steps):
        @pl.when(core == which_core)
        def _():
            for step in steps:
                step()

    own_load = pltpu.make_async_copy(wp_hbm, region(chip, core, 0, width), load_sems.at[0])
    own_load.start()
    loads = []
    for w in range(windows):
        loads.append(
            (
                pltpu.make_async_copy(qkv_hbm.at[w], qkv.at[w], load_sems.at[1 + 2 * w]),
                pltpu.make_async_copy(txt_hbm.at[w], txt.at[w], load_sems.at[2 + 2 * w]),
            )
        )
    base = 1 + 2 * windows
    side_loads = [
        pltpu.make_async_copy(wout_hbm, wout, load_sems.at[base]),
        pltpu.make_async_copy(mod_hbm, mod, load_sems.at[base + 1]),
        pltpu.make_async_copy(anchors_hbm, anchors, load_sems.at[base + 2]),
        pltpu.make_async_copy(blend_hbm, blend, load_sems.at[base + 3]),
    ]
    hid_load = pltpu.make_async_copy(hid_hbm, hid, load_sems.at[base + 4])

    barrier = pltpu.get_barrier_semaphore()
    after = [(group, (me + 1) % n), (group, (me + 2) % n)]
    expected = 4
    for device in (onward, backward, across, partner):
        pl.semaphore_signal(barrier, inc=1, device_id=device, device_id_type=MESH_ID)
    for ahead in (-2, -1, 1, 2):
        there = (me + ahead >= 0) & (me + ahead < n)

        @pl.when(there)
        def _():
            pl.semaphore_signal(
                barrier, inc=1, device_id=(group, (me + ahead + n) % n), device_id_type=MESH_ID
            )

        expected = expected + there.astype(jnp.int32)
    for copy in loads[0]:
        copy.start()
    pl.semaphore_wait(barrier, expected)

    own_load.wait()
    for d, piece in slots[:5]:
        ring(0, d, piece, 0).start()
        ring(1, d, piece, 0).start()
    part(("own",)).start()
    for both in loads[1:]:
        for copy in both:
            copy.start()
    for copy in side_loads:
        copy.start()
    hid_load.start()

    scale = LOG2E / math.sqrt(HD)

    def attend(w, h):
        col = pl.multiple_of(h * HD, HD)
        cols = pl.ds(col, HD)
        kcols = pl.ds(pl.multiple_of(col + features, HD), HD)
        vcols = pl.ds(pl.multiple_of(col + 2 * features, HD), HD)
        q = qkv[w, :, cols]
        dims = (((1,), (1,)), ((), ()))
        st = lax.dot_general(txt[w, :, cols], q, dims, preferred_element_type=jnp.float32)
        si = lax.dot_general(qkv[w, :, kcols], q, dims, preferred_element_type=jnp.float32)
        top = jnp.maximum(jnp.max(st, axis=0, keepdims=True), jnp.max(si, axis=0, keepdims=True))
        pt = jnp.exp2((st - top) * scale)
        pi = jnp.exp2((si - top) * scale)
        total = jnp.sum(pt, axis=0, keepdims=True) + jnp.sum(pi, axis=0, keepdims=True)
        back = (((0,), (0,)), ((), ()))
        out = lax.dot_general(
            txt[w, :, kcols], pt.astype(jnp.bfloat16), back, preferred_element_type=jnp.float32
        ) + lax.dot_general(
            qkv[w, :, vcols], pi.astype(jnp.bfloat16), back, preferred_element_type=jnp.float32
        )
        att[pl.ds(col, HD), pl.ds(pl.multiple_of(w * tokens, 128), tokens)] = (
            out * (1.0 / total)
        ).astype(jnp.bfloat16)

    def spot(which_chip):
        return pl.ds(pl.multiple_of(which_chip * deep, 16), deep)

    def turn_left():
        def joined(chips_held):
            return jnp.concatenate([att[spot(c), :] for c in chips_held], axis=0).T

        left_first[...] = joined([chip, source(0, 1), source(1, 1)])
        for d in range(2, reach):
            left_mid[d - 2] = joined([source(0, d), source(1, d)])
        for way in range(2):
            left_side[way] = joined([source(way, last)])
            left_close[way] = joined([source(way, last), source(0, reach)])
        left_last[...] = joined([source(0, reach)])

    def right(chips_held, at):
        return jnp.concatenate([weights[spot(c), at] for c in chips_held], axis=0)

    def project_first(t):
        at = pl.ds(t * unit, unit)
        held = [chip, source(0, 1), source(1, 1)]
        acc[:, at] = jnp.dot(left_first[...], right(held, at), preferred_element_type=jnp.float32)

    def project_mid(d, col):
        at = pl.ds(pl.multiple_of(col, 128), unit)
        held = [source(0, d), source(1, d)]
        term = jnp.dot(left_mid[d - 2], right(held, at), preferred_element_type=jnp.float32)
        if d == 2:
            acc[:, at] = hid[:, at].astype(jnp.float32) + mod[0:1, at] * (acc[:, at] + term)
        else:
            acc[:, at] += mod[0:1, at] * term

    def project_side(t, way):
        at = pl.ds(t * unit, unit)
        term = jnp.dot(
            left_side[way], weights[spot(toward(way, last)), at], preferred_element_type=jnp.float32
        )
        acc[:, at] += mod[0:1, at] * term

    def finalize(cols, far=None, first=False):
        spans = [pl.ds(pl.multiple_of(col, 128), half) for col in cols]
        held = [source(0, reach)] if far is None else [toward(far, last), source(0, reach)]
        term = jnp.dot(
            left_last[...] if far is None else left_close[far],
            jnp.concatenate([right(held, at) for at in spans], axis=1),
            preferred_element_type=jnp.float32,
        )
        lanes = centre.shape[1]
        pieces = []
        for i, at in enumerate(spans):
            residual = acc[:, at] + mod[0:1, at] * term[:, i * half : (i + 1) * half]
            if first and i == 0:
                mean = jnp.sum(residual, axis=-1, keepdims=True) * (1.0 / half)
                centre[...] = jnp.broadcast_to(mean, centre.shape)
            pieces += [residual[:, k : k + lanes] - centre[...] for k in range(0, half, lanes)]
        two = functools.reduce(lambda a, b: a + b, [x * x for x in pieces])
        sum_two[...] = two if first else sum_two[...] + two
        moved = jnp.concatenate(pieces, axis=1).astype(jnp.bfloat16)
        term = lax.dot_general(
            jnp.concatenate([wperm[:, at] for at in spans], axis=1),
            moved,
            (((1,), (1,)), ((), ())),
            preferred_element_type=jnp.float32,
        )
        term = jnp.concatenate([term[:outs] + term[outs : 2 * outs], term[2 * outs :]], axis=0)
        vel[...] = term if first else vel[...] + term

    grid_log = GRID.bit_length() - 1
    spread = hot.shape[2]
    band = spread // 3
    quarters = band // 128

    def parity(w):
        row_at = anchors[w : w + 1, 0:1] - me * BAND
        return row_at & 1, row_at >> 1, anchors[w : w + 1, 1:2]

    def prepare_weights():
        for copy in side_loads:
            copy.wait()
        order = lax.broadcasted_iota(jnp.int32, (outs, outs), 0)
        taken = lax.broadcasted_iota(jnp.int32, (outs, outs), 1)
        wanted = (order % C) * (PATCH * PATCH) + order // C
        permute = (taken == wanted).astype(jnp.bfloat16)
        plain = jnp.dot(permute, wout[...], preferred_element_type=jnp.float32)
        gained = plain * (1.0 + mod[1:2, :])
        high = gained.astype(jnp.bfloat16)
        wperm[:outs, :] = high
        wperm[outs : 2 * outs, :] = (gained - high.astype(jnp.float32)).astype(jnp.bfloat16)
        wperm[2 * outs :, :] = jnp.ones((wperm.shape[0] - 2 * outs, width), jnp.bfloat16)
        gain = jnp.sum(gained, axis=-1, keepdims=True)
        shift = jnp.sum(plain * mod[2:3, :], axis=-1, keepdims=True)
        feature[0] = jnp.broadcast_to(gain, feature.shape[1:])
        feature[1] = jnp.broadcast_to(shift, feature.shape[1:])
        token = lax.broadcasted_iota(jnp.int32, (WIN, tokens), 1)
        line = lax.broadcasted_iota(jnp.int32, (WIN, tokens), 0)
        for w in range(windows):
            held = blend[w].astype(jnp.float32).astype(jnp.bfloat16)
            for b in range(PATCH):
                pick = (line == PATCH * (token & (GRID - 1)) + b).astype(jnp.bfloat16)
                wide = jnp.dot(held, pick, preferred_element_type=jnp.float32)
                for a in range(PATCH):
                    mine = jnp.where(line == PATCH * (token >> grid_log) + a, wide, 0.0)
                    row = jnp.sum(mine, axis=0, keepdims=True)
                    cells[a * PATCH + b, :, w * tokens : (w + 1) * tokens] = jnp.broadcast_to(
                        row, (8, tokens)
                    )

    def prepare_hot(alpha):
        token = lax.broadcasted_iota(jnp.int32, (tokens, 128), 0)
        lane = lax.broadcasted_iota(jnp.int32, (tokens, 128), 1)
        for w in range(windows):
            odd, row_at, col_at = parity(w)
            tall = (token >> grid_log) + row_at + odd * (1 - alpha)
            wide = (PATCH * (token & (GRID - 1)) + col_at) & (LW - 1)
            target = tall * LW + wide - lane
            for j in range(spread // 128):
                hot[alpha, w * tokens : (w + 1) * tokens, j * 128 : (j + 1) * 128] = jnp.where(
                    target == j * 128, 1.0, 0.0
                ).astype(jnp.bfloat16)

    def turned(field):
        lane = lax.broadcasted_iota(jnp.int32, (field.shape[0], 128), 1) & (LW - 1)
        moved = []
        for j in range(0, field.shape[1], 128):
            piece = field[:, j : j + 128]
            step, wrap = pltpu.roll(piece, 1, 1), pltpu.roll(piece, 1 + LW, 1)
            moved.append(jnp.where(lane == 0, wrap, step))
        return jnp.concatenate(moved, axis=1)

    def by_parity(w, straight, swapped):
        odd = parity(w)[0]
        return jnp.where(jnp.broadcast_to(odd, straight.shape) == 0, straight, swapped)

    def prepare_totals():
        found = []
        for alpha in range(PATCH):
            sides = []
            for b in range(PATCH):
                held = []
                for w in range(windows):
                    at = slice(w * tokens, (w + 1) * tokens)
                    straight = cells[alpha * PATCH + b, :, at]
                    swapped = cells[(1 - alpha) * PATCH + b, :, at]
                    held.append(by_parity(w, straight, swapped))
                sides.append(jnp.concatenate(held, axis=1))
            left = jnp.concatenate(sides, axis=0).astype(jnp.bfloat16)
            total = jnp.dot(left, hot[alpha], preferred_element_type=jnp.float32)
            found.append(total[:8] + turned(total[8:]))
        line = lax.broadcasted_iota(jnp.int32, (8, 128), 0)
        for i in range(3):
            total = jnp.zeros((8, 128), jnp.float32)
            for alpha in range(PATCH):
                for q in range(quarters):
                    at = i * band + q * 128
                    mine = found[alpha][:, at : at + 128]
                    total = jnp.where(line == alpha * quarters + q, mine, total)
            totals[i] = total

    halos = (
        (1, remote(totals.at[1], total_near, halo_send.at[0], halo_recv.at[0], after[0])),
        (2, remote(totals.at[2], total_far, halo_send.at[1], halo_recv.at[1], after[1])),
        (1, remote(near_out, near_in, halo_send.at[2], halo_recv.at[2], after[0])),
        (2, remote(far_out, far_in, halo_send.at[3], halo_recv.at[3], after[1])),
    )

    def send_halo(i):
        ahead, copy = halos[i]

        @pl.when(me + ahead < n)
        def _():
            copy.start()

    def take_halo(i):
        ahead, copy = halos[i]

        @pl.when(me >= ahead)
        def _():
            copy.wait_recv()

    def close_halo(i):
        ahead, copy = halos[i]

        @pl.when(me + ahead < n)
        def _():
            copy.wait_send()

    def clear_halos():
        @pl.when(me < 1)
        def _():
            total_near[...] = jnp.zeros_like(total_near)
            near_in[...] = jnp.zeros_like(near_in)

        @pl.when(me < 2)
        def _():
            total_far[...] = jnp.zeros_like(total_far)
            far_in[...] = jnp.zeros_like(far_in)

    def send_totals():
        send_halo(0)
        send_halo(1)

    def close_totals():
        take_halo(0)
        take_halo(1)
        summed = totals[0] + total_near[...] + total_far[...]
        totals[0] = 1.0 / jnp.maximum(summed, 1.0)

    def hand(kind, d, way, piece):
        if piece == opening[0]:
            return
        if piece == opening[1]:
            piece = whole[0]
        part((kind, d, way, piece)).start()

    def serve(d, piece):
        u = piece[0]
        arrived(ring_recv.at[slots.index((d, piece))], 2 * size_of(piece))
        for way in range(2):
            if d + 1 < reach:
                ring(way, d + 1, piece, 0).start()
            elif d == last and piece == opening[1]:
                ring(way, reach, whole[0], 0).start()
            elif d == last and u == 1:
                ring(way, reach, whole[1], 0).start()
            if d < reach and u < 2:
                yy(d, piece, way, group).start()
        if d == last and u == 2:

            @pl.when(core == 1)
            def _():
                for way in range(2):
                    final_ring(way, 0, 1).start()

        for way in range(2):
            hand("ring", d, way, piece)

    def send_final():
        need(("ring", 2))

        @pl.when(core == 1)
        def _():
            for side_of, which_core in ((0, 0), (1, 1), (1, 0)):
                for way in range(2):
                    final_ring(way, side_of, which_core).start()

    def serve_final(side_of):
        arrived(ring_recv.at[len(slots) + side_of], 4)
        for way in range(2):
            final_part(way, side_of).start()

    def take_final(side_of):
        arrived(part_recv.at[len(part_groups) + side_of], 4)

    def serve_across(j):
        held = across_groups[j]
        arrived(y_recv.at[j], sum(size_of(piece) for _, piece, _ in held))
        for d, piece, way in held:
            hand("far", d, way, piece)

    units = [(w, h) for w in range(windows) for h in range(HEADS)]
    ready = set()

    def attend_some(count):
        for _ in range(min(count, len(units))):
            w, h = units.pop(0)
            if w not in ready:
                for copy in loads[w]:
                    copy.wait()
                ready.add(w)
            attend(w, h)

    def first_ones(which):
        need("own")
        need("first")
        for t in which:
            project_first(t)

    def mid_ones(d, u):
        need(("mid", d, u))
        for t in (u, 5 - u):
            project_mid(d, t * unit)

    def third_inner():
        wait_part(("ring", 3))
        for t in (2, 3):
            project_mid(last, t * unit)

    def third_side(u):
        need(("ring", u))
        project_side(u, group)
        project_side(5 - u, 1 - group)

    def end(u):
        wait_part(("far", u))
        wait_part(("end", u))
        for t, far in ((u, 1 - group), (5 - u, group)):
            finalize([t * unit, t * unit + half], far, first=t == 0)

    def close(side_of):
        finalize([t * unit + side_of * half for t in (2, 3)])

    across_done = [0]

    def take_across(count):
        for _ in range(count):
            serve_across(across_done[0])
            across_done[0] += 1

    def some(fn, *args, **kwargs):
        return functools.partial(fn, *args, **kwargs)

    count = len(units)
    plan = {
        0: [some(attend_some, count // 3 - 1)],
        1: [some(attend_some, count // 12)],
        2: [some(attend_some, count // 5 + 1)],
        3: [some(attend_some, count // 5 + 1)],
        4: [some(attend_some, count // 5 + 1)],
        5: [some(attend_some, count), turn_left],
        6: [prepare_weights, clear_halos],
        7: [some(prepare_hot, 0), some(prepare_hot, 1)],
        8: [prepare_totals, send_totals],
        9: [some(first_ones, range(3))],
        11: [some(first_ones, range(3, 6)), hid_load.wait],
    }
    across_after = {4: 1, 7: 1}
    for d in range(2, last):
        plan.setdefault(5 * d + 2, []).extend([some(mid_ones, d, 2), some(mid_ones, d, 0)])
        plan.setdefault(5 * d + 4, []).append(some(mid_ones, d, 1))
        across_after[5 * d - 1] = 1
        across_after[5 * d + 2] = 1
    plan.setdefault(5 * last - 2, []).append(some(third_side, 0))
    plan.setdefault(5 * last - 1, []).append(some(third_side, 1))
    tail = len(slots) - 2
    across_after[tail - 1] = 1
    for i, (d, piece) in enumerate(slots[:tail]):
        for step in plan.get(i, []):
            step()
        serve(d, piece)
        take_across(across_after.get(i, 0))
    send_final()
    only(0, third_inner)
    serve(*slots[tail])
    take_across(1)
    only(1, third_inner)
    close_totals()
    only(0, some(end, 0))
    serve(*slots[tail + 1])
    take_across(1)
    only(1, some(end, 0), some(serve_final, 0), some(close, 0), some(serve_final, 1), some(close, 1))
    end(1)
    only(0, some(take_final, 0), some(close, 0), some(take_final, 1), some(close, 1))

    flat_one = vel[outs : outs + 1, :] * (1.0 / width)
    flat_two = jnp.sum(sum_two[...].T, axis=0, keepdims=True) * (1.0 / width)
    rate = lax.rsqrt(flat_two - flat_one * flat_one + 1e-06)
    gain = jnp.concatenate([feature[0]] * (windows * tokens // 128), axis=1)
    shift = jnp.concatenate([feature[1]] * (windows * tokens // 128), axis=1)
    value = rate * (vel[:outs, :] - flat_one * gain) + shift
    weighted = []
    for q in range(PATCH * PATCH):
        cell = jnp.concatenate([cells[q]] * (C // 8), axis=0)
        weighted.append(value[q * C : (q + 1) * C] * cell)
    chosen = []
    for alpha in range(PATCH):
        rows_of = []
        for b in range(PATCH):
            held = []
            for w in range(windows):
                at = slice(w * tokens, (w + 1) * tokens)
                straight = weighted[alpha * PATCH + b][:, at]
                swapped = weighted[(1 - alpha) * PATCH + b][:, at]
                held.append(by_parity(w, straight, swapped))
            both = jnp.concatenate(held, axis=1)
            high = both.astype(jnp.bfloat16)
            rows_of += [high, (both - high.astype(jnp.float32)).astype(jnp.bfloat16)]
        chosen.append(jnp.concatenate(rows_of, axis=0))

    def placed(alpha, which):
        at = slice(which * band, (which + 1) * band)
        total = jnp.dot(chosen[alpha], hot[alpha, :, at], preferred_element_type=jnp.float32)
        return total[:C] + total[C : 2 * C] + turned(total[2 * C : 3 * C] + total[3 * C :])

    for which, ref, halo in ((2, far_out, 3), (1, near_out, 2)):
        for alpha in range(PATCH):
            ref[alpha * C : (alpha + 1) * C, :] = placed(alpha, which).astype(ref.dtype)
        send_halo(halo)
    own = [placed(alpha, 0) for alpha in range(PATCH)]
    inverse = totals[0]
    everything = weights.at[pl.ds(0, (4 * reach - 3) * rows), :]
    pltpu.make_async_copy(everything, everything, sent.at[0]).wait()
    for side_of in range(2):

        @pl.when(core == side_of)
        def _():
            arrived(sent.at[1], 16 * (1 + side_of))

    take_halo(2)
    take_halo(3)
    for alpha in range(PATCH):
        at = slice(alpha * C, (alpha + 1) * C)
        lines = range(alpha * quarters, (alpha + 1) * quarters)
        factor = jnp.concatenate([inverse[q : q + 1, :] for q in lines], axis=1)
        summed = (own[alpha] + near_in[at, :] + far_in[at, :].astype(jnp.float32)) * factor
        for i in range(band // LW):
            out_ref[pl.ds(PATCH * i + alpha, C, stride=BAND), :] = summed[:, i * LW : (i + 1) * LW]

    for i in range(len(halos)):
        close_halo(i)


def shards(n, img_qkv, txt_kv, hidden, w_proj, w_out, modulation, anchors, blend_weight):
    windows, tokens, qkv_width = img_qkv.shape
    rows, width = w_proj.shape
    total = windows * tokens
    reach = n // 4
    deep = 2 * rows
    outs = w_out.shape[1]
    spread = (BAND + WIN) // PATCH * LW
    band = spread // 3
    any_space = pl.BlockSpec(memory_space=pl.ANY)
    vmem = pl.BlockSpec(memory_space=pltpu.VMEM)
    dma = pltpu.SemaphoreType.DMA
    f32, bf16 = jnp.float32, jnp.bfloat16
    velocity = pl.pallas_call(
        functools.partial(block_kernel, n),
        out_shape=pltpu.VMEM((C * BAND, LW), f32),
        in_specs=[any_space] * 8,
        out_specs=vmem,
        scratch_shapes=[
            pltpu.VMEM(img_qkv.shape, bf16),
            pltpu.VMEM(txt_kv.shape, bf16),
            pltpu.VMEM((total, width), bf16),
            pltpu.VMEM((n * rows, width), bf16),
            pltpu.VMEM((n * rows, total), bf16),
            pltpu.VMEM((total, 3 * deep), bf16),
            pltpu.VMEM((reach - 2, total, 2 * deep), bf16),
            pltpu.VMEM((2, total, deep), bf16),
            pltpu.VMEM((2, total, 2 * deep), bf16),
            pltpu.VMEM((total, deep), bf16),
            pltpu.VMEM((total, width), f32),
            pltpu.VMEM((outs, width), bf16),
            pltpu.VMEM((2 * outs + 16, width), bf16),
            pltpu.VMEM(modulation.shape, f32),
            pltpu.VMEM(anchors.shape, jnp.int32),
            pltpu.VMEM(blend_weight.shape, jnp.int32),
            pltpu.VMEM((PATCH * PATCH, 8, total), f32),
            pltpu.VMEM((PATCH, total, spread), bf16),
            pltpu.VMEM((3, 8, 128), f32),
            pltpu.VMEM((8, 128), f32),
            pltpu.VMEM((8, 128), f32),
            pltpu.VMEM((total, 128), f32),
            pltpu.VMEM((total, 128), f32),
            pltpu.VMEM((outs + 16, total), f32),
            pltpu.VMEM((2, outs, 128), f32),
            pltpu.VMEM((PATCH * C, band), f32),
            pltpu.VMEM((PATCH * C, band), bf16),
            pltpu.VMEM((PATCH * C, band), f32),
            pltpu.VMEM((PATCH * C, band), bf16),
            dma((6 + 2 * windows,)),
            dma((2,)),
            dma((5 * reach - 1,)),
            dma((2 * (reach - 2) + 3,)),
            dma((3 * (reach - 3) + 12,)),
            dma((4,)),
            dma((4,)),
        ],
        compiler_params=pltpu.CompilerParams(
            collective_id=0, has_side_effects=True, vmem_limit_bytes=60 * 1024 * 1024
        ),
    )(
        img_qkv,
        txt_kv,
        hidden.reshape(total, width),
        w_proj,
        w_out.T,
        modulation,
        anchors,
        blend_weight,
    )
    return velocity.reshape(C, BAND, LW)


def solution(mesh):
    in_specs = (
        P(("group", "win"), None, None),
        P(("group", "win"), None, None),
        P(("group", "win"), None, None),
        P("win", None),
        P(),
        P("group", None),
        P(("group", "win"), None),
        P(("group", "win"), None, None),
    )
    out_specs = P(None, ("group", "win"), None)
    n = mesh.shape["win"]

    def body(*args):
        rows, width = args[3].shape
        ringed = (
            mesh.shape["group"] == 2
            and n % 4 == 0
            and n >= 16
            and rows % 16 == 0
            and width % 3072 == 0
        )
        if ringed:
            return shards(n, *args)
        return plain_shards(*args)

    return jax.shard_map(body, mesh=mesh, in_specs=in_specs, out_specs=out_specs, check_vma=False)
```

```python
import functools
import math

import jax
import jax.numpy as jnp
from jax import lax
from jax.experimental import pallas as pl
from jax.experimental.pallas import tpu as pltpu
from jax.sharding import PartitionSpec as P

HD = 128
C = 16
HEADS = 12
PATCH = 2
WIN = 32
LW = 64
BAND = 16
GRID = 16


def shifted(block, axis, distance):
    devices = range(lax.axis_size(axis))
    route = [(i - distance, i) for i in devices if i - distance in devices]
    return lax.ppermute(block, axis, route)


def place_window(canvas, totals, contrib, weights, row_at, col_at):
    zero_index = jnp.zeros((), jnp.int32)
    region = lax.dynamic_slice(canvas, (zero_index, row_at, col_at), (C, WIN, WIN))
    canvas = lax.dynamic_update_slice(canvas, region + contrib, (zero_index, row_at, col_at))
    weight_region = lax.dynamic_slice(totals, (row_at, col_at), (WIN, WIN))
    totals = lax.dynamic_update_slice(totals, weight_region + weights, (row_at, col_at))
    return (canvas, totals)


def fold_columns(field):
    span_cols = field.shape[-1] - WIN
    leading = field[..., :span_cols]
    wrapped = field[..., span_cols:]
    padding = [(0, 0)] * (field.ndim - 1) + [(0, span_cols - WIN)]
    return leading + jnp.pad(wrapped, padding)


def plain_shards(img_qkv, txt_kv, hidden, w_proj, w_out, modulation, anchors, blend_weight):
    window_count, tokens, _ = img_qkv.shape
    features = HEADS * HD
    queries = img_qkv[:, :, :features].reshape(window_count, tokens, HEADS, HD)
    all_keys = jnp.concatenate(
        [txt_kv[:, :, :features], img_qkv[:, :, features : 2 * features]], axis=1
    )
    all_keys = all_keys.reshape(window_count, -1, HEADS, HD)
    all_values = jnp.concatenate([txt_kv[:, :, features:], img_qkv[:, :, 2 * features :]], axis=1)
    all_values = all_values.reshape(window_count, -1, HEADS, HD)
    scores = jnp.einsum(
        "wqhd,wkhd->whqk", queries, all_keys, preferred_element_type=jnp.float32
    ) / math.sqrt(HD)
    scores = scores - jnp.max(scores, axis=-1, keepdims=True)
    exp_scores = jnp.exp(scores)
    soft_weights = (exp_scores / jnp.sum(exp_scores, axis=-1, keepdims=True)).astype(jnp.bfloat16)
    attended = jnp.einsum(
        "whqk,wkhd->wqhd", soft_weights, all_values, preferred_element_type=jnp.float32
    )
    attended = attended.reshape(window_count * tokens, features).astype(jnp.bfloat16)
    whole_proj = lax.all_gather(w_proj, "win", axis=0, tiled=True)
    projected = jnp.dot(attended, whole_proj, preferred_element_type=jnp.float32)
    residual = (
        hidden.reshape(window_count * tokens, -1).astype(jnp.float32) + modulation[0] * projected
    )
    row_mean = jnp.mean(residual, axis=-1, keepdims=True)
    centred = residual - row_mean
    row_var = jnp.mean(centred * centred, axis=-1, keepdims=True)
    normed = centred * lax.rsqrt(row_var + 1e-06)
    modulated = (normed * (1.0 + modulation[1]) + modulation[2]).astype(jnp.bfloat16)
    patch_vel = jnp.dot(modulated, w_out, preferred_element_type=jnp.float32)
    patch_grid = patch_vel.reshape(window_count, GRID, GRID, C, PATCH, PATCH)
    window_vel = patch_grid.transpose(0, 3, 1, 4, 2, 5).reshape(window_count, C, WIN, WIN)
    weights = blend_weight.astype(jnp.float32)
    contrib = window_vel * weights[:, None]
    band_start = lax.axis_index("win") * BAND
    canvas = jnp.zeros((C, BAND + WIN, LW + WIN), jnp.float32)
    totals = jnp.zeros((BAND + WIN, LW + WIN), jnp.float32)

    def add_one(window, running):
        row_at = anchors[window, 0] - band_start
        col_at = anchors[window, 1]
        return place_window(
            running[0], running[1], contrib[window], weights[window], row_at, col_at
        )

    canvas, totals = lax.fori_loop(0, window_count, add_one, (canvas, totals))
    canvas = fold_columns(canvas)
    totals = fold_columns(totals)
    own_canvas = canvas[:, :BAND]
    own_totals = totals[:BAND]
    near_canvas = canvas[:, BAND : 2 * BAND]
    near_totals = totals[BAND : 2 * BAND]
    far_canvas = canvas[:, 2 * BAND :]
    far_totals = totals[2 * BAND :]
    prev_canvas, prev_totals = shifted((near_canvas, near_totals), "win", 1)
    second_canvas, second_totals = shifted((far_canvas, far_totals), "win", 2)
    sum_canvas = own_canvas + prev_canvas + second_canvas
    sum_totals = own_totals + prev_totals + second_totals
    return sum_canvas / jnp.maximum(sum_totals, 1.0)[None]


LOG2E = 1.4426950408889634
MESH_ID = pl.DeviceIdType.MESH


def block_kernel(
    n,
    qkv_hbm,
    txt_hbm,
    hid_hbm,
    wp_hbm,
    wout_hbm,
    mod_hbm,
    anchors_hbm,
    blend_hbm,
    out_ref,
    qkv,
    txt,
    hid,
    weights,
    att,
    left_first,
    left_mid,
    left_side,
    left_close,
    left_last,
    acc,
    wout,
    wperm,
    mod,
    anchors,
    blend,
    cells,
    hot,
    totals,
    total_near,
    total_far,
    sum_two,
    centre,
    vel,
    feature,
    near_out,
    far_out,
    near_in,
    far_in,
    load_sems,
    sent,
    ring_recv,
    y_recv,
    part_recv,
    halo_send,
    halo_recv,
):
    windows, tokens, _ = qkv.shape
    rows = wp_hbm.shape[0]
    width = weights.shape[1]
    features = HEADS * HD
    deep = 2 * rows
    unit = width // 6
    half = unit // 2
    outs = wout.shape[0]
    chips = n // 2
    reach = chips // 2
    group = lax.axis_index("group")
    me = lax.axis_index("win")
    core = me % 2
    chip = me // 2
    depth, side = chip // 2, chip % 2
    place = depth + side * (chips - 1 - 2 * depth)

    def chip_at(position):
        spot = (position + chips) % chips
        turn = spot // reach
        return 2 * (spot + turn * (chips - 1 - 2 * spot)) + turn

    onward = (group, chip_at(place + 1) * 2 + core)
    backward = (group, chip_at(place - 1) * 2 + core)
    across = (1 - group, me)
    partner = (group, me + 1 - 2 * core)

    def source(way, d):
        return chip_at(place + d) if way else chip_at(place - d)

    def toward(way, d):
        return chip_at(place + (2 * way - 1) * d)

    def column(way, which, u):
        flip = which * (5 - 2 * u) * unit
        return (5 - u) * unit - flip if way else u * unit + flip

    def region(which_chip, which_core, col, cols):
        row = pl.multiple_of((which_chip * 2 + which_core) * rows, 16)
        return weights.at[pl.ds(row, rows), pl.ds(pl.multiple_of(col, 128), cols)]

    def remote(src, dst, send, recv, device):
        return pltpu.make_async_remote_copy(
            src_ref=src, dst_ref=dst, send_sem=send, recv_sem=recv,
            device_id=device, device_id_type=MESH_ID,
        )

    def cut(way, which, piece):
        u, side_of = piece
        col = column(way, which, u)
        if side_of is None:
            return col, unit
        return col + side_of * half, half

    whole = [(u, None) for u in range(4)]
    opening = [(0, 0), (0, 1)]
    slots = [(d, piece) for d in range(1, reach) for piece in opening + whole[1:]]
    slots += [(reach, piece) for piece in whole[:2]]
    last = reach - 1
    across_groups = []
    for d in range(1, reach):
        across_groups.append([(d, piece, way) for piece in opening for way in range(2)])
        if d < last:
            across_groups.append([(d, whole[1], way) for way in range(2)])
        else:
            across_groups += [[(d, whole[1], way)] for way in range(2)]
    across_of = {copy: i for i, group_of in enumerate(across_groups) for copy in group_of}

    def block_of(d, pieces, crossed, ways=(0, 1)):
        found = [("ring", d, way, piece) for way in ways for piece in pieces]
        return found + [("far", d, way, piece) for way in ways for piece in crossed]

    part_groups = {"own": [("own",)], "first": block_of(1, whole, whole[:2])}
    for d in range(2, last):
        for u in range(2):
            part_groups["mid", d, u] = block_of(d, whole[u : u + 1], whole[u : u + 1])
        part_groups["mid", d, 2] = block_of(d, whole[2:], [])
    for u in range(4):
        part_groups["ring", u] = block_of(last, whole[u : u + 1], [])
    for u in range(2):
        part_groups["far", u] = block_of(last, [], whole[u : u + 1])
    for u in range(2):
        part_groups["end", u] = block_of(reach, whole[u : u + 1], [])
    part_of = {name: i for i, held in enumerate(part_groups.values()) for name in held}

    def ring(way, d, piece, hop):
        ref = region(source(way, d - 1 + hop), core, *cut(way, group, piece))
        there = ring_recv.at[slots.index((d, piece))]
        return remote(ref, ref, sent.at[d // reach], there, backward if way else onward)

    def final_cut(way, side_of):
        col = column(way, group, 2)
        return (col + 3 * half // 2, half // 2) if side_of else (col, 3 * half // 2)

    def final_ring(way, side_of, which_core):
        ref = region(source(way, last), which_core, *final_cut(way, side_of))
        there = ring_recv.at[len(slots) + side_of]
        return remote(ref, ref, sent.at[1], there, backward if way else onward)

    def final_part(way, side_of):
        col, cols = final_cut(way, side_of)
        row = pl.multiple_of(source(way, reach) * deep, 16)
        ref = weights.at[pl.ds(row, deep), pl.ds(pl.multiple_of(col, 128), cols)]
        there = part_recv.at[len(part_groups) + side_of]
        return remote(ref, ref, sent.at[1], there, partner)

    def yy(d, piece, way, which):
        ref = region(source(way, d), core, *cut(way, which, piece))
        return remote(ref, ref, sent.at[0], y_recv.at[across_of[d, piece, way]], across)

    def part(name):
        d = 0
        if name[0] == "own":
            ref = region(chip, core, 0, width)
        else:
            kind, d, way, piece = name
            which = group if kind == "ring" else 1 - group
            ref = region(source(way, d), core, *cut(way, which, piece))
        return remote(ref, ref, sent.at[d // reach], part_recv.at[part_of[name]], partner)

    def arrived(sem, halves):
        if halves % 2:
            ref = weights.at[pl.ds(0, halves * rows), pl.ds(0, half)]
        else:
            ref = weights.at[pl.ds(0, halves // 2 * rows), pl.ds(0, unit)]
        pltpu.make_async_copy(ref, ref, sem).wait()

    def size_of(piece):
        return 2 if piece[1] is None else 1

    landed = set()

    def wait_part(name):
        held = part_groups[name]
        sizes = [12 if one[0] == "own" else size_of(one[3]) for one in held]
        arrived(part_recv.at[part_of[held[0]]], sum(sizes))

    def need(name):
        if name not in landed:
            landed.add(name)
            wait_part(name)

    def only(which_core, *steps):
        @pl.when(core == which_core)
        def _():
            for step in steps:
                step()

    own_load = pltpu.make_async_copy(wp_hbm, region(chip, core, 0, width), load_sems.at[0])
    own_load.start()
    loads = []
    for w in range(windows):
        loads.append(
            (
                pltpu.make_async_copy(qkv_hbm.at[w], qkv.at[w], load_sems.at[1 + 2 * w]),
                pltpu.make_async_copy(txt_hbm.at[w], txt.at[w], load_sems.at[2 + 2 * w]),
            )
        )
    base = 1 + 2 * windows
    side_loads = [
        pltpu.make_async_copy(wout_hbm, wout, load_sems.at[base]),
        pltpu.make_async_copy(mod_hbm, mod, load_sems.at[base + 1]),
        pltpu.make_async_copy(anchors_hbm, anchors, load_sems.at[base + 2]),
        pltpu.make_async_copy(blend_hbm, blend, load_sems.at[base + 3]),
    ]
    hid_load = pltpu.make_async_copy(hid_hbm, hid, load_sems.at[base + 4])

    barrier = pltpu.get_barrier_semaphore()
    after = [(group, (me + 1) % n), (group, (me + 2) % n)]
    expected = 4
    for device in (onward, backward, across, partner):
        pl.semaphore_signal(barrier, inc=1, device_id=device, device_id_type=MESH_ID)
    for ahead in (-2, -1, 1, 2):
        there = (me + ahead >= 0) & (me + ahead < n)

        @pl.when(there)
        def _():
            pl.semaphore_signal(
                barrier, inc=1, device_id=(group, (me + ahead + n) % n), device_id_type=MESH_ID
            )

        expected = expected + there.astype(jnp.int32)
    for copy in loads[0]:
        copy.start()
    pl.semaphore_wait(barrier, expected)

    own_load.wait()
    for d, piece in slots[:5]:
        ring(0, d, piece, 0).start()
        ring(1, d, piece, 0).start()
    part(("own",)).start()
    for both in loads[1:]:
        for copy in both:
            copy.start()
    for copy in side_loads:
        copy.start()
    hid_load.start()

    scale = LOG2E / math.sqrt(HD)

    def attend(w, h):
        col = pl.multiple_of(h * HD, HD)
        cols = pl.ds(col, HD)
        kcols = pl.ds(pl.multiple_of(col + features, HD), HD)
        vcols = pl.ds(pl.multiple_of(col + 2 * features, HD), HD)
        q = qkv[w, :, cols]
        dims = (((1,), (1,)), ((), ()))
        st = lax.dot_general(txt[w, :, cols], q, dims, preferred_element_type=jnp.float32)
        si = lax.dot_general(qkv[w, :, kcols], q, dims, preferred_element_type=jnp.float32)
        top = jnp.maximum(jnp.max(st, axis=0, keepdims=True), jnp.max(si, axis=0, keepdims=True))
        pt = jnp.exp2((st - top) * scale)
        pi = jnp.exp2((si - top) * scale)
        total = jnp.sum(pt, axis=0, keepdims=True) + jnp.sum(pi, axis=0, keepdims=True)
        back = (((0,), (0,)), ((), ()))
        out = lax.dot_general(
            txt[w, :, kcols], pt.astype(jnp.bfloat16), back, preferred_element_type=jnp.float32
        ) + lax.dot_general(
            qkv[w, :, vcols], pi.astype(jnp.bfloat16), back, preferred_element_type=jnp.float32
        )
        att[pl.ds(col, HD), pl.ds(pl.multiple_of(w * tokens, 128), tokens)] = (
            out * (1.0 / total)
        ).astype(jnp.bfloat16)

    def spot(which_chip):
        return pl.ds(pl.multiple_of(which_chip * deep, 16), deep)

    def turn_left():
        def joined(chips_held):
            return jnp.concatenate([att[spot(c), :] for c in chips_held], axis=0).T

        left_first[...] = joined([chip, source(0, 1), source(1, 1)])
        for d in range(2, reach):
            left_mid[d - 2] = joined([source(0, d), source(1, d)])
        for way in range(2):
            left_side[way] = joined([source(way, last)])
            left_close[way] = joined([source(way, last), source(0, reach)])
        left_last[...] = joined([source(0, reach)])

    def right(chips_held, at):
        return jnp.concatenate([weights[spot(c), at] for c in chips_held], axis=0)

    def project_first(t):
        at = pl.ds(t * unit, unit)
        held = [chip, source(0, 1), source(1, 1)]
        acc[:, at] = jnp.dot(left_first[...], right(held, at), preferred_element_type=jnp.float32)

    def project_mid(d, col):
        at = pl.ds(pl.multiple_of(col, 128), unit)
        held = [source(0, d), source(1, d)]
        term = jnp.dot(left_mid[d - 2], right(held, at), preferred_element_type=jnp.float32)
        if d == 2:
            acc[:, at] = hid[:, at].astype(jnp.float32) + mod[0:1, at] * (acc[:, at] + term)
        else:
            acc[:, at] += mod[0:1, at] * term

    def project_side(t, way):
        at = pl.ds(t * unit, unit)
        term = jnp.dot(
            left_side[way], weights[spot(toward(way, last)), at], preferred_element_type=jnp.float32
        )
        acc[:, at] += mod[0:1, at] * term

    def finalize(cols, far=None, first=False, wide=half):
        spans = [pl.ds(pl.multiple_of(col, 128), wide) for col in cols]
        held = [source(0, reach)] if far is None else [toward(far, last), source(0, reach)]
        term = jnp.dot(
            left_last[...] if far is None else left_close[far],
            jnp.concatenate([right(held, at) for at in spans], axis=1),
            preferred_element_type=jnp.float32,
        )
        lanes = centre.shape[1]
        pieces = []
        for i, at in enumerate(spans):
            residual = acc[:, at] + mod[0:1, at] * term[:, i * wide : (i + 1) * wide]
            if first and i == 0:
                mean = jnp.sum(residual, axis=-1, keepdims=True) * (1.0 / wide)
                centre[...] = jnp.broadcast_to(mean, centre.shape)
            pieces += [residual[:, k : k + lanes] - centre[...] for k in range(0, wide, lanes)]
        two = functools.reduce(lambda a, b: a + b, [x * x for x in pieces])
        sum_two[...] = two if first else sum_two[...] + two
        moved = jnp.concatenate(pieces, axis=1).astype(jnp.bfloat16)
        term = lax.dot_general(
            jnp.concatenate([wperm[:, at] for at in spans], axis=1),
            moved,
            (((1,), (1,)), ((), ())),
            preferred_element_type=jnp.float32,
        )
        term = jnp.concatenate([term[:outs] + term[outs : 2 * outs], term[2 * outs :]], axis=0)
        vel[...] = term if first else vel[...] + term

    grid_log = GRID.bit_length() - 1
    spread = hot.shape[2]
    band = spread // 3
    quarters = band // 128

    def parity(w):
        row_at = anchors[w : w + 1, 0:1] - me * BAND
        return row_at & 1, row_at >> 1, anchors[w : w + 1, 1:2]

    def prepare_weights():
        for copy in side_loads:
            copy.wait()
        order = lax.broadcasted_iota(jnp.int32, (outs, outs), 0)
        taken = lax.broadcasted_iota(jnp.int32, (outs, outs), 1)
        wanted = (order % C) * (PATCH * PATCH) + order // C
        permute = (taken == wanted).astype(jnp.bfloat16)
        plain = jnp.dot(permute, wout[...], preferred_element_type=jnp.float32)
        gained = plain * (1.0 + mod[1:2, :])
        high = gained.astype(jnp.bfloat16)
        wperm[:outs, :] = high
        wperm[outs : 2 * outs, :] = (gained - high.astype(jnp.float32)).astype(jnp.bfloat16)
        wperm[2 * outs :, :] = jnp.ones((wperm.shape[0] - 2 * outs, width), jnp.bfloat16)
        gain = jnp.sum(gained, axis=-1, keepdims=True)
        shift = jnp.sum(plain * mod[2:3, :], axis=-1, keepdims=True)
        feature[0] = jnp.broadcast_to(gain, feature.shape[1:])
        feature[1] = jnp.broadcast_to(shift, feature.shape[1:])
        token = lax.broadcasted_iota(jnp.int32, (WIN, tokens), 1)
        line = lax.broadcasted_iota(jnp.int32, (WIN, tokens), 0)
        for w in range(windows):
            held = blend[w].astype(jnp.float32).astype(jnp.bfloat16)
            for b in range(PATCH):
                pick = (line == PATCH * (token & (GRID - 1)) + b).astype(jnp.bfloat16)
                wide = jnp.dot(held, pick, preferred_element_type=jnp.float32)
                for a in range(PATCH):
                    mine = jnp.where(line == PATCH * (token >> grid_log) + a, wide, 0.0)
                    row = jnp.sum(mine, axis=0, keepdims=True)
                    cells[a * PATCH + b, :, w * tokens : (w + 1) * tokens] = jnp.broadcast_to(
                        row, (8, tokens)
                    )

    def prepare_hot(alpha):
        token = lax.broadcasted_iota(jnp.int32, (tokens, 128), 0)
        lane = lax.broadcasted_iota(jnp.int32, (tokens, 128), 1)
        for w in range(windows):
            odd, row_at, col_at = parity(w)
            tall = (token >> grid_log) + row_at + odd * (1 - alpha)
            wide = (PATCH * (token & (GRID - 1)) + col_at) & (LW - 1)
            target = tall * LW + wide - lane
            for j in range(spread // 128):
                hot[alpha, w * tokens : (w + 1) * tokens, j * 128 : (j + 1) * 128] = jnp.where(
                    target == j * 128, 1.0, 0.0
                ).astype(jnp.bfloat16)

    def turned(field):
        lane = lax.broadcasted_iota(jnp.int32, (field.shape[0], 128), 1) & (LW - 1)
        moved = []
        for j in range(0, field.shape[1], 128):
            piece = field[:, j : j + 128]
            step, wrap = pltpu.roll(piece, 1, 1), pltpu.roll(piece, 1 + LW, 1)
            moved.append(jnp.where(lane == 0, wrap, step))
        return jnp.concatenate(moved, axis=1)

    def by_parity(w, straight, swapped):
        odd = parity(w)[0]
        return jnp.where(jnp.broadcast_to(odd, straight.shape) == 0, straight, swapped)

    def prepare_totals():
        found = []
        for alpha in range(PATCH):
            sides = []
            for b in range(PATCH):
                held = []
                for w in range(windows):
                    at = slice(w * tokens, (w + 1) * tokens)
                    straight = cells[alpha * PATCH + b, :, at]
                    swapped = cells[(1 - alpha) * PATCH + b, :, at]
                    held.append(by_parity(w, straight, swapped))
                sides.append(jnp.concatenate(held, axis=1))
            left = jnp.concatenate(sides, axis=0).astype(jnp.bfloat16)
            total = jnp.dot(left, hot[alpha], preferred_element_type=jnp.float32)
            found.append(total[:8] + turned(total[8:]))
        line = lax.broadcasted_iota(jnp.int32, (8, 128), 0)
        for i in range(3):
            total = jnp.zeros((8, 128), jnp.float32)
            for alpha in range(PATCH):
                for q in range(quarters):
                    at = i * band + q * 128
                    mine = found[alpha][:, at : at + 128]
                    total = jnp.where(line == alpha * quarters + q, mine, total)
            totals[i] = total

    halos = (
        (1, remote(totals.at[1], total_near, halo_send.at[0], halo_recv.at[0], after[0])),
        (2, remote(totals.at[2], total_far, halo_send.at[1], halo_recv.at[1], after[1])),
        (1, remote(near_out, near_in, halo_send.at[2], halo_recv.at[2], after[0])),
        (2, remote(far_out, far_in, halo_send.at[3], halo_recv.at[3], after[1])),
    )

    def send_halo(i):
        ahead, copy = halos[i]

        @pl.when(me + ahead < n)
        def _():
            copy.start()

    def take_halo(i):
        ahead, copy = halos[i]

        @pl.when(me >= ahead)
        def _():
            copy.wait_recv()

    def close_halo(i):
        ahead, copy = halos[i]

        @pl.when(me + ahead < n)
        def _():
            copy.wait_send()

    def clear_halos():
        @pl.when(me < 1)
        def _():
            total_near[...] = jnp.zeros_like(total_near)
            near_in[...] = jnp.zeros_like(near_in)

        @pl.when(me < 2)
        def _():
            total_far[...] = jnp.zeros_like(total_far)
            far_in[...] = jnp.zeros_like(far_in)

    def send_totals():
        send_halo(0)
        send_halo(1)

    def close_totals():
        take_halo(0)
        take_halo(1)
        summed = totals[0] + total_near[...] + total_far[...]
        totals[0] = 1.0 / jnp.maximum(summed, 1.0)

    def hand(kind, d, way, piece):
        if piece == opening[0]:
            return
        if piece == opening[1]:
            piece = whole[0]
        part((kind, d, way, piece)).start()

    def serve(d, piece):
        u = piece[0]
        arrived(ring_recv.at[slots.index((d, piece))], 2 * size_of(piece))
        for way in range(2):
            if d + 1 < reach:
                ring(way, d + 1, piece, 0).start()
            elif d == last and piece == opening[1]:
                ring(way, reach, whole[0], 0).start()
            elif d == last and u == 1:
                ring(way, reach, whole[1], 0).start()
            if d < reach and u < 2:
                yy(d, piece, way, group).start()
        if d == last and u == 2:

            @pl.when(core == 1)
            def _():
                for way in range(2):
                    final_ring(way, 0, 1).start()

        for way in range(2):
            hand("ring", d, way, piece)

    def send_final():
        need(("ring", 2))

        @pl.when(core == 1)
        def _():
            for side_of, which_core in ((0, 0), (1, 1), (1, 0)):
                for way in range(2):
                    final_ring(way, side_of, which_core).start()

    def serve_final(side_of):
        arrived(ring_recv.at[len(slots) + side_of], 2 if side_of else 6)
        for way in range(2):
            final_part(way, side_of).start()

    def take_final(side_of):
        arrived(part_recv.at[len(part_groups) + side_of], 2 if side_of else 6)

    def serve_across(j):
        held = across_groups[j]
        arrived(y_recv.at[j], sum(size_of(piece) for _, piece, _ in held))
        for d, piece, way in held:
            hand("far", d, way, piece)

    units = [(w, h) for w in range(windows) for h in range(HEADS)]
    ready = set()

    def attend_some(count):
        for _ in range(min(count, len(units))):
            w, h = units.pop(0)
            if w not in ready:
                for copy in loads[w]:
                    copy.wait()
                ready.add(w)
            attend(w, h)

    def first_ones(which):
        need("own")
        need("first")
        for t in which:
            project_first(t)

    def mid_ones(d, u):
        need(("mid", d, u))
        for t in (u, 5 - u):
            project_mid(d, t * unit)

    def third_inner():
        wait_part(("ring", 3))
        for t in (2, 3):
            project_mid(last, t * unit)

    def third_side(u):
        need(("ring", u))
        project_side(u, group)
        project_side(5 - u, 1 - group)

    def end(u):
        wait_part(("far", u))
        wait_part(("end", u))
        for t, far in ((u, 1 - group), (5 - u, group)):
            finalize([t * unit, t * unit + half], far, first=t == 0)

    def close(side_of):
        start, wide = (3 * half // 2, half // 2) if side_of else (0, 3 * half // 2)
        finalize([t * unit + start for t in (2, 3)], wide=wide)

    across_done = [0]

    def take_across(count):
        for _ in range(count):
            serve_across(across_done[0])
            across_done[0] += 1

    def some(fn, *args, **kwargs):
        return functools.partial(fn, *args, **kwargs)

    count = len(units)
    plan = {
        0: [some(attend_some, count // 3 - 1)],
        1: [some(attend_some, count // 12)],
        2: [some(attend_some, count // 5 + 1)],
        3: [some(attend_some, count // 5 + 1)],
        4: [some(attend_some, count // 5 + 1)],
        5: [some(attend_some, count), turn_left],
        6: [prepare_weights, clear_halos],
        7: [some(prepare_hot, 0), some(prepare_hot, 1)],
        8: [prepare_totals, send_totals],
        9: [some(first_ones, range(3))],
        11: [some(first_ones, range(3, 6)), hid_load.wait],
    }
    across_after = {4: 1, 7: 1}
    for d in range(2, last):
        plan.setdefault(5 * d + 2, []).extend([some(mid_ones, d, 2), some(mid_ones, d, 0)])
        plan.setdefault(5 * d + 4, []).append(some(mid_ones, d, 1))
        across_after[5 * d - 1] = 1
        across_after[5 * d + 2] = 1
    plan.setdefault(5 * last - 2, []).append(some(third_side, 0))
    plan.setdefault(5 * last - 1, []).append(some(third_side, 1))
    tail = len(slots) - 2
    across_after[tail - 1] = 1
    for i, (d, piece) in enumerate(slots[:tail]):
        for step in plan.get(i, []):
            step()
        serve(d, piece)
        take_across(across_after.get(i, 0))
    send_final()
    only(0, third_inner)
    serve(*slots[tail])
    take_across(1)
    only(1, third_inner)
    close_totals()
    only(0, some(end, 0))
    serve(*slots[tail + 1])
    take_across(1)
    only(1, some(end, 0), some(serve_final, 0), some(close, 0), some(serve_final, 1), some(close, 1))
    end(1)
    only(0, some(take_final, 0), some(close, 0), some(take_final, 1), some(close, 1))

    flat_one = vel[outs : outs + 1, :] * (1.0 / width)
    flat_two = jnp.sum(sum_two[...].T, axis=0, keepdims=True) * (1.0 / width)
    rate = lax.rsqrt(flat_two - flat_one * flat_one + 1e-06)
    gain = jnp.concatenate([feature[0]] * (windows * tokens // 128), axis=1)
    shift = jnp.concatenate([feature[1]] * (windows * tokens // 128), axis=1)
    value = rate * (vel[:outs, :] - flat_one * gain) + shift
    weighted = []
    for q in range(PATCH * PATCH):
        cell = jnp.concatenate([cells[q]] * (C // 8), axis=0)
        weighted.append(value[q * C : (q + 1) * C] * cell)
    chosen = []
    for alpha in range(PATCH):
        rows_of = []
        for b in range(PATCH):
            held = []
            for w in range(windows):
                at = slice(w * tokens, (w + 1) * tokens)
                straight = weighted[alpha * PATCH + b][:, at]
                swapped = weighted[(1 - alpha) * PATCH + b][:, at]
                held.append(by_parity(w, straight, swapped))
            both = jnp.concatenate(held, axis=1)
            high = both.astype(jnp.bfloat16)
            rows_of += [high, (both - high.astype(jnp.float32)).astype(jnp.bfloat16)]
        chosen.append(jnp.concatenate(rows_of, axis=0))

    def placed(alpha, which):
        at = slice(which * band, (which + 1) * band)
        total = jnp.dot(chosen[alpha], hot[alpha, :, at], preferred_element_type=jnp.float32)
        return total[:C] + total[C : 2 * C] + turned(total[2 * C : 3 * C] + total[3 * C :])

    for which, ref, halo in ((2, far_out, 3), (1, near_out, 2)):
        for alpha in range(PATCH):
            ref[alpha * C : (alpha + 1) * C, :] = placed(alpha, which).astype(ref.dtype)
        send_halo(halo)
    own = [placed(alpha, 0) for alpha in range(PATCH)]
    inverse = totals[0]
    everything = weights.at[pl.ds(0, (4 * reach - 3) * rows), :]
    pltpu.make_async_copy(everything, everything, sent.at[0]).wait()
    for side_of in range(2):

        @pl.when(core == side_of)
        def _():
            arrived(sent.at[1], 16 * (1 + side_of))

    take_halo(2)
    take_halo(3)
    for alpha in range(PATCH):
        at = slice(alpha * C, (alpha + 1) * C)
        lines = range(alpha * quarters, (alpha + 1) * quarters)
        factor = jnp.concatenate([inverse[q : q + 1, :] for q in lines], axis=1)
        summed = (own[alpha] + near_in[at, :] + far_in[at, :].astype(jnp.float32)) * factor
        for i in range(band // LW):
            out_ref[pl.ds(PATCH * i + alpha, C, stride=BAND), :] = summed[:, i * LW : (i + 1) * LW]

    for i in range(len(halos)):
        close_halo(i)


def shards(n, img_qkv, txt_kv, hidden, w_proj, w_out, modulation, anchors, blend_weight):
    windows, tokens, qkv_width = img_qkv.shape
    rows, width = w_proj.shape
    total = windows * tokens
    reach = n // 4
    deep = 2 * rows
    outs = w_out.shape[1]
    spread = (BAND + WIN) // PATCH * LW
    band = spread // 3
    any_space = pl.BlockSpec(memory_space=pl.ANY)
    vmem = pl.BlockSpec(memory_space=pltpu.VMEM)
    dma = pltpu.SemaphoreType.DMA
    f32, bf16 = jnp.float32, jnp.bfloat16
    velocity = pl.pallas_call(
        functools.partial(block_kernel, n),
        out_shape=pltpu.VMEM((C * BAND, LW), f32),
        in_specs=[any_space] * 8,
        out_specs=vmem,
        scratch_shapes=[
            pltpu.VMEM(img_qkv.shape, bf16),
            pltpu.VMEM(txt_kv.shape, bf16),
            pltpu.VMEM((total, width), bf16),
            pltpu.VMEM((n * rows, width), bf16),
            pltpu.VMEM((n * rows, total), bf16),
            pltpu.VMEM((total, 3 * deep), bf16),
            pltpu.VMEM((reach - 2, total, 2 * deep), bf16),
            pltpu.VMEM((2, total, deep), bf16),
            pltpu.VMEM((2, total, 2 * deep), bf16),
            pltpu.VMEM((total, deep), bf16),
            pltpu.VMEM((total, width), f32),
            pltpu.VMEM((outs, width), bf16),
            pltpu.VMEM((2 * outs + 16, width), bf16),
            pltpu.VMEM(modulation.shape, f32),
            pltpu.VMEM(anchors.shape, jnp.int32),
            pltpu.VMEM(blend_weight.shape, jnp.int32),
            pltpu.VMEM((PATCH * PATCH, 8, total), f32),
            pltpu.VMEM((PATCH, total, spread), bf16),
            pltpu.VMEM((3, 8, 128), f32),
            pltpu.VMEM((8, 128), f32),
            pltpu.VMEM((8, 128), f32),
            pltpu.VMEM((total, 128), f32),
            pltpu.VMEM((total, 128), f32),
            pltpu.VMEM((outs + 16, total), f32),
            pltpu.VMEM((2, outs, 128), f32),
            pltpu.VMEM((PATCH * C, band), f32),
            pltpu.VMEM((PATCH * C, band), bf16),
            pltpu.VMEM((PATCH * C, band), f32),
            pltpu.VMEM((PATCH * C, band), bf16),
            dma((6 + 2 * windows,)),
            dma((2,)),
            dma((5 * reach - 1,)),
            dma((2 * (reach - 2) + 3,)),
            dma((3 * (reach - 3) + 12,)),
            dma((4,)),
            dma((4,)),
        ],
        compiler_params=pltpu.CompilerParams(
            collective_id=0, has_side_effects=True, vmem_limit_bytes=60 * 1024 * 1024
        ),
    )(
        img_qkv,
        txt_kv,
        hidden.reshape(total, width),
        w_proj,
        w_out.T,
        modulation,
        anchors,
        blend_weight,
    )
    return velocity.reshape(C, BAND, LW)


def solution(mesh):
    in_specs = (
        P(("group", "win"), None, None),
        P(("group", "win"), None, None),
        P(("group", "win"), None, None),
        P("win", None),
        P(),
        P("group", None),
        P(("group", "win"), None),
        P(("group", "win"), None, None),
    )
    out_specs = P(None, ("group", "win"), None)
    n = mesh.shape["win"]

    def body(*args):
        rows, width = args[3].shape
        ringed = (
            mesh.shape["group"] == 2
            and n % 4 == 0
            and n >= 16
            and rows % 16 == 0
            and width % 3072 == 0
        )
        if ringed:
            return shards(n, *args)
        return plain_shards(*args)

    return jax.shard_map(body, mesh=mesh, in_specs=in_specs, out_specs=out_specs, check_vma=False)
```
